16 devices in a mesh: data: 2 (over y, z), model: 8 (over x, core).
Axes of the slice: x: 4, y: 2, z: 1, core: 2. Of those that a mesh axis runs over, the one named last changes fastest.
The devices are a block of a 4x4x8 slice.
Arguments:
- hidden: bfloat16 [256, 3072], P(('data', 'model')), parts along dimension 0
- positions: int32 [256], P('data'), parts along dimension 0
- attn_gain: bfloat16 [1, 3072], replicated
- mlp_gain: bfloat16 [1, 3072], replicated
- w_query: bfloat16 [1, 3072, 4096], P(None, None, 'model')
- w_key: bfloat16 [1, 3072, 4096], P(None, None, 'model')
- w_value: bfloat16 [1, 3072, 4096], P(None, None, 'model')
- w_out: bfloat16 [1, 4096, 3072], P(None, 'model')
- w_gate: bfloat16 [1, 3072, 24576], P(None, None, 'model')
- w_up: bfloat16 [1, 3072, 24576], P(None, None, 'model')
- w_down: bfloat16 [1, 24576, 3072], P(None, 'model')
- k_cache: bfloat16 [1, 256, 64, 16, 256], P(None, 'data', None, 'model'), parts along dimension 1
- v_cache: bfloat16 [1, 256, 64, 16, 256], P(None, 'data', None, 'model'), parts along dimension 1
Outputs:
- output 1: bfloat16 [256, 3072], P(('data', 'model')), parts along dimension 0
- output 2: bfloat16 [1, 256, 64, 16, 256], P(None, 'data', None, 'model'), parts along dimension 1
- output 3: bfloat16 [1, 256, 64, 16, 256], P(None, 'data', None, 'model'), parts along dimension 1
There are 2 independent parts. The reference program is written for one: setup_inputs(seed, part) draws one part's arguments, and reference() takes and returns one part's arrays. A program takes and returns all parts, laid end to end along the dimension named above; an argument that names none is the same for every part.
All inputs are finite; a program needn't handle non-finite values.
Results may differ from the reference program's by a relative error of at most 0.0145115.
Values are sent between devices in bfloat16 or wider.
A program may use at most 768 MiB of HBM per device.

```python
import math
import jax
import jax.numpy as jnp
from jax import lax

N_LAYERS = 1
D_MODEL = 3072
N_HEADS = 16
KV_HEADS = 16
HEAD_DIM = 256
FFN_DIM = 24576
N_TOKENS = 128
CACHE_LEN = 64

NORM_EPS = 1e-5
ROPE_BASE = 10000.0
LOG_LEN = int(math.log2(CACHE_LEN))


def normal_weight(w_key, shape, fan_in):
    return (jax.random.normal(w_key, shape, jnp.float32) * fan_in ** -0.5).astype(jnp.bfloat16)


def draw_positions(pos_key):
    sub_keys = jax.random.split(pos_key, 3)
    raw_pos = jax.random.randint(sub_keys[0], (N_TOKENS,), 0, CACHE_LEN)
    shift_bits = jax.random.randint(sub_keys[1], (N_TOKENS,), 0, LOG_LEN)
    longest = jax.random.randint(sub_keys[2], (), 0, N_TOKENS)
    short_pos = jnp.right_shift(raw_pos, shift_bits)
    return jnp.where(jnp.arange(N_TOKENS) == longest, CACHE_LEN - 1, short_pos).astype(jnp.int32)


def setup_inputs(seed: int = 0, part: int = 0) -> dict:
    base_key = jax.random.key(seed)
    part_key = jax.random.fold_in(base_key, part)
    shared = jax.random.split(base_key, 9)
    local = jax.random.split(part_key, 5)
    q_width = N_HEADS * HEAD_DIM
    kv_width = KV_HEADS * HEAD_DIM
    hidden = jax.random.normal(local[0], (N_TOKENS, D_MODEL), jnp.float32).astype(jnp.bfloat16)
    positions = draw_positions(local[1])
    attn_gain = jax.random.uniform(shared[0], (N_LAYERS, D_MODEL), jnp.float32, 0.5, 1.5).astype(jnp.bfloat16)
    mlp_gain = jax.random.uniform(shared[1], (N_LAYERS, D_MODEL), jnp.float32, 0.5, 1.5).astype(jnp.bfloat16)
    w_query = normal_weight(shared[2], (N_LAYERS, D_MODEL, q_width), D_MODEL)
    w_key = normal_weight(shared[3], (N_LAYERS, D_MODEL, kv_width), D_MODEL)
    w_value = normal_weight(shared[4], (N_LAYERS, D_MODEL, kv_width), D_MODEL)
    w_out = normal_weight(shared[5], (N_LAYERS, q_width, D_MODEL), q_width)
    w_gate = normal_weight(shared[6], (N_LAYERS, D_MODEL, FFN_DIM), D_MODEL)
    w_up = normal_weight(shared[7], (N_LAYERS, D_MODEL, FFN_DIM), D_MODEL)
    w_down = normal_weight(shared[8], (N_LAYERS, FFN_DIM, D_MODEL), FFN_DIM)
    cache_shape = (N_LAYERS, N_TOKENS, CACHE_LEN, KV_HEADS, HEAD_DIM)
    k_cache = jax.random.normal(local[2], cache_shape, jnp.float32).astype(jnp.bfloat16)
    v_mean = jax.random.normal(local[3], (N_LAYERS, N_TOKENS, 1, KV_HEADS, HEAD_DIM), jnp.float32)
    v_cache = (0.6 * v_mean + jax.random.normal(local[4], cache_shape, jnp.float32)).astype(jnp.bfloat16)
    return {'hidden': hidden, 'positions': positions, 'attn_gain': attn_gain, 'mlp_gain': mlp_gain, 'w_query': w_query, 'w_key': w_key, 'w_value': w_value, 'w_out': w_out, 'w_gate': w_gate, 'w_up': w_up, 'w_down': w_down, 'k_cache': k_cache, 'v_cache': v_cache}


def rms_norm(row_vals, gain_vec):
    values_f = row_vals.astype(jnp.float32)
    inv_rms = lax.rsqrt(jnp.mean(values_f * values_f, axis=-1, keepdims=True) + NORM_EPS)
    return (values_f * inv_rms * gain_vec.astype(jnp.float32)).astype(jnp.bfloat16)


def rope_tables(positions):
    half_dim = HEAD_DIM // 2
    inv_freq = ROPE_BASE ** (-2.0 * jnp.arange(half_dim, dtype=jnp.float32) / HEAD_DIM)
    angles = positions.astype(jnp.float32)[:, None] * inv_freq[None, :]
    return jnp.cos(angles), jnp.sin(angles)


def rope_rotate(head_vecs, cos_tab, sin_tab):
    half_dim = head_vecs.shape[-1] // 2
    lead_shape = (cos_tab.shape[0],) + (1,) * (head_vecs.ndim - 2) + (half_dim,)
    cos_b = cos_tab.reshape(lead_shape)
    sin_b = sin_tab.reshape(lead_shape)
    front_half = head_vecs[..., :half_dim].astype(jnp.float32)
    back_half = head_vecs[..., half_dim:].astype(jnp.float32)
    rotated = jnp.concatenate([front_half * cos_b - back_half * sin_b, back_half * cos_b + front_half * sin_b], axis=-1)
    return rotated.astype(jnp.bfloat16)


def reference(hidden, positions, attn_gain, mlp_gain, w_query, w_key, w_value, w_out, w_gate, w_up, w_down, k_cache, v_cache):
    group_size = N_HEADS // KV_HEADS
    row_ids = jnp.arange(N_TOKENS)
    cos_tab, sin_tab = rope_tables(positions)
    allowed = jnp.arange(CACHE_LEN)[None, :] <= positions[:, None]

    def layer_step(hidden_state, layer_args):
        gain_attn, gain_mlp, wq_layer, wk_layer, wv_layer, wo_layer, wg_layer, wu_layer, wd_layer, k_layer, v_layer = layer_args
        normed = rms_norm(hidden_state, gain_attn)
        queries = jnp.dot(normed, wq_layer, preferred_element_type=jnp.float32).astype(jnp.bfloat16)
        keys_new = jnp.dot(normed, wk_layer, preferred_element_type=jnp.float32).astype(jnp.bfloat16)
        values_new = jnp.dot(normed, wv_layer, preferred_element_type=jnp.float32).astype(jnp.bfloat16)
        queries = rope_rotate(queries.reshape(N_TOKENS, KV_HEADS, group_size, HEAD_DIM), cos_tab, sin_tab)
        keys_new = rope_rotate(keys_new.reshape(N_TOKENS, KV_HEADS, HEAD_DIM), cos_tab, sin_tab)
        values_new = values_new.reshape(N_TOKENS, KV_HEADS, HEAD_DIM)
        k_layer = k_layer.at[row_ids, positions].set(keys_new)
        v_layer = v_layer.at[row_ids, positions].set(values_new)
        scores = jnp.einsum('bgrd,bsgd->bgrs', queries.astype(jnp.float32), k_layer.astype(jnp.float32)) * (HEAD_DIM ** -0.5)
        scores = jnp.where(allowed[:, None, None, :], scores, -1e30)
        attn_probs = jax.nn.softmax(scores, axis=-1).astype(jnp.bfloat16)
        mixed_out = jnp.einsum('bgrs,bsgd->bgrd', attn_probs.astype(jnp.float32), v_layer.astype(jnp.float32)).astype(jnp.bfloat16)
        attn_rows = mixed_out.reshape(N_TOKENS, N_HEADS * HEAD_DIM)
        hidden_state = (hidden_state.astype(jnp.float32) + jnp.dot(attn_rows, wo_layer, preferred_element_type=jnp.float32)).astype(jnp.bfloat16)
        normed = rms_norm(hidden_state, gain_mlp)
        gate_proj = jnp.dot(normed, wg_layer, preferred_element_type=jnp.float32)
        up_proj = jnp.dot(normed, wu_layer, preferred_element_type=jnp.float32)
        mlp_act = (jax.nn.silu(gate_proj) * up_proj).astype(jnp.bfloat16)
        hidden_state = (hidden_state.astype(jnp.float32) + jnp.dot(mlp_act, wd_layer, preferred_element_type=jnp.float32)).astype(jnp.bfloat16)
        return hidden_state, (k_layer, v_layer)

    final_state, caches = lax.scan(layer_step, hidden, (attn_gain, mlp_gain, w_query, w_key, w_value, w_out, w_gate, w_up, w_down, k_cache, v_cache))
    return (final_state, caches[0], caches[1])
```

```python
import functools
import math
import jax
import jax.numpy as jnp
from jax import lax
from jax.experimental import pallas as pl
from jax.experimental.pallas import tpu as pltpu
from jax.sharding import PartitionSpec as P

NORM_EPS = 1e-5
ROPE_BASE = 10000.0
BF16 = jnp.bfloat16
F32 = jnp.float32
VMEM = pl.BlockSpec(memory_space=pltpu.VMEM)
SMEM = pl.BlockSpec(memory_space=pltpu.SMEM)
HBM = pl.BlockSpec(memory_space=pltpu.HBM)
MLP_VMEM = 65800000
CHIPS = 4
MLP_CHUNK = 512


def places():
    me = lax.axis_index('model')
    core = lax.rem(me, 2)
    chip = lax.div(me, 2)
    other = me + 1 - 2 * core
    right = lax.rem(chip + 1, CHIPS) * 2 + core
    left = lax.rem(chip + CHIPS - 1, CHIPS) * 2 + core
    return me, core, chip, other, right, left


def enter(other, right, left):
    barrier = pltpu.get_barrier_semaphore()
    for peer in (other, right, left):
        pl.semaphore_signal(barrier, inc=1, device_id={'model': peer})
    pl.semaphore_wait(barrier, 3)


def remote(src, dst, send_sem, recv_sem, peer):
    return pltpu.make_async_remote_copy(src_ref=src, dst_ref=dst, send_sem=send_sem, recv_sem=recv_sem, device_id={'model': peer})


def norm_rows(x_f, gain_f):
    inv_rms = lax.rsqrt(jnp.mean(x_f * x_f, axis=-1, keepdims=True) + NORM_EPS)
    return (x_f * inv_rms * gain_f).astype(BF16)


def gather_rows(buf, send_sems, recv_sems):
    me, core, chip, other, right, left = places()
    width = buf.shape[2]
    half = width // 2
    lo, hi = pl.ds(0, half), pl.ds(half, half)
    far = lax.rem(chip + 2, CHIPS) * 2 + core
    full = pl.ds(0, width)

    def hop(blk, cols, idx, peer):
        view = buf.at[blk, :, cols]
        return remote(view, view, send_sems.at[idx], recv_sems.at[idx], peer)

    def arrive(blk, cols, idx):
        hop(blk, cols, idx, other).wait_recv()

    sends = [hop(me, lo, 0, right), hop(me, hi, 2, left), hop(me, hi, 1, right), hop(me, lo, 3, left), hop(me, full, 6, other)]
    for copy in sends:
        copy.start()

    def forward(blk, cols, idx, peer):
        copy = hop(blk, cols, idx, peer)
        copy.start()
        sends.append(copy)

    arrive(left, lo, 0)
    forward(left, lo, 4, right)
    forward(left, lo, 7, other)
    arrive(right, hi, 2)
    forward(right, hi, 5, left)
    forward(right, hi, 8, other)
    arrive(left, hi, 1)
    forward(left, hi, 9, other)
    arrive(right, lo, 3)
    forward(right, lo, 10, other)
    arrive(far, lo, 4)
    forward(far, lo, 11, other)
    arrive(far, hi, 5)
    forward(far, hi, 12, other)

    def across(blk):
        return blk + 1 - 2 * core

    arrive(other, full, 6)
    arrive(across(left), lo, 7)
    arrive(across(right), hi, 8)
    arrive(across(left), hi, 9)
    arrive(across(right), lo, 10)
    arrive(across(far), lo, 11)
    arrive(across(far), hi, 12)
    for copy in sends:
        copy.wait_send()


GATHER_SEMS = 13


def qkv_kernel(x_hbm, gain_hbm, pos_hbm, wq_hbm, wk_hbm, wv_hbm, q_ref, k_ref, v_ref, x_buf, gain_ref, pos_ref, h_buf, w_buf, load_sems, send_sems, recv_sems):
    me, core, chip, other, right, left = places()
    loads = [pltpu.make_async_copy(src, dst, load_sems.at[3 + i]) for i, (src, dst) in enumerate(((x_hbm, x_buf), (gain_hbm, gain_ref), (pos_hbm, pos_ref)))]
    for copy in loads:
        copy.start()
    w_copies = [pltpu.make_async_copy(w.at[0], w_buf.at[i], load_sems.at[i]) for i, w in enumerate((wq_hbm, wk_hbm, wv_hbm))]
    for copy in w_copies:
        copy.start()
    for copy in loads:
        copy.wait()
    h_buf[me] = norm_rows(x_buf[...].astype(F32), gain_ref[...].astype(F32))
    enter(other, right, left)
    gather_rows(h_buf, send_sems, recv_sems)

    n_tok = pos_ref.shape[1]
    half = 128
    head = 2 * half
    pos_row = jnp.broadcast_to(pos_ref[...].astype(F32), (n_tok, n_tok))
    diag = lax.broadcasted_iota(jnp.int32, (n_tok, n_tok), 0) == lax.broadcasted_iota(jnp.int32, (n_tok, n_tok), 1)
    pos_col = jnp.sum(jnp.where(diag, pos_row, 0.0), axis=1, keepdims=True)
    lane = lax.broadcasted_iota(jnp.int32, (n_tok, half), 1).astype(F32)
    angles = pos_col * jnp.exp(lane * (-2.0 * math.log(ROPE_BASE) / head))
    cos_tab, sin_tab = jnp.cos(angles), jnp.sin(angles)
    h_all = h_buf[...].reshape(n_tok, h_buf.shape[2])
    for i, out_ref in enumerate((q_ref, k_ref, v_ref)):
        w_copies[i].wait()
        proj = jnp.dot(h_all, w_buf[i], preferred_element_type=F32).astype(BF16)
        if i == 2:
            out_ref[...] = proj
            continue
        for h0 in range(0, proj.shape[1], head):
            front = proj[:, h0:h0 + half].astype(F32)
            back = proj[:, h0 + half:h0 + head].astype(F32)
            out_ref[:, h0:h0 + half] = (front * cos_tab - back * sin_tab).astype(BF16)
            out_ref[:, h0 + half:h0 + head] = (back * cos_tab + front * sin_tab).astype(BF16)


TOK_STEP = 16
TOK_SUB = 8


def attn_kernel(pos_smem, pos_ref, q_ref, k_ref, v_ref, wo_ref, kc_hbm, vc_hbm, part_ref, ko_hbm, vo_hbm,
                k_buf, v_buf, new_buf, q_buf, o_buf, pc_buf, in_sems, out_sems):
    _, n_tok, n_rows, n_heads, head = kc_hbm.shape
    lanes = 128
    steps = n_tok // TOK_STEP
    per_tok = n_rows * n_heads
    bufs = (k_buf, v_buf)

    def copies(t, hbm_pair, sems, outward):
        made = []
        for kv in range(2):
            flat = hbm_pair[kv].reshape(1, n_tok, per_tok, head)
            for c in range(2):
                far = flat.at[0, pl.ds(t * TOK_STEP, TOK_STEP), :, pl.ds(c * lanes, lanes)]
                near = bufs[kv].at[c, pl.ds(t * TOK_STEP, TOK_STEP)]
                src, dst = (near, far) if outward else (far, near)
                made.append(pltpu.make_async_copy(src, dst, sems.at[kv, c, t]))
        return made

    for t in range(steps):
        for copy in copies(t, (kc_hbm, vc_hbm), in_sems, False):
            copy.start()

    for h in range(n_heads):
        for c in range(2):
            cols = slice(h * head + c * lanes, h * head + (c + 1) * lanes)
            q_buf.at[c][pl.ds(h, n_tok, stride=2), :] = q_ref[:, cols].astype(F32)
            new_buf[0, h, c] = k_ref[:, cols].astype(F32)
            new_buf[1, h, c] = v_ref[:, cols].astype(F32)
    rows2 = n_tok * n_heads
    pos_row = jnp.broadcast_to(pos_ref[...].astype(F32), (rows2, n_tok))
    own = lax.broadcasted_iota(jnp.int32, (rows2, n_tok), 0) // 2 == lax.broadcasted_iota(jnp.int32, (rows2, n_tok), 1)
    pc_buf[...] = jnp.broadcast_to(jnp.sum(jnp.where(own, pos_row, 0.0), axis=1, keepdims=True), (rows2, n_tok))

    tile_row = lax.broadcasted_iota(jnp.int32, (16, lanes), 0)
    sub_rows = TOK_SUB * n_heads
    q_row = lax.broadcasted_iota(jnp.int32, (sub_rows, lanes), 0)
    key_col = lax.broadcasted_iota(jnp.int32, (sub_rows, lanes), 1)
    same_head = (q_row % 2) == (key_col % 2)
    key_pos = (key_col // 2).astype(F32)
    q_tok = q_row // 2

    def step(t, carry):
        for copy in copies(t, (kc_hbm, vc_hbm), in_sems, False):
            copy.wait()
        for i in range(TOK_STEP):
            b = t * TOK_STEP + i
            pos = pos_smem[0, b]
            tile = pl.ds(pl.multiple_of((pos >> 3) * 16, 16), 16)
            hit = (tile_row >> 1) == (pos & 7)
            for kv in range(2):
                for c in range(2):
                    old = bufs[kv][c, b, tile, :].astype(F32)
                    new = jnp.where((tile_row & 1) == 1, new_buf[kv, 1, c, pl.ds(b, 1), :], new_buf[kv, 0, c, pl.ds(b, 1), :])
                    bufs[kv][c, b, tile, :] = jnp.where(hit, new, old).astype(BF16)
        for sub in range(TOK_STEP // TOK_SUB):
            b0 = t * TOK_STEP + sub * TOK_SUB
            rows = pl.ds(pl.multiple_of(b0 * n_heads, 16), sub_rows)
            toks = pl.ds(b0, TOK_SUB)
            q = jnp.concatenate([q_buf[0, rows, :], q_buf[1, rows, :]], axis=1).astype(BF16)
            keys = jnp.concatenate([k_buf[c, toks].reshape(TOK_SUB * per_tok, lanes) for c in range(2)], axis=1)
            scores = lax.dot_general(q, keys, (((1,), (1,)), ((), ())), preferred_element_type=F32)
            mine = jnp.zeros((sub_rows, lanes), F32)
            for m in range(TOK_SUB):
                mine = jnp.where(q_tok == m, scores[:, m * lanes:(m + 1) * lanes], mine)
            mine = mine * (head ** -0.5)
            mine = jnp.where(same_head & (key_pos <= pc_buf[rows, :]), mine, -1e30)
            e = jnp.exp(mine - jnp.max(mine, axis=1, keepdims=True))
            probs = (e / jnp.sum(e, axis=1, keepdims=True)).astype(BF16).astype(F32)
            wide = jnp.concatenate([jnp.where(q_tok == m, probs, 0.0) for m in range(TOK_SUB)], axis=1).astype(BF16)
            vals = jnp.concatenate([v_buf[c, toks].reshape(TOK_SUB * per_tok, lanes) for c in range(2)], axis=1)
            out = jnp.dot(wide, vals, preferred_element_type=F32).astype(BF16).astype(F32)
            o_buf[0, rows, :] = out[:, :lanes]
            o_buf[1, rows, :] = out[:, lanes:]
        for copy in copies(t, (ko_hbm, vo_hbm), out_sems, True):
            copy.start()
        return carry

    lax.fori_loop(0, steps, step, 0)
    attn = jnp.concatenate([o_buf.at[c][pl.ds(h, n_tok, stride=2), :] for h in range(n_heads) for c in range(2)], axis=1).astype(BF16)
    width = part_ref.shape[1]
    for n0 in range(0, width, 768):
        part_ref[:, n0:n0 + 768] = jnp.dot(attn, wo_ref[0, :, n0:n0 + 768], preferred_element_type=F32).astype(BF16)
    for t in range(steps):
        for copy in copies(t, (ko_hbm, vo_hbm), out_sems, True):
            copy.wait()


class Reducer:
    def __init__(self, part, from_other, chip_sum, far_in, near_in, last_in, send_sems, recv_sems):
        self.part, self.from_other, self.chip_sum = part, from_other, chip_sum
        self.far_in, self.near_in, self.last_in = far_in, near_in, last_in
        self.send_sems, self.recv_sems = send_sems, recv_sems
        self.me, self.core, self.chip, self.other, self.right, self.left = places()
        self.sends = []

    def copy(self, kind, j, cols, way):
        nxt, prv = (self.right, self.left) if way > 0 else (self.left, self.right)
        ahead = lax.rem(self.chip + CHIPS + way, CHIPS)
        behind = lax.rem(self.chip + CHIPS - way, CHIPS)
        opposite = lax.rem(self.chip + 2, CHIPS)
        src, dst, peer = (
            (self.part.at[:, 1 - self.core, :, cols], self.from_other.at[:, :, cols], self.other),
            (self.chip_sum.at[opposite, :, cols], self.far_in.at[:, cols], nxt),
            (self.chip_sum.at[behind, :, cols], self.near_in.at[:, cols], prv),
            (self.chip_sum.at[ahead, :, cols], self.last_in.at[:, cols], nxt),
        )[kind]
        return remote(src, dst, self.send_sems.at[kind, j], self.recv_sems.at[kind, j], peer)

    def go(self, kind, j, cols, way):
        copy = self.copy(kind, j, cols, way)
        copy.start()
        self.sends.append(copy)

    def begin(self, j, cols, way):
        self.go(0, j, cols, way)

    def add_chip(self, k, cols):
        total = self.part[k, self.core, :, cols].astype(F32) + self.from_other[k, :, cols].astype(F32)
        self.chip_sum[k, :, cols] = total.astype(BF16)

    def second(self, j, cols, way):
        self.copy(0, j, cols, way).wait_recv()
        self.add_chip(lax.rem(self.chip + 2, CHIPS), cols)
        self.go(1, j, cols, way)
        self.add_chip(lax.rem(self.chip + CHIPS - way, CHIPS), cols)
        self.go(2, j, cols, way)

    def third(self, j, cols, way):
        ahead = lax.rem(self.chip + CHIPS + way, CHIPS)
        mine = self.part[ahead, self.core, :, cols].astype(F32) + self.from_other[ahead, :, cols].astype(F32)
        self.copy(1, j, cols, way).wait_recv()
        self.chip_sum[ahead, :, cols] = (mine + self.far_in[:, cols].astype(F32)).astype(BF16)
        self.go(3, j, cols, way)

    def last(self, j, cols, way):
        own = self.part[self.chip, self.core, :, cols].astype(F32) + self.from_other[self.chip, :, cols].astype(F32)
        self.copy(2, j, cols, way).wait_recv()
        own = own + self.near_in[:, cols].astype(F32)
        self.copy(3, j, cols, way).wait_recv()
        return own + self.last_in[:, cols].astype(F32)

    def finish(self):
        for copy in self.sends:
            copy.wait_send()


def mlp_kernel(part1, x_buf, gain_ref, w1_hbm, w3_hbm, w2_hbm, out_ref,
               other1, sum1, far1, near1, last1, part2, other2, sum2, far2, near2, last2,
               x1_buf, h_buf, act_buf, w1_buf, w3_buf, w2_buf,
               w_sems, rs1_send, rs1_recv, ag_send, ag_recv, rs2_send, rs2_recv):
    me, core, chip, other, right, left = places()
    width = x_buf.shape[1]
    n_chunks = w1_buf.shape[0]
    chunk = w1_buf.shape[2]

    def weight(kind, i):
        src = (w1_hbm, w3_hbm, w2_hbm)[kind]
        dst = (w1_buf, w3_buf, w2_buf)[kind]
        return pltpu.make_async_copy(src.at[0, :, pl.ds(pl.multiple_of(i * chunk, 128), chunk)], dst.at[i], w_sems.at[kind, i])

    for i in range(n_chunks):
        weight(0, i).start()
        weight(1, i).start()
    for i in range(n_chunks):
        weight(2, i).start()

    enter(other, right, left)
    half = width // 2
    plan1 = [(0, pl.ds(0, half), 1), (1, pl.ds(half, half), -1)]
    rs1 = Reducer(part1, other1, sum1, far1, near1, last1, rs1_send, rs1_recv)
    for stage in (rs1.begin, rs1.second, rs1.third):
        for item in plan1:
            stage(*item)
    for item in plan1:
        cols = item[1]
        x1_buf[:, cols] = (x_buf[:, cols].astype(F32) + rs1.last(*item)).astype(BF16)
    h_buf[me] = norm_rows(x1_buf[...].astype(F32), gain_ref[...].astype(F32))
    gather_rows(h_buf, ag_send, ag_recv)

    n_tok = act_buf.shape[0]

    def gate_up(i, carry):
        weight(0, i).wait()
        weight(1, i).wait()
        h_all = h_buf[...].reshape(n_tok, width)
        gate = jnp.dot(h_all, w1_buf[i], preferred_element_type=F32)
        up = jnp.dot(h_all, w3_buf[i], preferred_element_type=F32)
        act_buf[:, pl.ds(pl.multiple_of(i * chunk, 128), chunk)] = (gate * jax.nn.sigmoid(gate) * up).astype(BF16)
        return carry

    lax.fori_loop(0, n_chunks, gate_up, 0)

    rs2 = Reducer(part2, other2, sum2, far2, near2, last2, rs2_send, rs2_recv)
    plan2 = [(j, pl.ds(j * chunk, chunk), 1 if j % 2 == 0 else -1) for j in range(n_chunks)]

    def final(item):
        cols = item[1]
        out_ref[:, cols] = (x1_buf[:, cols].astype(F32) + rs2.last(*item)).astype(BF16)

    for j in range(n_chunks + 4):
        if j < n_chunks:
            weight(2, j).wait()
            down = jnp.dot(act_buf[...], w2_buf[j], preferred_element_type=F32).astype(BF16)
            part2[:, :, :, plan2[j][1]] = down.reshape(CHIPS, 2, n_tok // (2 * CHIPS), chunk)
            rs2.begin(*plan2[j])
        for lag, stage in ((1, rs2.second), (3, rs2.third), (4, final)):
            if 0 <= j - lag < n_chunks:
                stage(*plan2[j - lag]) if lag != 4 else final(plan2[j - lag])
    rs1.finish()
    rs2.finish()


def shape(dims, dtype=BF16):
    return jax.ShapeDtypeStruct(dims, dtype)


def run_qkv(x, gain, pos2, wq, wk, wv):
    n_tok = pos2.shape[1]
    rows, width = x.shape
    cols = wq.shape[2]
    blocks = n_tok // rows
    dma = pltpu.SemaphoreType.DMA
    return pl.pallas_call(
        qkv_kernel,
        out_shape=[shape((n_tok, cols))] * 3,
        in_specs=[HBM] * 6,
        out_specs=[VMEM] * 3,
        scratch_shapes=[
            pltpu.VMEM((rows, width), BF16), pltpu.VMEM(gain.shape, BF16), pltpu.VMEM(pos2.shape, pos2.dtype),
            pltpu.VMEM((blocks, rows, width), BF16), pltpu.VMEM((3, width, cols), BF16),
            dma((6,)), dma((GATHER_SEMS,)), dma((GATHER_SEMS,))],
        compiler_params=pltpu.CompilerParams(collective_id=0, has_side_effects=True, vmem_limit_bytes=32 << 20),
        name='gather_qkv',
    )(x, gain, pos2, wq, wk, wv)


def run_attn(pos2, q, k, v, wo, k_cache, v_cache):
    _, n_tok, n_rows, n_heads, head = k_cache.shape
    width = wo.shape[2]
    steps = n_tok // TOK_STEP
    dma = pltpu.SemaphoreType.DMA
    cache = pltpu.VMEM((2, n_tok, n_rows * n_heads, 128), BF16)
    wide = pltpu.VMEM((2, n_tok * n_heads, 128), F32)
    return pl.pallas_call(
        attn_kernel,
        out_shape=[shape((n_tok, width)), shape(k_cache.shape), shape(v_cache.shape)],
        in_specs=[SMEM, VMEM, VMEM, VMEM, VMEM, VMEM, HBM, HBM],
        out_specs=[VMEM, HBM, HBM],
        scratch_shapes=[
            cache, cache, pltpu.VMEM((2, n_heads, 2, n_tok, 128), F32), wide, wide, pltpu.VMEM((n_tok * n_heads, n_tok), F32),
            dma((2, 2, steps)), dma((2, 2, steps))],
        compiler_params=pltpu.CompilerParams(vmem_limit_bytes=48 << 20),
        name='attention',
    )(pos2, pos2, q, k, v, wo, k_cache, v_cache)


def run_mlp(part, x, gain, w1, w3, w2):
    rows, width = x.shape
    n_tok = part.shape[1] * part.shape[0] * part.shape[2]
    ffn = w1.shape[2]
    chunk = MLP_CHUNK
    n_chunks = ffn // chunk
    dma = pltpu.SemaphoreType.DMA
    block = pltpu.VMEM((rows, width), BF16)
    reduce_bufs = [pltpu.VMEM((CHIPS, 2, rows, width), BF16), pltpu.VMEM((CHIPS, rows, width), BF16), pltpu.VMEM((CHIPS, rows, width), BF16)] + [block] * 3
    return pl.pallas_call(
        mlp_kernel,
        out_shape=shape((rows, width)),
        in_specs=[VMEM, VMEM, VMEM, HBM, HBM, HBM],
        out_specs=VMEM,
        scratch_shapes=reduce_bufs[1:] + reduce_bufs + [
            block, pltpu.VMEM((n_tok // rows, rows, width), BF16), pltpu.VMEM((n_tok, ffn), BF16),
            pltpu.VMEM((n_chunks, width, chunk), BF16), pltpu.VMEM((n_chunks, width, chunk), BF16), pltpu.VMEM((width // chunk, ffn, chunk), BF16),
            dma((3, n_chunks)), dma((4, 2)), dma((4, 2)), dma((GATHER_SEMS,)), dma((GATHER_SEMS,)),
            dma((4, n_chunks)), dma((4, n_chunks))],
        compiler_params=pltpu.CompilerParams(collective_id=1, has_side_effects=True, vmem_limit_bytes=MLP_VMEM),
        name='reduce_mlp',
    )(part, x, gain, w1, w3, w2)


def solution(mesh):
    row_spec = P(('data', 'model'), None)
    cache_spec = P(None, 'data', None, 'model', None)
    col_spec = P(None, None, 'model')
    inner_spec = P(None, 'model', None)
    in_specs = (row_spec, P('data'), P(), P(), col_spec, col_spec, col_spec, inner_spec, col_spec, col_spec, inner_spec, cache_spec, cache_spec)
    out_specs = (row_spec, cache_spec, cache_spec)

    def device_step(hidden, positions, attn_gain, mlp_gain, w_query, w_key, w_value, w_out, w_gate, w_up, w_down, k_cache, v_cache):
        rows, width = hidden.shape
        n_tok = positions.shape[0]
        pos2 = positions.reshape(1, n_tok)
        q, k, v = run_qkv(hidden, attn_gain, pos2, w_query, w_key, w_value)
        part, k_out, v_out = run_attn(pos2, q, k, v, w_out, k_cache, v_cache)
        out = run_mlp(part.reshape(CHIPS, 2, rows, width), hidden, mlp_gain, w_gate, w_up, w_down)
        return out, k_out, v_out

    return jax.shard_map(device_step, mesh=mesh, in_specs=in_specs, out_specs=out_specs, check_vma=False)
```

```python
import functools
import math
import jax
import jax.numpy as jnp
from jax import lax
from jax.experimental import pallas as pl
from jax.experimental.pallas import tpu as pltpu
from jax.sharding import PartitionSpec as P

NORM_EPS = 1e-5
ROPE_BASE = 10000.0
BF16 = jnp.bfloat16
F32 = jnp.float32
VMEM = pl.BlockSpec(memory_space=pltpu.VMEM)
SMEM = pl.BlockSpec(memory_space=pltpu.SMEM)
HBM = pl.BlockSpec(memory_space=pltpu.HBM)
MLP_VMEM = 63400000
CHIPS = 4
MLP_CHUNK = 512
RS1_PIECES = 4
RS2_LAG = 3
GATHER_SEMS = 21


def places():
    me = lax.axis_index('model')
    core = lax.rem(me, 2)
    chip = lax.div(me, 2)
    other = me + 1 - 2 * core
    right = lax.rem(chip + 1, CHIPS) * 2 + core
    left = lax.rem(chip + CHIPS - 1, CHIPS) * 2 + core
    return me, core, chip, other, right, left


def knock(other, right, left):
    barrier = pltpu.get_barrier_semaphore()
    for peer in (other, right, left):
        pl.semaphore_signal(barrier, inc=1, device_id={'model': peer})


def enter():
    pl.semaphore_wait(pltpu.get_barrier_semaphore(), 3)


def remote(src, dst, send_sem, recv_sem, peer):
    return pltpu.make_async_remote_copy(src_ref=src, dst_ref=dst, send_sem=send_sem, recv_sem=recv_sem, device_id={'model': peer})


def norm_rows(x_f, gain_f):
    inv_rms = lax.rsqrt(jnp.mean(x_f * x_f, axis=-1, keepdims=True) + NORM_EPS)
    return (x_f * inv_rms * gain_f).astype(BF16)


def gather_rows(buf, send_sems, recv_sems):
    me, core, chip, other, right, left = places()
    width = buf.shape[2]
    quarter = width // 4
    q0, q1, q2, q3 = (pl.ds(i * quarter, quarter) for i in range(4))
    lo, hi, full = pl.ds(0, 2 * quarter), pl.ds(2 * quarter, 2 * quarter), pl.ds(0, width)
    far = lax.rem(chip + 2, CHIPS) * 2 + core
    sends = []

    def hop(blk, cols, idx, peer):
        view = buf.at[blk, :, cols]
        return remote(view, view, send_sems.at[idx], recv_sems.at[idx], peer)

    def arrive(blk, cols, idx):
        hop(blk, cols, idx, other).wait_recv()

    def send(blk, cols, idx, peer):
        copy = hop(blk, cols, idx, peer)
        copy.start()
        sends.append(copy)

    for cols, idx, peer in ((q0, 0, right), (q2, 1, left), (q1, 2, right), (q3, 3, left), (hi, 4, right), (lo, 5, left), (full, 6, other)):
        send(me, cols, idx, peer)
    across = []
    for blk, cols, idx, onward, peer in (
            (left, q0, 0, 7, right), (right, q2, 1, 8, left), (left, q1, 2, 9, right), (right, q3, 3, 10, left),
            (left, hi, 4, None, None), (right, lo, 5, None, None),
            (far, q0, 7, None, None), (far, q2, 8, None, None), (far, q1, 9, None, None), (far, q3, 10, None, None)):
        arrive(blk, cols, idx)
        if onward is not None:
            send(blk, cols, onward, peer)
        send(blk, cols, 11 + len(across), other)
        across.append((blk + 1 - 2 * core, cols, 11 + len(across)))
    arrive(other, full, 6)
    for item in across:
        arrive(*item)
    for copy in sends:
        copy.wait_send()


LANES = 128


def cache_copies(hbm, buf, sems, start, size, outward=False):
    _, n_tok, n_rows, n_heads, head = hbm.shape
    flat = hbm.reshape(1, n_tok, n_rows * n_heads, head)
    made = []
    for c in range(2):
        far = flat.at[0, pl.ds(start, size), :, pl.ds(c * LANES, LANES)]
        near = buf.at[c, pl.ds(start, size)]
        src, dst = (near, far) if outward else (far, near)
        made.append(pltpu.make_async_copy(src, dst, sems.at[c]))
    return made


def qkv_kernel(x_hbm, gain_hbm, pos_hbm, wq_hbm, wk_hbm, wv_hbm, kc_hbm, vc_hbm, q_ref, k_ref, v_ref, kb_ref, vb_ref,
               x_buf, gain_ref, pos_ref, h_buf, w_buf, load_sems, cache_sems, send_sems, recv_sems):
    me, core, chip, other, right, left = places()
    knock(other, right, left)
    loads = [pltpu.make_async_copy(src, dst, load_sems.at[3 + i]) for i, (src, dst) in enumerate(((x_hbm, x_buf), (gain_hbm, gain_ref), (pos_hbm, pos_ref)))]
    w_copies = [pltpu.make_async_copy(w.at[0], w_buf.at[i], load_sems.at[i]) for i, w in enumerate((wq_hbm, wk_hbm, wv_hbm))]
    piece = kb_ref.shape[1] // 2
    cache_in = []
    for kv, (hbm, buf) in enumerate(((kc_hbm, kb_ref), (vc_hbm, vb_ref))):
        for p in range(2):
            for c in range(2):
                src = hbm.at[0, pl.ds(p * piece, piece), :, :, pl.ds(c * LANES, LANES)]
                cache_in.append(pltpu.make_async_copy(src, buf.at[c, pl.ds(p * piece, piece)], cache_sems.at[kv, p, c]))
    for copy in loads + w_copies + cache_in:
        copy.start()
    for copy in loads:
        copy.wait()
    h_buf[me] = norm_rows(x_buf[...].astype(F32), gain_ref[...].astype(F32))
    enter()
    gather_rows(h_buf, send_sems, recv_sems)

    n_tok = pos_ref.shape[1]
    half = 128
    head = 2 * half
    pos_row = jnp.broadcast_to(pos_ref[...].astype(F32), (n_tok, n_tok))
    diag = lax.broadcasted_iota(jnp.int32, (n_tok, n_tok), 0) == lax.broadcasted_iota(jnp.int32, (n_tok, n_tok), 1)
    pos_col = jnp.sum(jnp.where(diag, pos_row, 0.0), axis=1, keepdims=True)
    lane = lax.broadcasted_iota(jnp.int32, (n_tok, half), 1).astype(F32)
    angles = pos_col * jnp.exp(lane * (-2.0 * math.log(ROPE_BASE) / head))
    cos_tab, sin_tab = jnp.cos(angles), jnp.sin(angles)
    h_all = h_buf[...].reshape(n_tok, h_buf.shape[2])
    for i, out_ref in enumerate((q_ref, k_ref, v_ref)):
        w_copies[i].wait()
        proj = jnp.dot(h_all, w_buf[i], preferred_element_type=F32).astype(BF16)
        if i == 2:
            out_ref[...] = proj
            continue
        for h0 in range(0, proj.shape[1], head):
            front = proj[:, h0:h0 + half].astype(F32)
            back = proj[:, h0 + half:h0 + head].astype(F32)
            out_ref[:, h0:h0 + half] = (front * cos_tab - back * sin_tab).astype(BF16)
            out_ref[:, h0 + half:h0 + head] = (back * cos_tab + front * sin_tab).astype(BF16)
    for copy in cache_in:
        copy.wait()


TOK_STEP = 16
TOK_SUB = 8


def attn_kernel(pos_smem, pos_ref, q_ref, k_ref, v_ref, kb_in, vb_in, attn_ref, k_buf, v_buf, ko_hbm, vo_hbm,
                new_buf, q_buf, o_buf, pc_buf, out_sems):
    _, n_tok, n_rows, n_heads, head = ko_hbm.shape
    lanes = LANES
    steps = n_tok // TOK_STEP
    per_tok = n_rows * n_heads
    bufs = (k_buf, v_buf)

    def write_out(t):
        made = []
        for kv, hbm in enumerate((ko_hbm, vo_hbm)):
            made += cache_copies(hbm, bufs[kv], out_sems.at[kv, t], t * TOK_STEP, TOK_STEP, True)
        return made

    for h in range(n_heads):
        for c in range(2):
            cols = slice(h * head + c * lanes, h * head + (c + 1) * lanes)
            q_buf.at[c][pl.ds(h, n_tok, stride=2), :] = q_ref[:, cols].astype(F32)
            new_buf[0, h, c] = k_ref[:, cols].astype(F32)
            new_buf[1, h, c] = v_ref[:, cols].astype(F32)
    rows2 = n_tok * n_heads
    pos_row = jnp.broadcast_to(pos_ref[...].astype(F32), (rows2, n_tok))
    own = lax.broadcasted_iota(jnp.int32, (rows2, n_tok), 0) // 2 == lax.broadcasted_iota(jnp.int32, (rows2, n_tok), 1)
    pc_buf[...] = jnp.broadcast_to(jnp.sum(jnp.where(own, pos_row, 0.0), axis=1, keepdims=True), (rows2, n_tok))

    tile_row = lax.broadcasted_iota(jnp.int32, (16, lanes), 0)
    sub_rows = TOK_SUB * n_heads
    q_row = lax.broadcasted_iota(jnp.int32, (sub_rows, lanes), 0)
    key_col = lax.broadcasted_iota(jnp.int32, (sub_rows, lanes), 1)
    same_head = (q_row % 2) == (key_col % 2)
    key_pos = (key_col // 2).astype(F32)
    q_tok = q_row // 2

    def step(t, carry):
        for i in range(TOK_STEP):
            b = t * TOK_STEP + i
            pos = pos_smem[0, b]
            tile = pl.ds(pl.multiple_of((pos >> 3) * 16, 16), 16)
            hit = (tile_row >> 1) == (pos & 7)
            for kv in range(2):
                for c in range(2):
                    old = bufs[kv][c, b, tile, :].astype(F32)
                    new = jnp.where((tile_row & 1) == 1, new_buf[kv, 1, c, pl.ds(b, 1), :], new_buf[kv, 0, c, pl.ds(b, 1), :])
                    bufs[kv][c, b, tile, :] = jnp.where(hit, new, old).astype(BF16)
        for sub in range(TOK_STEP // TOK_SUB):
            b0 = t * TOK_STEP + sub * TOK_SUB
            rows = pl.ds(pl.multiple_of(b0 * n_heads, 16), sub_rows)
            toks = pl.ds(b0, TOK_SUB)
            q = jnp.concatenate([q_buf[0, rows, :], q_buf[1, rows, :]], axis=1).astype(BF16)
            keys = jnp.concatenate([k_buf[c, toks].reshape(TOK_SUB * per_tok, lanes) for c in range(2)], axis=1)
            scores = lax.dot_general(q, keys, (((1,), (1,)), ((), ())), preferred_element_type=F32)
            mine = jnp.zeros((sub_rows, lanes), F32)
            for m in range(TOK_SUB):
                mine = jnp.where(q_tok == m, scores[:, m * lanes:(m + 1) * lanes], mine)
            mine = mine * (head ** -0.5)
            mine = jnp.where(same_head & (key_pos <= pc_buf[rows, :]), mine, -1e30)
            e = jnp.exp(mine - jnp.max(mine, axis=1, keepdims=True))
            probs = (e / jnp.sum(e, axis=1, keepdims=True)).astype(BF16).astype(F32)
            wide = jnp.concatenate([jnp.where(q_tok == m, probs, 0.0) for m in range(TOK_SUB)], axis=1).astype(BF16)
            vals = jnp.concatenate([v_buf[c, toks].reshape(TOK_SUB * per_tok, lanes) for c in range(2)], axis=1)
            out = jnp.dot(wide, vals, preferred_element_type=F32).astype(BF16).astype(F32)
            o_buf[0, rows, :] = out[:, :lanes]
            o_buf[1, rows, :] = out[:, lanes:]
        for copy in write_out(t):
            copy.start()
        return carry

    lax.fori_loop(0, steps, step, 0)
    attn_ref[...] = jnp.concatenate([o_buf.at[c][pl.ds(h, n_tok, stride=2), :] for h in range(n_heads) for c in range(2)], axis=1).astype(BF16)
    for t in range(steps):
        for copy in write_out(t):
            copy.wait()


class Reducer:
    def __init__(self, part, from_other, chip_sum, far_in, near_in, last_in, send_sems, recv_sems):
        self.part, self.from_other, self.chip_sum = part, from_other, chip_sum
        self.far_in, self.near_in, self.last_in = far_in, near_in, last_in
        self.send_sems, self.recv_sems = send_sems, recv_sems
        self.me, self.core, self.chip, self.other, self.right, self.left = places()
        self.sends = []

    def copy(self, kind, j, cols, way):
        nxt, prv = (self.right, self.left) if way > 0 else (self.left, self.right)
        ahead = lax.rem(self.chip + CHIPS + way, CHIPS)
        behind = lax.rem(self.chip + CHIPS - way, CHIPS)
        opposite = lax.rem(self.chip + 2, CHIPS)
        if kind < 4:
            k = (opposite, behind, ahead, self.chip)[kind]
            src, dst, peer = self.part.at[k, 1 - self.core, :, cols], self.from_other.at[k, :, cols], self.other
        else:
            src, dst, peer = (
                (self.chip_sum.at[opposite, :, cols], self.far_in.at[:, cols], nxt),
                (self.chip_sum.at[behind, :, cols], self.near_in.at[:, cols], prv),
                (self.chip_sum.at[ahead, :, cols], self.last_in.at[:, cols], nxt),
            )[kind - 4]
        return remote(src, dst, self.send_sems.at[kind, j], self.recv_sems.at[kind, j], peer)

    def go(self, kind, j, cols, way):
        copy = self.copy(kind, j, cols, way)
        copy.start()
        self.sends.append(copy)

    def begin(self, j, cols, way):
        for kind in range(4):
            self.go(kind, j, cols, way)

    def pair(self, kind, k, j, cols, way):
        self.copy(kind, j, cols, way).wait_recv()
        return self.part[k, self.core, :, cols].astype(F32) + self.from_other[k, :, cols].astype(F32)

    def far(self, j, cols, way):
        opposite = lax.rem(self.chip + 2, CHIPS)
        self.chip_sum[opposite, :, cols] = self.pair(0, opposite, j, cols, way).astype(BF16)
        self.go(4, j, cols, way)

    def near(self, j, cols, way):
        behind = lax.rem(self.chip + CHIPS - way, CHIPS)
        self.chip_sum[behind, :, cols] = self.pair(1, behind, j, cols, way).astype(BF16)
        self.go(5, j, cols, way)

    def third(self, j, cols, way):
        ahead = lax.rem(self.chip + CHIPS + way, CHIPS)
        mine = self.pair(2, ahead, j, cols, way)
        self.copy(4, j, cols, way).wait_recv()
        self.chip_sum[ahead, :, cols] = (mine + self.far_in[:, cols].astype(F32)).astype(BF16)
        self.go(6, j, cols, way)

    def last(self, j, cols, way):
        own = self.pair(3, self.chip, j, cols, way)
        self.copy(5, j, cols, way).wait_recv()
        own = own + self.near_in[:, cols].astype(F32)
        self.copy(6, j, cols, way).wait_recv()
        return own + self.last_in[:, cols].astype(F32)

    def finish(self):
        for copy in self.sends:
            copy.wait_send()


def mlp_kernel(attn_ref, x_buf, gain_ref, wo_ref, w1_hbm, w3_hbm, w2_hbm, out_ref,
               part, other_in, chip_sum, far_in, near_in, last_in,
               x1_buf, h_buf, act_buf, w1_buf, w3_buf, w2_buf,
               w_sems, rs1_send, rs1_recv, ag_send, ag_recv, rs2_send, rs2_recv):
    me, core, chip, other, right, left = places()
    knock(other, right, left)
    width = x_buf.shape[1]
    n_tok = act_buf.shape[0]
    n_chunks = w1_buf.shape[0]
    chunk = w1_buf.shape[2]

    def weight(kind, i):
        src = (w1_hbm, w3_hbm, w2_hbm)[kind]
        dst = (w1_buf, w3_buf, w2_buf)[kind]
        return pltpu.make_async_copy(src.at[0, :, pl.ds(pl.multiple_of(i * chunk, 128), chunk)], dst.at[i], w_sems.at[kind, i])

    for i in range(n_chunks):
        weight(0, i).start()
        weight(1, i).start()
    for i in range(n_chunks):
        weight(2, i).start()

    def plan(pieces):
        size = width // pieces
        return [(j, pl.ds(j * size, size), 1 if j % 2 == 0 else -1) for j in range(pieces)]

    def put_part(cols, value):
        part[:, :, :, cols] = value.astype(BF16).reshape(CHIPS, 2, n_tok // (2 * CHIPS), value.shape[1])

    plan1 = plan(RS1_PIECES)
    rs1 = Reducer(part, other_in, chip_sum, far_in, near_in, last_in, rs1_send, rs1_recv)
    attn = attn_ref[...]
    for item in plan1:
        put_part(item[1], jnp.dot(attn, wo_ref[0, :, item[1]], preferred_element_type=F32))
        if item[0] == 0:
            enter()
        rs1.begin(*item)
    for stage in (rs1.far, rs1.near, rs1.third):
        for item in plan1:
            stage(*item)
    for item in plan1:
        cols = item[1]
        x1_buf[:, cols] = (x_buf[:, cols].astype(F32) + rs1.last(*item)).astype(BF16)
    rs1.finish()
    h_buf[me] = norm_rows(x1_buf[...].astype(F32), gain_ref[...].astype(F32))
    gather_rows(h_buf, ag_send, ag_recv)

    def gate_up(i, carry):
        weight(0, i).wait()
        weight(1, i).wait()
        h_all = h_buf[...].reshape(n_tok, width)
        gate = jnp.dot(h_all, w1_buf[i], preferred_element_type=F32)
        up = jnp.dot(h_all, w3_buf[i], preferred_element_type=F32)
        act_buf[:, pl.ds(pl.multiple_of(i * chunk, 128), chunk)] = (gate * jax.nn.sigmoid(gate) * up).astype(BF16)
        return carry

    lax.fori_loop(0, n_chunks, gate_up, 0)

    rs2 = Reducer(part, other_in, chip_sum, far_in, near_in, last_in, rs2_send, rs2_recv)
    plan2 = plan(n_chunks)
    for j in range(n_chunks + RS2_LAG):
        if j < n_chunks:
            weight(2, j).wait()
            put_part(plan2[j][1], jnp.dot(act_buf[...], w2_buf[j], preferred_element_type=F32))
            rs2.begin(*plan2[j])
        if j >= RS2_LAG:
            rs2.far(*plan2[j - RS2_LAG])
            rs2.near(*plan2[j - RS2_LAG])
    for item in plan2:
        rs2.third(*item)
    for item in plan2:
        cols = item[1]
        out_ref[:, cols] = (x1_buf[:, cols].astype(F32) + rs2.last(*item)).astype(BF16)
    rs2.finish()


def shape(dims, dtype=BF16):
    return jax.ShapeDtypeStruct(dims, dtype)


def run_qkv(x, gain, pos2, wq, wk, wv, k_cache, v_cache):
    _, n_tok, n_rows, n_heads, head = k_cache.shape
    rows, width = x.shape
    cols = wq.shape[2]
    blocks = n_tok // rows
    dma = pltpu.SemaphoreType.DMA
    args = (x, gain, pos2, wq, wk, wv, k_cache, v_cache)
    return pl.pallas_call(
        qkv_kernel,
        out_shape=[shape((n_tok, cols))] * 3 + [shape((2, n_tok, n_rows, n_heads, LANES))] * 2,
        in_specs=[HBM] * len(args),
        out_specs=[VMEM] * 5,
        scratch_shapes=[
            pltpu.VMEM((rows, width), BF16), pltpu.VMEM(gain.shape, BF16), pltpu.VMEM(pos2.shape, pos2.dtype),
            pltpu.VMEM((blocks, rows, width), BF16), pltpu.VMEM((3, width, cols), BF16),
            dma((6,)), dma((2, 2, 2)), dma((GATHER_SEMS,)), dma((GATHER_SEMS,))],
        compiler_params=pltpu.CompilerParams(collective_id=0, has_side_effects=True, vmem_limit_bytes=36 << 20),
        name='gather_qkv',
    )(*(pltpu.with_memory_space_constraint(a, pltpu.HBM) for a in args))


def run_attn(pos2, q, k, v, k_tiles, v_tiles, k_cache, v_cache):
    _, n_tok, n_rows, n_heads, head = k_cache.shape
    steps = n_tok // TOK_STEP
    dma = pltpu.SemaphoreType.DMA
    wide = pltpu.VMEM((2, n_tok * n_heads, LANES), F32)
    k_tiles, v_tiles = (a.reshape(2, n_tok, n_rows * n_heads, LANES) for a in (k_tiles, v_tiles))
    tiles = shape(k_tiles.shape)
    attn, _, _, k_out, v_out = pl.pallas_call(
        attn_kernel,
        out_shape=[shape(q.shape), tiles, tiles, shape(k_cache.shape), shape(v_cache.shape)],
        in_specs=[SMEM, VMEM, VMEM, VMEM, VMEM, VMEM, VMEM],
        out_specs=[VMEM, VMEM, VMEM, HBM, HBM],
        scratch_shapes=[
            pltpu.VMEM((2, n_heads, 2, n_tok, LANES), F32), wide, wide, pltpu.VMEM((n_tok * n_heads, n_tok), F32),
            dma((2, steps, 2))],
        input_output_aliases={5: 1, 6: 2},
        compiler_params=pltpu.CompilerParams(vmem_limit_bytes=24 << 20),
        name='attention',
    )(pos2, pos2, q, k, v, k_tiles, v_tiles)
    return attn, k_out, v_out


def run_mlp(attn, x, gain, wo, w1, w3, w2):
    rows, width = x.shape
    n_tok = attn.shape[0]
    ffn = w1.shape[2]
    chunk = MLP_CHUNK
    n_chunks = ffn // chunk
    dma = pltpu.SemaphoreType.DMA
    block = pltpu.VMEM((rows, width), BF16)
    chips = pltpu.VMEM((CHIPS, rows, width), BF16)
    return pl.pallas_call(
        mlp_kernel,
        out_shape=shape((rows, width)),
        in_specs=[VMEM, VMEM, VMEM, VMEM, HBM, HBM, HBM],
        out_specs=VMEM,
        scratch_shapes=[
            pltpu.VMEM((CHIPS, 2, rows, width), BF16), chips, chips, block, block, block,
            block, pltpu.VMEM((n_tok // rows, rows, width), BF16), pltpu.VMEM((n_tok, ffn), BF16),
            pltpu.VMEM((n_chunks, width, chunk), BF16), pltpu.VMEM((n_chunks, width, chunk), BF16), pltpu.VMEM((width // chunk, ffn, chunk), BF16),
            dma((3, n_chunks)), dma((7, RS1_PIECES)), dma((7, RS1_PIECES)), dma((GATHER_SEMS,)), dma((GATHER_SEMS,)),
            dma((7, n_chunks)), dma((7, n_chunks))],
        compiler_params=pltpu.CompilerParams(collective_id=1, has_side_effects=True, vmem_limit_bytes=MLP_VMEM),
        name='reduce_mlp',
    )(*(pltpu.with_memory_space_constraint(a, pltpu.VMEM) for a in (attn, x, gain, wo)), w1, w3, w2)


def solution(mesh):
    row_spec = P(('data', 'model'), None)
    cache_spec = P(None, 'data', None, 'model', None)
    col_spec = P(None, None, 'model')
    inner_spec = P(None, 'model', None)
    in_specs = (row_spec, P('data'), P(), P(), col_spec, col_spec, col_spec, inner_spec, col_spec, col_spec, inner_spec, cache_spec, cache_spec)
    out_specs = (row_spec, cache_spec, cache_spec)

    def device_step(hidden, positions, attn_gain, mlp_gain, w_query, w_key, w_value, w_out, w_gate, w_up, w_down, k_cache, v_cache):
        n_tok = positions.shape[0]
        pos2 = positions.reshape(1, n_tok)
        q, k, v, k_tiles, v_tiles = run_qkv(hidden, attn_gain, pos2, w_query, w_key, w_value, k_cache, v_cache)
        attn, k_out, v_out = run_attn(pos2, q, k, v, k_tiles, v_tiles, k_cache, v_cache)
        out = run_mlp(attn, hidden, mlp_gain, w_out, w_gate, w_up, w_down)
        return out, k_out, v_out

    return jax.shard_map(device_step, mesh=mesh, in_specs=in_specs, out_specs=out_specs, check_vma=False)
```

```python
import functools
import math
import jax
import jax.numpy as jnp
from jax import lax
from jax.experimental import pallas as pl
from jax.experimental.pallas import tpu as pltpu
from jax.sharding import PartitionSpec as P

NORM_EPS = 1e-5
ROPE_BASE = 10000.0
BF16 = jnp.bfloat16
F32 = jnp.float32
VMEM = pl.BlockSpec(memory_space=pltpu.VMEM)
SMEM = pl.BlockSpec(memory_space=pltpu.SMEM)
HBM = pl.BlockSpec(memory_space=pltpu.HBM)
MLP_VMEM = 63400000
CHIPS = 4
MLP_CHUNK = 512
RS1_PIECES = 4
RS2_LAG = 3
GATHER_SEMS = 21


def places():
    me = lax.axis_index('model')
    core = lax.rem(me, 2)
    chip = lax.div(me, 2)
    other = me + 1 - 2 * core
    right = lax.rem(chip + 1, CHIPS) * 2 + core
    left = lax.rem(chip + CHIPS - 1, CHIPS) * 2 + core
    return me, core, chip, other, right, left


def knock(other, right, left):
    barrier = pltpu.get_barrier_semaphore()
    for peer in (other, right, left):
        pl.semaphore_signal(barrier, inc=1, device_id={'model': peer})


def enter():
    pl.semaphore_wait(pltpu.get_barrier_semaphore(), 3)


def remote(src, dst, send_sem, recv_sem, peer):
    return pltpu.make_async_remote_copy(src_ref=src, dst_ref=dst, send_sem=send_sem, recv_sem=recv_sem, device_id={'model': peer})


def norm_rows(x_f, gain_f):
    inv_rms = lax.rsqrt(jnp.mean(x_f * x_f, axis=-1, keepdims=True) + NORM_EPS)
    return (x_f * inv_rms * gain_f).astype(BF16)


def gather_rows(buf, send_sems, recv_sems):
    me, core, chip, other, right, left = places()
    width = buf.shape[2]
    quarter = width // 4
    q0, q1, q2, q3 = (pl.ds(i * quarter, quarter) for i in range(4))
    lo, hi, full = pl.ds(0, 2 * quarter), pl.ds(2 * quarter, 2 * quarter), pl.ds(0, width)
    far = lax.rem(chip + 2, CHIPS) * 2 + core
    sends = []

    def hop(blk, cols, idx, peer):
        view = buf.at[blk, :, cols]
        return remote(view, view, send_sems.at[idx], recv_sems.at[idx], peer)

    def arrive(blk, cols, idx):
        hop(blk, cols, idx, other).wait_recv()

    def send(blk, cols, idx, peer):
        copy = hop(blk, cols, idx, peer)
        copy.start()
        sends.append(copy)

    for cols, idx, peer in ((q0, 0, right), (q2, 1, left), (q1, 2, right), (q3, 3, left), (hi, 4, right), (lo, 5, left), (full, 6, other)):
        send(me, cols, idx, peer)
    across = []
    for blk, cols, idx, onward, peer in (
            (left, q0, 0, 7, right), (right, q2, 1, 8, left), (left, q1, 2, 9, right), (right, q3, 3, 10, left),
            (left, hi, 4, None, None), (right, lo, 5, None, None),
            (far, q0, 7, None, None), (far, q2, 8, None, None), (far, q1, 9, None, None), (far, q3, 10, None, None)):
        arrive(blk, cols, idx)
        if onward is not None:
            send(blk, cols, onward, peer)
        send(blk, cols, 11 + len(across), other)
        across.append((blk + 1 - 2 * core, cols, 11 + len(across)))
    arrive(other, full, 6)
    for item in across:
        arrive(*item)
    for copy in sends:
        copy.wait_send()


LANES = 128


def qkv_kernel(x_hbm, gain_hbm, pos_hbm, wq_hbm, wk_hbm, wv_hbm, kc_hbm, vc_hbm, q_ref, k_ref, v_ref, kb_ref, vb_ref,
               x_buf, gain_ref, pos_ref, h_buf, w_buf, load_sems, cache_sems, send_sems, recv_sems):
    me, core, chip, other, right, left = places()
    knock(other, right, left)
    loads = [pltpu.make_async_copy(src, dst, load_sems.at[3 + i]) for i, (src, dst) in enumerate(((x_hbm, x_buf), (gain_hbm, gain_ref), (pos_hbm, pos_ref)))]
    w_copies = [pltpu.make_async_copy(w.at[0], w_buf.at[i], load_sems.at[i]) for i, w in enumerate((wq_hbm, wk_hbm, wv_hbm))]
    pieces = cache_sems.shape[1]
    piece = kb_ref.shape[0] // pieces
    cache_in = []
    for kv, (hbm, buf) in enumerate(((kc_hbm, kb_ref), (vc_hbm, vb_ref))):
        for p in range(pieces):
            toks = pl.ds(p * piece, piece)
            cache_in.append(pltpu.make_async_copy(hbm.at[toks], buf.at[toks], cache_sems.at[kv, p]))
    for copy in loads + w_copies + cache_in:
        copy.start()
    for copy in loads:
        copy.wait()
    h_buf[me] = norm_rows(x_buf[...].astype(F32), gain_ref[...].astype(F32))
    enter()
    gather_rows(h_buf, send_sems, recv_sems)

    n_tok = pos_ref.shape[1]
    half = 128
    head = 2 * half
    pos_row = jnp.broadcast_to(pos_ref[...].astype(F32), (n_tok, n_tok))
    diag = lax.broadcasted_iota(jnp.int32, (n_tok, n_tok), 0) == lax.broadcasted_iota(jnp.int32, (n_tok, n_tok), 1)
    pos_col = jnp.sum(jnp.where(diag, pos_row, 0.0), axis=1, keepdims=True)
    lane = lax.broadcasted_iota(jnp.int32, (n_tok, half), 1).astype(F32)
    angles = pos_col * jnp.exp(lane * (-2.0 * math.log(ROPE_BASE) / head))
    cos_tab, sin_tab = jnp.cos(angles), jnp.sin(angles)
    h_all = h_buf[...].reshape(n_tok, h_buf.shape[2])
    for i, out_ref in enumerate((q_ref, k_ref, v_ref)):
        w_copies[i].wait()
        proj = jnp.dot(h_all, w_buf[i], preferred_element_type=F32).astype(BF16)
        if i == 2:
            out_ref[...] = proj
            continue
        for h0 in range(0, proj.shape[1], head):
            front = proj[:, h0:h0 + half].astype(F32)
            back = proj[:, h0 + half:h0 + head].astype(F32)
            out_ref[:, h0:h0 + half] = (front * cos_tab - back * sin_tab).astype(BF16)
            out_ref[:, h0 + half:h0 + head] = (back * cos_tab + front * sin_tab).astype(BF16)
    for copy in cache_in:
        copy.wait()


TOK_STEP = 16
TOK_SUB = 8


def attn_kernel(pos_smem, pos_ref, q_ref, k_ref, v_ref, kb_in, vb_in, attn_ref, k_buf, v_buf, ko_hbm, vo_hbm,
                new_buf, q_buf, o_buf, pc_buf, out_sems):
    n_tok, per_tok, lanes = k_buf.shape
    n_heads = 2
    head = q_ref.shape[1] // n_heads
    steps = n_tok // TOK_STEP
    bufs = (k_buf, v_buf)

    def write_out(t):
        toks = pl.ds(t * TOK_STEP, TOK_STEP)
        return [pltpu.make_async_copy(buf.at[toks], hbm.at[toks], out_sems.at[kv, t]) for kv, (buf, hbm) in enumerate(zip(bufs, (ko_hbm, vo_hbm)))]

    for h in range(n_heads):
        for c in range(2):
            cols = slice(h * head + c * lanes, h * head + (c + 1) * lanes)
            q_buf.at[c][pl.ds(h, n_tok, stride=2), :] = q_ref[:, cols].astype(F32)
            for kv, ref in enumerate((k_ref, v_ref)):
                new = ref[:, cols].astype(F32)
                for again in range(2):
                    new_buf.at[kv][pl.ds(4 * again + 2 * c + h, n_tok, stride=8), :] = new
    rows2 = n_tok * n_heads
    pos_row = jnp.broadcast_to(pos_ref[...].astype(F32), (rows2, n_tok))
    own = lax.broadcasted_iota(jnp.int32, (rows2, n_tok), 0) // 2 == lax.broadcasted_iota(jnp.int32, (rows2, n_tok), 1)
    pc_buf[...] = jnp.broadcast_to(jnp.sum(jnp.where(own, pos_row, 0.0), axis=1, keepdims=True), (rows2, n_tok))

    tile_row = lax.broadcasted_iota(jnp.int32, (16, lanes), 0)
    sub = TOK_SUB * n_heads
    tok_of = (lax.broadcasted_iota(jnp.int32, (4 * sub, per_tok), 0) % sub) // 2
    row = lax.broadcasted_iota(jnp.int32, (2 * sub, per_tok), 0)
    col = lax.broadcasted_iota(jnp.int32, (2 * sub, per_tok), 1)
    counts = ((col & 2) == 0) & ((col & 1) == (row & 1))
    key_pos = (col >> 2).astype(F32)

    def shift(x, by):
        return jnp.concatenate([pltpu.roll(x[:, i:i + lanes], by % lanes, 1) for i in range(0, per_tok, lanes)], axis=1)

    def step(t, carry):
        b0 = t * TOK_STEP
        for i in range(TOK_STEP):
            b = b0 + i
            pos = pos_smem[0, b]
            tile = pl.ds(pl.multiple_of((pos >> 2) * 16, 16), 16)
            hit = (tile_row >> 2) == (pos & 3)
            for kv in range(2):
                new = new_buf[kv, pl.ds(pl.multiple_of(b * 8, 8), 8), :]
                old = bufs[kv][b, tile, :].astype(F32)
                bufs[kv][b, tile, :] = jnp.where(hit, jnp.concatenate([new, new], axis=0), old).astype(BF16)

        def pair(buf):
            return jnp.concatenate([buf[pl.ds(b0 + g * TOK_SUB, TOK_SUB)].reshape(TOK_SUB * per_tok, lanes) for g in range(2)], axis=1)

        rows = [pl.ds(pl.multiple_of(b0 * n_heads + g * sub, sub), sub) for g in range(2)]
        none = jnp.zeros((sub, lanes), F32)
        q = jnp.concatenate(
            [jnp.concatenate([q_buf[c, rows[0], :], none], axis=1) for c in range(2)] +
            [jnp.concatenate([none, q_buf[c, rows[1], :]], axis=1) for c in range(2)], axis=0).astype(BF16)
        scores = lax.dot_general(q, pair(k_buf), (((1,), (1,)), ((), ())), preferred_element_type=F32)
        mine = scores[:, :per_tok]
        for m in range(1, TOK_SUB):
            mine = jnp.where(tok_of == m, scores[:, m * per_tok:(m + 1) * per_tok], mine)
        first = jnp.concatenate([mine[:sub], mine[2 * sub:3 * sub]], axis=0)
        second = jnp.concatenate([mine[sub:2 * sub], mine[3 * sub:]], axis=0)
        total = (first + shift(second, -2)) * (head ** -0.5)
        pos_of = pc_buf[pl.ds(pl.multiple_of(b0 * n_heads, 2 * sub), 2 * sub), :]
        total = jnp.where(counts & (key_pos <= jnp.concatenate([pos_of] * (per_tok // lanes), axis=1)), total, -1e30)
        e = jnp.exp(total - jnp.max(total, axis=1, keepdims=True))
        probs = (e / jnp.sum(e, axis=1, keepdims=True)).astype(BF16).astype(F32)
        moved = shift(probs, 2)
        probs = jnp.concatenate([probs[:sub], moved[:sub], probs[sub:], moved[sub:]], axis=0)
        wide = jnp.concatenate([jnp.where(tok_of == m, probs, 0.0) for m in range(TOK_SUB)], axis=1).astype(BF16)
        out = jnp.dot(wide, pair(v_buf), preferred_element_type=F32).astype(BF16).astype(F32)
        for g in range(2):
            for c in range(2):
                at = (2 * g + c) * sub
                o_buf[c, rows[g], :] = out[at:at + sub, g * lanes:(g + 1) * lanes]
        for copy in write_out(t):
            copy.start()
        return carry

    lax.fori_loop(0, steps, step, 0)
    attn_ref[...] = jnp.concatenate([o_buf.at[c][pl.ds(h, n_tok, stride=2), :] for h in range(n_heads) for c in range(2)], axis=1).astype(BF16)
    for t in range(steps):
        for copy in write_out(t):
            copy.wait()


class Reducer:
    def __init__(self, part, from_other, chip_sum, far_in, near_in, last_in, send_sems, recv_sems):
        self.part, self.from_other, self.chip_sum = part, from_other, chip_sum
        self.far_in, self.near_in, self.last_in = far_in, near_in, last_in
        self.send_sems, self.recv_sems = send_sems, recv_sems
        self.me, self.core, self.chip, self.other, self.right, self.left = places()
        self.sends = []

    def copy(self, kind, j, cols, way):
        nxt, prv = (self.right, self.left) if way > 0 else (self.left, self.right)
        ahead = lax.rem(self.chip + CHIPS + way, CHIPS)
        behind = lax.rem(self.chip + CHIPS - way, CHIPS)
        opposite = lax.rem(self.chip + 2, CHIPS)
        if kind < 4:
            k = (opposite, behind, ahead, self.chip)[kind]
            src, dst, peer = self.part.at[k, 1 - self.core, :, cols], self.from_other.at[k, :, cols], self.other
        else:
            src, dst, peer = (
                (self.chip_sum.at[opposite, :, cols], self.far_in.at[:, cols], nxt),
                (self.chip_sum.at[behind, :, cols], self.near_in.at[:, cols], prv),
                (self.chip_sum.at[ahead, :, cols], self.last_in.at[:, cols], nxt),
            )[kind - 4]
        return remote(src, dst, self.send_sems.at[kind, j], self.recv_sems.at[kind, j], peer)

    def go(self, kind, j, cols, way):
        copy = self.copy(kind, j, cols, way)
        copy.start()
        self.sends.append(copy)

    def begin(self, j, cols, way):
        for kind in range(4):
            self.go(kind, j, cols, way)

    def pair(self, kind, k, j, cols, way):
        self.copy(kind, j, cols, way).wait_recv()
        return self.part[k, self.core, :, cols].astype(F32) + self.from_other[k, :, cols].astype(F32)

    def far(self, j, cols, way):
        opposite = lax.rem(self.chip + 2, CHIPS)
        self.chip_sum[opposite, :, cols] = self.pair(0, opposite, j, cols, way).astype(BF16)
        self.go(4, j, cols, way)

    def near(self, j, cols, way):
        behind = lax.rem(self.chip + CHIPS - way, CHIPS)
        self.chip_sum[behind, :, cols] = self.pair(1, behind, j, cols, way).astype(BF16)
        self.go(5, j, cols, way)

    def third(self, j, cols, way):
        ahead = lax.rem(self.chip + CHIPS + way, CHIPS)
        mine = self.pair(2, ahead, j, cols, way)
        self.copy(4, j, cols, way).wait_recv()
        self.chip_sum[ahead, :, cols] = (mine + self.far_in[:, cols].astype(F32)).astype(BF16)
        self.go(6, j, cols, way)

    def last(self, j, cols, way):
        own = self.pair(3, self.chip, j, cols, way)
        self.copy(5, j, cols, way).wait_recv()
        own = own + self.near_in[:, cols].astype(F32)
        self.copy(6, j, cols, way).wait_recv()
        return own + self.last_in[:, cols].astype(F32)

    def finish(self):
        for copy in self.sends:
            copy.wait_send()


def mlp_kernel(attn_ref, x_buf, gain_ref, wo_ref, w1_hbm, w3_hbm, w2_hbm, out_ref,
               part, other_in, chip_sum, far_in, near_in, last_in,
               x1_buf, h_buf, act_buf, w1_buf, w3_buf, w2_buf,
               w_sems, rs1_send, rs1_recv, ag_send, ag_recv, rs2_send, rs2_recv):
    me, core, chip, other, right, left = places()
    knock(other, right, left)
    width = x_buf.shape[1]
    n_tok = act_buf.shape[0]
    n_chunks = w1_buf.shape[0]
    chunk = w1_buf.shape[2]

    def weight(kind, i):
        src = (w1_hbm, w3_hbm, w2_hbm)[kind]
        dst = (w1_buf, w3_buf, w2_buf)[kind]
        return pltpu.make_async_copy(src.at[0, :, pl.ds(pl.multiple_of(i * chunk, 128), chunk)], dst.at[i], w_sems.at[kind, i])

    for i in range(n_chunks):
        weight(0, i).start()
        weight(1, i).start()
    for i in range(n_chunks):
        weight(2, i).start()

    def plan(pieces):
        size = width // pieces
        return [(j, pl.ds(j * size, size), 1 if j % 2 == 0 else -1) for j in range(pieces)]

    def put_part(cols, value):
        part[:, :, :, cols] = value.astype(BF16).reshape(CHIPS, 2, n_tok // (2 * CHIPS), value.shape[1])

    plan1 = plan(RS1_PIECES)
    rs1 = Reducer(part, other_in, chip_sum, far_in, near_in, last_in, rs1_send, rs1_recv)
    attn = attn_ref[...]
    for item in plan1:
        put_part(item[1], jnp.dot(attn, wo_ref[0, :, item[1]], preferred_element_type=F32))
        if item[0] == 0:
            enter()
        rs1.begin(*item)
    for stage in (rs1.far, rs1.near, rs1.third):
        for item in plan1:
            stage(*item)
    for item in plan1:
        cols = item[1]
        x1_buf[:, cols] = (x_buf[:, cols].astype(F32) + rs1.last(*item)).astype(BF16)
    rs1.finish()
    h_buf[me] = norm_rows(x1_buf[...].astype(F32), gain_ref[...].astype(F32))
    gather_rows(h_buf, ag_send, ag_recv)

    def gate_up(i, carry):
        weight(0, i).wait()
        weight(1, i).wait()
        h_all = h_buf[...].reshape(n_tok, width)
        gate = jnp.dot(h_all, w1_buf[i], preferred_element_type=F32)
        up = jnp.dot(h_all, w3_buf[i], preferred_element_type=F32)
        act_buf[:, pl.ds(pl.multiple_of(i * chunk, 128), chunk)] = (gate * jax.nn.sigmoid(gate) * up).astype(BF16)
        return carry

    lax.fori_loop(0, n_chunks, gate_up, 0)

    rs2 = Reducer(part, other_in, chip_sum, far_in, near_in, last_in, rs2_send, rs2_recv)
    plan2 = plan(n_chunks)
    for j in range(n_chunks + RS2_LAG):
        if j < n_chunks:
            weight(2, j).wait()
            put_part(plan2[j][1], jnp.dot(act_buf[...], w2_buf[j], preferred_element_type=F32))
            rs2.begin(*plan2[j])
        if j >= RS2_LAG:
            rs2.far(*plan2[j - RS2_LAG])
            rs2.near(*plan2[j - RS2_LAG])
    for item in plan2:
        rs2.third(*item)
    for item in plan2:
        cols = item[1]
        out_ref[:, cols] = (x1_buf[:, cols].astype(F32) + rs2.last(*item)).astype(BF16)
    rs2.finish()


def shape(dims, dtype=BF16):
    return jax.ShapeDtypeStruct(dims, dtype)


def to_tiles(cache):
    _, n_tok, n_rows, n_heads, head = cache.shape
    halves = head // LANES
    return cache.reshape(n_tok, n_rows, n_heads, halves, LANES).transpose(0, 1, 3, 2, 4).reshape(n_tok, n_rows * halves * n_heads, LANES)


def from_tiles(tiles, like):
    _, n_tok, n_rows, n_heads, head = like.shape
    halves = head // LANES
    return tiles.reshape(n_tok, n_rows, halves, n_heads, LANES).transpose(0, 1, 3, 2, 4).reshape(like.shape)


def run_qkv(x, gain, pos2, wq, wk, wv, k_tiles, v_tiles):
    n_tok = k_tiles.shape[0]
    rows, width = x.shape
    cols = wq.shape[2]
    blocks = n_tok // rows
    dma = pltpu.SemaphoreType.DMA
    args = (x, gain, pos2, wq, wk, wv, k_tiles, v_tiles)
    return pl.pallas_call(
        qkv_kernel,
        out_shape=[shape((n_tok, cols))] * 3 + [shape(k_tiles.shape)] * 2,
        in_specs=[HBM] * len(args),
        out_specs=[VMEM] * 5,
        scratch_shapes=[
            pltpu.VMEM((rows, width), BF16), pltpu.VMEM(gain.shape, BF16), pltpu.VMEM(pos2.shape, pos2.dtype),
            pltpu.VMEM((blocks, rows, width), BF16), pltpu.VMEM((3, width, cols), BF16),
            dma((6,)), dma((2, 4)), dma((GATHER_SEMS,)), dma((GATHER_SEMS,))],
        compiler_params=pltpu.CompilerParams(collective_id=0, has_side_effects=True, vmem_limit_bytes=36 << 20),
        name='gather_qkv',
    )(*(pltpu.with_memory_space_constraint(a, pltpu.HBM) for a in args))


def run_attn(pos2, q, k, v, k_tiles, v_tiles):
    n_tok = k_tiles.shape[0]
    rows2 = q.shape[1] // (2 * LANES) * n_tok
    dma = pltpu.SemaphoreType.DMA
    wide = pltpu.VMEM((2, rows2, LANES), F32)
    tiles = shape(k_tiles.shape)
    attn, _, _, k_out, v_out = pl.pallas_call(
        attn_kernel,
        out_shape=[shape(q.shape), tiles, tiles, tiles, tiles],
        in_specs=[SMEM, VMEM, VMEM, VMEM, VMEM, VMEM, VMEM],
        out_specs=[VMEM, VMEM, VMEM, HBM, HBM],
        scratch_shapes=[
            pltpu.VMEM((2, n_tok * 8, LANES), F32), wide, wide, pltpu.VMEM((rows2, n_tok), F32),
            dma((2, n_tok // TOK_STEP))],
        input_output_aliases={5: 1, 6: 2},
        compiler_params=pltpu.CompilerParams(vmem_limit_bytes=24 << 20),
        name='attention',
    )(pos2, pos2, q, k, v, k_tiles, v_tiles)
    return attn, k_out, v_out


def run_mlp(attn, x, gain, wo, w1, w3, w2):
    rows, width = x.shape
    n_tok = attn.shape[0]
    ffn = w1.shape[2]
    chunk = MLP_CHUNK
    n_chunks = ffn // chunk
    dma = pltpu.SemaphoreType.DMA
    block = pltpu.VMEM((rows, width), BF16)
    chips = pltpu.VMEM((CHIPS, rows, width), BF16)
    return pl.pallas_call(
        mlp_kernel,
        out_shape=shape((rows, width)),
        in_specs=[VMEM, VMEM, VMEM, VMEM, HBM, HBM, HBM],
        out_specs=VMEM,
        scratch_shapes=[
            pltpu.VMEM((CHIPS, 2, rows, width), BF16), chips, chips, block, block, block,
            block, pltpu.VMEM((n_tok // rows, rows, width), BF16), pltpu.VMEM((n_tok, ffn), BF16),
            pltpu.VMEM((n_chunks, width, chunk), BF16), pltpu.VMEM((n_chunks, width, chunk), BF16), pltpu.VMEM((width // chunk, ffn, chunk), BF16),
            dma((3, n_chunks)), dma((7, RS1_PIECES)), dma((7, RS1_PIECES)), dma((GATHER_SEMS,)), dma((GATHER_SEMS,)),
            dma((7, n_chunks)), dma((7, n_chunks))],
        compiler_params=pltpu.CompilerParams(collective_id=1, has_side_effects=True, vmem_limit_bytes=MLP_VMEM),
        name='reduce_mlp',
    )(*(pltpu.with_memory_space_constraint(a, pltpu.VMEM) for a in (attn, x, gain, wo)), w1, w3, w2)


def solution(mesh):
    row_spec = P(('data', 'model'), None)
    cache_spec = P(None, 'data', None, 'model', None)
    col_spec = P(None, None, 'model')
    inner_spec = P(None, 'model', None)
    in_specs = (row_spec, P('data'), P(), P(), col_spec, col_spec, col_spec, inner_spec, col_spec, col_spec, inner_spec, cache_spec, cache_spec)
    out_specs = (row_spec, cache_spec, cache_spec)

    def device_step(hidden, positions, attn_gain, mlp_gain, w_query, w_key, w_value, w_out, w_gate, w_up, w_down, k_cache, v_cache):
        n_tok = positions.shape[0]
        pos2 = positions.reshape(1, n_tok)
        q, k, v, k_tiles, v_tiles = run_qkv(hidden, attn_gain, pos2, w_query, w_key, w_value, to_tiles(k_cache), to_tiles(v_cache))
        attn, k_out, v_out = run_attn(pos2, q, k, v, k_tiles, v_tiles)
        out = run_mlp(attn, hidden, mlp_gain, w_out, w_gate, w_up, w_down)
        return out, from_tiles(k_out, k_cache), from_tiles(v_out, v_cache)

    return jax.shard_map(device_step, mesh=mesh, in_specs=in_specs, out_specs=out_specs, check_vma=False)
```

```python
import functools
import math
import jax
import jax.numpy as jnp
from jax import lax
from jax.experimental import pallas as pl
from jax.experimental.pallas import tpu as pltpu
from jax.sharding import PartitionSpec as P

NORM_EPS = 1e-5
ROPE_BASE = 10000.0
BF16 = jnp.bfloat16
F32 = jnp.float32
VMEM = pl.BlockSpec(memory_space=pltpu.VMEM)
SMEM = pl.BlockSpec(memory_space=pltpu.SMEM)
HBM = pl.BlockSpec(memory_space=pltpu.HBM)
MLP_VMEM = 63400000
CHIPS = 4
MLP_CHUNK = 512
RS1_PIECES = 4
RS2_LAG = 3
RS2_STRAIGHT = 2
GATHER_SEMS = 21


def places():
    me = lax.axis_index('model')
    core = lax.rem(me, 2)
    chip = lax.div(me, 2)
    other = me + 1 - 2 * core
    right = lax.rem(chip + 1, CHIPS) * 2 + core
    left = lax.rem(chip + CHIPS - 1, CHIPS) * 2 + core
    return me, core, chip, other, right, left


def knock(*peers):
    barrier = pltpu.get_barrier_semaphore()
    for peer in peers:
        pl.semaphore_signal(barrier, inc=1, device_id={'model': peer})


def enter(peers):
    pl.semaphore_wait(pltpu.get_barrier_semaphore(), peers)


def remote(src, dst, send_sem, recv_sem, peer):
    return pltpu.make_async_remote_copy(src_ref=src, dst_ref=dst, send_sem=send_sem, recv_sem=recv_sem, device_id={'model': peer})


def norm_rows(x_f, gain_f):
    inv_rms = lax.rsqrt(jnp.mean(x_f * x_f, axis=-1, keepdims=True) + NORM_EPS)
    return (x_f * inv_rms * gain_f).astype(BF16)


def gather_rows(buf, send_sems, recv_sems):
    me, core, chip, other, right, left = places()
    width = buf.shape[2]
    quarter = width // 4
    q0, q1, q2, q3 = (pl.ds(i * quarter, quarter) for i in range(4))
    lo, hi, full = pl.ds(0, 2 * quarter), pl.ds(2 * quarter, 2 * quarter), pl.ds(0, width)
    far = lax.rem(chip + 2, CHIPS) * 2 + core
    sends = []

    def hop(blk, cols, idx, peer):
        view = buf.at[blk, :, cols]
        return remote(view, view, send_sems.at[idx], recv_sems.at[idx], peer)

    def arrive(blk, cols, idx):
        hop(blk, cols, idx, other).wait_recv()

    def send(blk, cols, idx, peer):
        copy = hop(blk, cols, idx, peer)
        copy.start()
        sends.append(copy)

    for cols, idx, peer in ((q0, 0, right), (q2, 1, left), (q1, 2, right), (q3, 3, left), (hi, 4, right), (lo, 5, left), (full, 6, other)):
        send(me, cols, idx, peer)
    across = []
    for blk, cols, idx, onward, peer in (
            (left, q0, 0, 7, right), (right, q2, 1, 8, left), (left, q1, 2, 9, right), (right, q3, 3, 10, left),
            (left, hi, 4, None, None), (right, lo, 5, None, None),
            (far, q0, 7, None, None), (far, q2, 8, None, None), (far, q1, 9, None, None), (far, q3, 10, None, None)):
        arrive(blk, cols, idx)
        if onward is not None:
            send(blk, cols, onward, peer)
        send(blk, cols, 11 + len(across), other)
        across.append((blk + 1 - 2 * core, cols, 11 + len(across)))
    arrive(other, full, 6)
    for item in across:
        arrive(*item)
    for copy in sends:
        copy.wait_send()


LANES = 128


def qkv_kernel(x_hbm, gain_hbm, pos_hbm, wq_hbm, wk_hbm, wv_hbm, kc_hbm, vc_hbm, q_ref, k_ref, v_ref, kb_ref, vb_ref,
               x_buf, gain_ref, pos_ref, h_buf, w_buf, load_sems, cache_sems, send_sems, recv_sems):
    me, core, chip, other, right, left = places()
    knock(other, right, left)
    loads = [pltpu.make_async_copy(src, dst, load_sems.at[3 + i]) for i, (src, dst) in enumerate(((x_hbm, x_buf), (gain_hbm, gain_ref), (pos_hbm, pos_ref)))]
    w_copies = [pltpu.make_async_copy(w.at[0], w_buf.at[i], load_sems.at[i]) for i, w in enumerate((wq_hbm, wk_hbm, wv_hbm))]
    pieces = cache_sems.shape[1]
    piece = kb_ref.shape[0] // pieces
    cache_in = []
    for kv, (hbm, buf) in enumerate(((kc_hbm, kb_ref), (vc_hbm, vb_ref))):
        for p in range(pieces):
            toks = pl.ds(p * piece, piece)
            cache_in.append(pltpu.make_async_copy(hbm.at[toks], buf.at[toks], cache_sems.at[kv, p]))
    for copy in loads:
        copy.start()
    for copy in w_copies + cache_in:
        copy.start()
    for copy in loads:
        copy.wait()
    h_buf[me] = norm_rows(x_buf[...].astype(F32), gain_ref[...].astype(F32))
    enter(3)
    gather_rows(h_buf, send_sems, recv_sems)

    n_tok = pos_ref.shape[1]
    half = 128
    head = 2 * half
    pos_row = jnp.broadcast_to(pos_ref[...].astype(F32), (n_tok, n_tok))
    diag = lax.broadcasted_iota(jnp.int32, (n_tok, n_tok), 0) == lax.broadcasted_iota(jnp.int32, (n_tok, n_tok), 1)
    pos_col = jnp.sum(jnp.where(diag, pos_row, 0.0), axis=1, keepdims=True)
    lane = lax.broadcasted_iota(jnp.int32, (n_tok, half), 1).astype(F32)
    angles = pos_col * jnp.exp(lane * (-2.0 * math.log(ROPE_BASE) / head))
    cos_tab, sin_tab = jnp.cos(angles), jnp.sin(angles)
    h_all = h_buf[...].reshape(n_tok, h_buf.shape[2])
    for i, out_ref in enumerate((q_ref, k_ref, v_ref)):
        w_copies[i].wait()
        proj = jnp.dot(h_all, w_buf[i], preferred_element_type=F32).astype(BF16)
        if i == 2:
            out_ref[...] = proj
            continue
        for h0 in range(0, proj.shape[1], head):
            front = proj[:, h0:h0 + half].astype(F32)
            back = proj[:, h0 + half:h0 + head].astype(F32)
            out_ref[:, h0:h0 + half] = (front * cos_tab - back * sin_tab).astype(BF16)
            out_ref[:, h0 + half:h0 + head] = (back * cos_tab + front * sin_tab).astype(BF16)
    for copy in cache_in:
        copy.wait()


TOK_STEP = 16
TOK_SUB = 8
TURN = 16


def attn_kernel(pos_smem, pos_ref, q_ref, k_ref, v_ref, kb_in, vb_in, attn_ref, k_buf, v_buf, ko_hbm, vo_hbm,
                new_buf, q_buf, o_buf, pc_buf, out_sems):
    n_tok, per_tok, lanes = k_buf.shape
    n_heads = 2
    head = q_ref.shape[1] // n_heads
    steps = n_tok // TOK_STEP
    bufs = (k_buf, v_buf)

    def write_out(t):
        toks = pl.ds(t * TOK_STEP, TOK_STEP)
        return [pltpu.make_async_copy(buf.at[toks], hbm.at[toks], out_sems.at[kv, t]) for kv, (buf, hbm) in enumerate(zip(bufs, (ko_hbm, vo_hbm)))]

    for h in range(n_heads):
        for c in range(2):
            cols = slice(h * head + c * lanes, h * head + (c + 1) * lanes)
            q_buf.at[c][pl.ds(h, n_tok, stride=2), :] = q_ref[:, cols].astype(F32)
            for kv, ref in enumerate((k_ref, v_ref)):
                new = ref[:, cols].astype(F32)
                for again in range(2):
                    new_buf.at[kv][pl.ds(4 * again + 2 * c + h, n_tok, stride=8), :] = new
    rows2 = n_tok * n_heads
    pos_row = jnp.broadcast_to(pos_ref[...].astype(F32), (rows2, n_tok))
    own = lax.broadcasted_iota(jnp.int32, (rows2, n_tok), 0) // 2 == lax.broadcasted_iota(jnp.int32, (rows2, n_tok), 1)
    pc_buf[...] = jnp.broadcast_to(jnp.sum(jnp.where(own, pos_row, 0.0), axis=1, keepdims=True), (rows2, n_tok))

    tile_row = lax.broadcasted_iota(jnp.int32, (16, lanes), 0)
    sub = TOK_SUB * n_heads
    tok_of = (lax.broadcasted_iota(jnp.int32, (4 * sub, per_tok), 0) % sub) // 2
    row = lax.broadcasted_iota(jnp.int32, (2 * sub, per_tok), 0)
    col = lax.broadcasted_iota(jnp.int32, (2 * sub, per_tok), 1)
    counts = ((col & 2) == 0) & ((col & 1) == (row & 1))
    key_pos = (((col + jnp.where(row >= sub, TURN, 0)) % per_tok) >> 2).astype(F32)

    def shift(x, by):
        return jnp.concatenate([pltpu.roll(x[:, i:i + lanes], by % lanes, 1) for i in range(0, per_tok, lanes)], axis=1)

    def step(t, carry):
        b0 = t * TOK_STEP
        for i in range(TOK_STEP):
            b = b0 + i
            pos = pos_smem[0, b]
            tile = pl.ds(pl.multiple_of((pos >> 2) * 16, 16), 16)
            hit = (tile_row >> 2) == (pos & 3)
            for kv in range(2):
                new = new_buf[kv, pl.ds(pl.multiple_of(b * 8, 8), 8), :]
                old = bufs[kv][b, tile, :].astype(F32)
                bufs[kv][b, tile, :] = jnp.where(hit, jnp.concatenate([new, new], axis=0), old).astype(BF16)

        def pair(buf):
            one, two = (buf[pl.ds(b0 + g * TOK_SUB, TOK_SUB)] for g in range(2))
            two = jnp.concatenate([two[:, TURN:], two[:, :TURN]], axis=1)
            return jnp.concatenate([x.reshape(TOK_SUB * per_tok, lanes) for x in (one, two)], axis=1)

        rows = [pl.ds(pl.multiple_of(b0 * n_heads + g * sub, sub), sub) for g in range(2)]
        none = jnp.zeros((sub, lanes), F32)
        q = jnp.concatenate(
            [jnp.concatenate([q_buf[c, rows[0], :], none], axis=1) for c in range(2)] +
            [jnp.concatenate([none, q_buf[c, rows[1], :]], axis=1) for c in range(2)], axis=0).astype(BF16)
        scores = lax.dot_general(q, pair(k_buf), (((1,), (1,)), ((), ())), preferred_element_type=F32)
        mine = scores[:, :per_tok]
        for m in range(1, TOK_SUB):
            mine = jnp.where(tok_of == m, scores[:, m * per_tok:(m + 1) * per_tok], mine)
        first = jnp.concatenate([mine[:sub], mine[2 * sub:3 * sub]], axis=0)
        second = jnp.concatenate([mine[sub:2 * sub], mine[3 * sub:]], axis=0)
        total = (first + shift(second, -2)) * (head ** -0.5)
        pos_of = pc_buf[pl.ds(pl.multiple_of(b0 * n_heads, 2 * sub), 2 * sub), :]
        total = jnp.where(counts & (key_pos <= jnp.concatenate([pos_of] * (per_tok // lanes), axis=1)), total, -1e30)
        e = jnp.exp(total - jnp.max(total, axis=1, keepdims=True))
        probs = (e / jnp.sum(e, axis=1, keepdims=True)).astype(BF16).astype(F32)
        moved = shift(probs, 2)
        probs = jnp.concatenate([probs[:sub], moved[:sub], probs[sub:], moved[sub:]], axis=0)
        wide = jnp.concatenate([jnp.where(tok_of == m, probs, 0.0) for m in range(TOK_SUB)], axis=1).astype(BF16)
        out = jnp.dot(wide, pair(v_buf), preferred_element_type=F32).astype(BF16).astype(F32)
        for g in range(2):
            for c in range(2):
                at = (2 * g + c) * sub
                o_buf[c, rows[g], :] = out[at:at + sub, g * lanes:(g + 1) * lanes]
        for copy in write_out(t):
            copy.start()
        return carry

    lax.fori_loop(0, steps, step, 0)
    attn_ref[...] = jnp.concatenate([o_buf.at[c][pl.ds(h, n_tok, stride=2), :] for h in range(n_heads) for c in range(2)], axis=1).astype(BF16)
    for t in range(steps):
        for copy in write_out(t):
            copy.wait()


class Reducer:
    def __init__(self, part, from_other, chip_sum, far_in, near_in, last_in, send_sems, recv_sems):
        self.part, self.from_other, self.chip_sum = part, from_other, chip_sum
        self.far_in, self.near_in, self.last_in = far_in, near_in, last_in
        self.send_sems, self.recv_sems = send_sems, recv_sems
        self.me, self.core, self.chip, self.other, self.right, self.left = places()
        self.sends = []

    def copy(self, kind, j, cols, way, direct):
        nxt, prv = (self.right, self.left) if way > 0 else (self.left, self.right)
        ahead = lax.rem(self.chip + CHIPS + way, CHIPS)
        behind = lax.rem(self.chip + CHIPS - way, CHIPS)
        opposite = lax.rem(self.chip + 2, CHIPS)
        if kind < 4:
            k = (opposite, behind, ahead, self.chip)[kind]
            src, dst, peer = self.part.at[k, 1 - self.core, :, cols], self.from_other.at[k, :, cols], self.other
        else:
            src, dst, peer = (
                (self.chip_sum.at[opposite, :, cols], self.far_in.at[:, cols], opposite * 2 + self.core if direct else nxt),
                (self.chip_sum.at[behind, :, cols], self.near_in.at[:, cols], prv),
                (self.chip_sum.at[ahead, :, cols], self.last_in.at[:, cols], nxt),
            )[kind - 4]
        return remote(src, dst, self.send_sems.at[kind, j], self.recv_sems.at[kind, j], peer)

    def go(self, kind, j, cols, way, direct):
        copy = self.copy(kind, j, cols, way, direct)
        copy.start()
        self.sends.append(copy)

    def begin(self, j, cols, way, direct):
        for kind in range(4):
            self.go(kind, j, cols, way, direct)

    def pair(self, kind, k, j, cols, way, direct):
        self.copy(kind, j, cols, way, direct).wait_recv()
        return self.part[k, self.core, :, cols].astype(F32) + self.from_other[k, :, cols].astype(F32)

    def far(self, j, cols, way, direct):
        opposite = lax.rem(self.chip + 2, CHIPS)
        self.chip_sum[opposite, :, cols] = self.pair(0, opposite, j, cols, way, direct).astype(BF16)
        self.go(4, j, cols, way, direct)

    def near(self, j, cols, way, direct):
        behind = lax.rem(self.chip + CHIPS - way, CHIPS)
        self.chip_sum[behind, :, cols] = self.pair(1, behind, j, cols, way, direct).astype(BF16)
        self.go(5, j, cols, way, direct)

    def third(self, j, cols, way, direct):
        ahead = lax.rem(self.chip + CHIPS + way, CHIPS)
        mine = self.pair(2, ahead, j, cols, way, direct)
        if not direct:
            self.copy(4, j, cols, way, direct).wait_recv()
            mine = mine + self.far_in[:, cols].astype(F32)
        self.chip_sum[ahead, :, cols] = mine.astype(BF16)
        self.go(6, j, cols, way, direct)

    def last(self, j, cols, way, direct):
        own = self.pair(3, self.chip, j, cols, way, direct)
        self.copy(5, j, cols, way, direct).wait_recv()
        own = own + self.near_in[:, cols].astype(F32)
        if direct:
            self.copy(4, j, cols, way, direct).wait_recv()
            own = own + self.far_in[:, cols].astype(F32)
        self.copy(6, j, cols, way, direct).wait_recv()
        return own + self.last_in[:, cols].astype(F32)

    def finish(self):
        for copy in self.sends:
            copy.wait_send()


def mlp_kernel(attn_ref, x_buf, gain_ref, wo_ref, w1_hbm, w3_hbm, w2_hbm, out_ref,
               part, other_in, chip_sum, far_in, near_in, last_in,
               x1_buf, h_buf, act_buf, w1_buf, w3_buf, w2_buf,
               w_sems, rs1_send, rs1_recv, ag_send, ag_recv, rs2_send, rs2_recv):
    me, core, chip, other, right, left = places()
    knock(other, right, left, lax.rem(chip + 2, CHIPS) * 2 + core)
    width = x_buf.shape[1]
    n_tok = act_buf.shape[0]
    n_chunks = w1_buf.shape[0]
    chunk = w1_buf.shape[2]

    def weight(kind, i):
        src = (w1_hbm, w3_hbm, w2_hbm)[kind]
        dst = (w1_buf, w3_buf, w2_buf)[kind]
        return pltpu.make_async_copy(src.at[0, :, pl.ds(pl.multiple_of(i * chunk, 128), chunk)], dst.at[i], w_sems.at[kind, i])

    for i in range(n_chunks):
        weight(0, i).start()
        weight(1, i).start()
    for i in range(n_chunks):
        weight(2, i).start()

    def plan(pieces, straight=0):
        size = width // pieces
        return [(j, pl.ds(j * size, size), 1 if j % 2 == 0 else -1, j >= pieces - straight) for j in range(pieces)]

    def put_part(cols, value):
        part[:, :, :, cols] = value.astype(BF16).reshape(CHIPS, 2, n_tok // (2 * CHIPS), value.shape[1])

    plan1 = plan(RS1_PIECES)
    rs1 = Reducer(part, other_in, chip_sum, far_in, near_in, last_in, rs1_send, rs1_recv)
    attn = attn_ref[...]
    for item in plan1:
        put_part(item[1], jnp.dot(attn, wo_ref[0, :, item[1]], preferred_element_type=F32))
        if item[0] == 0:
            enter(4)
        rs1.begin(*item)
    for stage in (rs1.far, rs1.near, rs1.third):
        for item in plan1:
            stage(*item)
    for item in plan1:
        cols = item[1]
        x1_buf[:, cols] = (x_buf[:, cols].astype(F32) + rs1.last(*item)).astype(BF16)
    rs1.finish()
    h_buf[me] = norm_rows(x1_buf[...].astype(F32), gain_ref[...].astype(F32))
    gather_rows(h_buf, ag_send, ag_recv)

    def gate_up(i, carry):
        weight(0, i).wait()
        weight(1, i).wait()
        h_all = h_buf[...].reshape(n_tok, width)
        gate = jnp.dot(h_all, w1_buf[i], preferred_element_type=F32)
        up = jnp.dot(h_all, w3_buf[i], preferred_element_type=F32)
        act_buf[:, pl.ds(pl.multiple_of(i * chunk, 128), chunk)] = (gate * jax.nn.sigmoid(gate) * up).astype(BF16)
        return carry

    lax.fori_loop(0, n_chunks, gate_up, 0)

    rs2 = Reducer(part, other_in, chip_sum, far_in, near_in, last_in, rs2_send, rs2_recv)
    plan2 = plan(n_chunks, RS2_STRAIGHT)
    for j in range(n_chunks + RS2_LAG):
        if j < n_chunks:
            weight(2, j).wait()
            put_part(plan2[j][1], jnp.dot(act_buf[...], w2_buf[j], preferred_element_type=F32))
            rs2.begin(*plan2[j])
        if j >= RS2_LAG:
            rs2.far(*plan2[j - RS2_LAG])
            rs2.near(*plan2[j - RS2_LAG])
            if plan2[j - RS2_LAG][3]:
                rs2.third(*plan2[j - RS2_LAG])
    for item in plan2:
        if not item[3]:
            rs2.third(*item)
    for item in plan2:
        cols = item[1]
        out_ref[:, cols] = (x1_buf[:, cols].astype(F32) + rs2.last(*item)).astype(BF16)
    rs2.finish()


def shape(dims, dtype=BF16):
    return jax.ShapeDtypeStruct(dims, dtype)


def to_tiles(cache):
    _, n_tok, n_rows, n_heads, head = cache.shape
    halves = head // LANES
    return cache.reshape(n_tok, n_rows, n_heads, halves, LANES).transpose(0, 1, 3, 2, 4).reshape(n_tok, n_rows * halves * n_heads, LANES)


def from_tiles(tiles, like):
    _, n_tok, n_rows, n_heads, head = like.shape
    halves = head // LANES
    return tiles.reshape(n_tok, n_rows, halves, n_heads, LANES).transpose(0, 1, 3, 2, 4).reshape(like.shape)


def run_qkv(x, gain, pos2, wq, wk, wv, k_tiles, v_tiles):
    n_tok = k_tiles.shape[0]
    rows, width = x.shape
    cols = wq.shape[2]
    blocks = n_tok // rows
    dma = pltpu.SemaphoreType.DMA
    args = (x, gain, pos2, wq, wk, wv, k_tiles, v_tiles)
    return pl.pallas_call(
        qkv_kernel,
        out_shape=[shape((n_tok, cols))] * 3 + [shape(k_tiles.shape)] * 2,
        in_specs=[HBM] * len(args),
        out_specs=[VMEM] * 5,
        scratch_shapes=[
            pltpu.VMEM((rows, width), BF16), pltpu.VMEM(gain.shape, BF16), pltpu.VMEM(pos2.shape, pos2.dtype),
            pltpu.VMEM((blocks, rows, width), BF16), pltpu.VMEM((3, width, cols), BF16),
            dma((6,)), dma((2, 4)), dma((GATHER_SEMS,)), dma((GATHER_SEMS,))],
        compiler_params=pltpu.CompilerParams(collective_id=0, has_side_effects=True, vmem_limit_bytes=36 << 20),
        name='gather_qkv',
    )(*(pltpu.with_memory_space_constraint(a, pltpu.HBM) for a in args))


def run_attn(pos2, q, k, v, k_tiles, v_tiles):
    n_tok = k_tiles.shape[0]
    rows2 = q.shape[1] // (2 * LANES) * n_tok
    dma = pltpu.SemaphoreType.DMA
    wide = pltpu.VMEM((2, rows2, LANES), F32)
    tiles = shape(k_tiles.shape)
    attn, _, _, k_out, v_out = pl.pallas_call(
        attn_kernel,
        out_shape=[shape(q.shape), tiles, tiles, tiles, tiles],
        in_specs=[SMEM, VMEM, VMEM, VMEM, VMEM, VMEM, VMEM],
        out_specs=[VMEM, VMEM, VMEM, HBM, HBM],
        scratch_shapes=[
            pltpu.VMEM((2, n_tok * 8, LANES), F32), wide, wide, pltpu.VMEM((rows2, n_tok), F32),
            dma((2, n_tok // TOK_STEP))],
        input_output_aliases={5: 1, 6: 2},
        compiler_params=pltpu.CompilerParams(vmem_limit_bytes=24 << 20),
        name='attention',
    )(pos2, pos2, q, k, v, k_tiles, v_tiles)
    return attn, k_out, v_out


def run_mlp(attn, x, gain, wo, w1, w3, w2):
    rows, width = x.shape
    n_tok = attn.shape[0]
    ffn = w1.shape[2]
    chunk = MLP_CHUNK
    n_chunks = ffn // chunk
    dma = pltpu.SemaphoreType.DMA
    block = pltpu.VMEM((rows, width), BF16)
    chips = pltpu.VMEM((CHIPS, rows, width), BF16)
    return pl.pallas_call(
        mlp_kernel,
        out_shape=shape((rows, width)),
        in_specs=[VMEM, VMEM, VMEM, VMEM, HBM, HBM, HBM],
        out_specs=VMEM,
        scratch_shapes=[
            pltpu.VMEM((CHIPS, 2, rows, width), BF16), chips, chips, block, block, block,
            block, pltpu.VMEM((n_tok // rows, rows, width), BF16), pltpu.VMEM((n_tok, ffn), BF16),
            pltpu.VMEM((n_chunks, width, chunk), BF16), pltpu.VMEM((n_chunks, width, chunk), BF16), pltpu.VMEM((width // chunk, ffn, chunk), BF16),
            dma((3, n_chunks)), dma((7, RS1_PIECES)), dma((7, RS1_PIECES)), dma((GATHER_SEMS,)), dma((GATHER_SEMS,)),
            dma((7, n_chunks)), dma((7, n_chunks))],
        compiler_params=pltpu.CompilerParams(collective_id=1, has_side_effects=True, vmem_limit_bytes=MLP_VMEM),
        name='reduce_mlp',
    )(*(pltpu.with_memory_space_constraint(a, pltpu.VMEM) for a in (attn, x, gain, wo)), w1, w3, w2)


def solution(mesh):
    row_spec = P(('data', 'model'), None)
    cache_spec = P(None, 'data', None, 'model', None)
    col_spec = P(None, None, 'model')
    inner_spec = P(None, 'model', None)
    in_specs = (row_spec, P('data'), P(), P(), col_spec, col_spec, col_spec, inner_spec, col_spec, col_spec, inner_spec, cache_spec, cache_spec)
    out_specs = (row_spec, cache_spec, cache_spec)

    def device_step(hidden, positions, attn_gain, mlp_gain, w_query, w_key, w_value, w_out, w_gate, w_up, w_down, k_cache, v_cache):
        n_tok = positions.shape[0]
        pos2 = positions.reshape(1, n_tok)
        q, k, v, k_tiles, v_tiles = run_qkv(hidden, attn_gain, pos2, w_query, w_key, w_value, to_tiles(k_cache), to_tiles(v_cache))
        attn, k_out, v_out = run_attn(pos2, q, k, v, k_tiles, v_tiles)
        out = run_mlp(attn, hidden, mlp_gain, w_out, w_gate, w_up, w_down)
        return out, from_tiles(k_out, k_cache), from_tiles(v_out, v_cache)

    return jax.shard_map(device_step, mesh=mesh, in_specs=in_specs, out_specs=out_specs, check_vma=False)
```

```python
import functools
import math
import jax
import jax.numpy as jnp
from jax import lax
from jax.experimental import pallas as pl
from jax.experimental.pallas import tpu as pltpu
from jax.sharding import PartitionSpec as P

NORM_EPS = 1e-5
ROPE_BASE = 10000.0
BF16 = jnp.bfloat16
F32 = jnp.float32
VMEM = pl.BlockSpec(memory_space=pltpu.VMEM)
HBM = pl.BlockSpec(memory_space=pltpu.HBM)
MLP_VMEM = 63400000
CHIPS = 4
MLP_CHUNK = 512
RS1_PIECES = 4
RS2_LAG = 3
RS2_STRAIGHT = 2
GATHER_SEMS = 21


def places():
    me = lax.axis_index('model')
    core = lax.rem(me, 2)
    chip = lax.div(me, 2)
    other = me + 1 - 2 * core
    right = lax.rem(chip + 1, CHIPS) * 2 + core
    left = lax.rem(chip + CHIPS - 1, CHIPS) * 2 + core
    return me, core, chip, other, right, left


def knock(*peers):
    barrier = pltpu.get_barrier_semaphore()
    for peer in peers:
        pl.semaphore_signal(barrier, inc=1, device_id={'model': peer})


def enter(peers):
    pl.semaphore_wait(pltpu.get_barrier_semaphore(), peers)


def remote(src, dst, send_sem, recv_sem, peer):
    return pltpu.make_async_remote_copy(src_ref=src, dst_ref=dst, send_sem=send_sem, recv_sem=recv_sem, device_id={'model': peer})


def norm_rows(x_f, gain_f):
    inv_rms = lax.rsqrt(jnp.mean(x_f * x_f, axis=-1, keepdims=True) + NORM_EPS)
    return (x_f * inv_rms * gain_f).astype(BF16)


def gather_rows(buf, send_sems, recv_sems, behind=()):
    me, core, chip, other, right, left = places()
    width = buf.shape[2]
    quarter = width // 4
    q0, q1, q2, q3 = (pl.ds(i * quarter, quarter) for i in range(4))
    lo, hi, full = pl.ds(0, 2 * quarter), pl.ds(2 * quarter, 2 * quarter), pl.ds(0, width)
    far = lax.rem(chip + 2, CHIPS) * 2 + core
    sends = []

    def hop(blk, cols, idx, peer):
        view = buf.at[blk, :, cols]
        return remote(view, view, send_sems.at[idx], recv_sems.at[idx], peer)

    def arrive(blk, cols, idx):
        hop(blk, cols, idx, other).wait_recv()

    def send(blk, cols, idx, peer):
        copy = hop(blk, cols, idx, peer)
        copy.start()
        sends.append(copy)

    for cols, idx, peer in ((q0, 0, right), (q2, 1, left), (q1, 2, right), (q3, 3, left), (hi, 4, right), (lo, 5, left), (full, 6, other)):
        send(me, cols, idx, peer)
    across = []
    behind = list(behind)
    share = -(-len(behind) // 8)
    for copy in behind[:2 * share]:
        copy.start()
    behind = behind[2 * share:]
    for blk, cols, idx, onward, peer in (
            (left, q0, 0, 7, right), (right, q2, 1, 8, left), (left, q1, 2, 9, right), (right, q3, 3, 10, left),
            (left, hi, 4, None, None), (right, lo, 5, None, None),
            (far, q0, 7, None, None), (far, q2, 8, None, None), (far, q1, 9, None, None), (far, q3, 10, None, None)):
        arrive(blk, cols, idx)
        if onward is not None:
            send(blk, cols, onward, peer)
        send(blk, cols, 11 + len(across), other)
        across.append((blk + 1 - 2 * core, cols, 11 + len(across)))
        for copy in behind[:share]:
            copy.start()
        behind = behind[share:]
    arrive(other, full, 6)
    for item in across:
        arrive(*item)
    for copy in sends:
        copy.wait_send()


LANES = 128


def qkv_kernel(x_hbm, gain_hbm, pos_hbm, wq_hbm, wk_hbm, wv_hbm, kc_hbm, vc_hbm, q_ref, k_ref, v_ref, kb_ref, vb_ref,
               x_buf, gain_ref, pos_ref, h_buf, w_buf, load_sems, cache_sems, send_sems, recv_sems):
    me, core, chip, other, right, left = places()
    knock(other, right, left)
    loads = [pltpu.make_async_copy(src, dst, load_sems.at[3 + i]) for i, (src, dst) in enumerate(((x_hbm, x_buf), (gain_hbm, gain_ref), (pos_hbm, pos_ref)))]
    w_copies = [pltpu.make_async_copy(w.at[0], w_buf.at[i], load_sems.at[i]) for i, w in enumerate((wq_hbm, wk_hbm, wv_hbm))]
    pieces = cache_sems.shape[1]
    piece = kb_ref.shape[0] // pieces
    cache_in = []
    for kv, (hbm, buf) in enumerate(((kc_hbm, kb_ref), (vc_hbm, vb_ref))):
        for p in range(pieces):
            toks = pl.ds(p * piece, piece)
            cache_in.append(pltpu.make_async_copy(hbm.at[toks], buf.at[toks], cache_sems.at[kv, p]))
    for copy in loads:
        copy.start()
    for copy in w_copies:
        copy.start()
    for copy in loads:
        copy.wait()
    h_buf[me] = norm_rows(x_buf[...].astype(F32), gain_ref[...].astype(F32))
    enter(3)
    gather_rows(h_buf, send_sems, recv_sems, cache_in)

    n_tok = pos_ref.shape[1]
    half = 128
    head = 2 * half
    pos_row = jnp.broadcast_to(pos_ref[...].astype(F32), (n_tok, n_tok))
    diag = lax.broadcasted_iota(jnp.int32, (n_tok, n_tok), 0) == lax.broadcasted_iota(jnp.int32, (n_tok, n_tok), 1)
    pos_col = jnp.sum(jnp.where(diag, pos_row, 0.0), axis=1, keepdims=True)
    lane = lax.broadcasted_iota(jnp.int32, (n_tok, half), 1).astype(F32)
    angles = pos_col * jnp.exp(lane * (-2.0 * math.log(ROPE_BASE) / head))
    cos_tab, sin_tab = jnp.cos(angles), jnp.sin(angles)
    h_all = h_buf[...].reshape(n_tok, h_buf.shape[2])
    for i, out_ref in enumerate((q_ref, k_ref, v_ref)):
        w_copies[i].wait()
        proj = jnp.dot(h_all, w_buf[i], preferred_element_type=F32).astype(BF16)
        if i == 2:
            out_ref[...] = proj
            continue
        for h0 in range(0, proj.shape[1], head):
            front = proj[:, h0:h0 + half].astype(F32)
            back = proj[:, h0 + half:h0 + head].astype(F32)
            out_ref[:, h0:h0 + half] = (front * cos_tab - back * sin_tab).astype(BF16)
            out_ref[:, h0 + half:h0 + head] = (back * cos_tab + front * sin_tab).astype(BF16)
    for copy in cache_in:
        copy.wait()


TOK_STEP = 16
TOK_SUB = 8


def attn_kernel(pos_hbm, pos_ref, q_ref, k_ref, v_ref, kb_in, vb_in, attn_ref, k_buf, v_buf, ko_hbm, vo_hbm,
                pos_smem, new_buf, q_buf, o_buf, pc_buf, score_buf, prob_buf, pos_sem, out_sems):
    n_tok, per_tok, lanes = k_buf.shape
    n_heads = 2
    head = q_ref.shape[1] // n_heads
    steps = n_tok // TOK_STEP
    bufs = (k_buf, v_buf)
    pos_copy = pltpu.make_async_copy(pos_hbm, pos_smem, pos_sem)
    pos_copy.start()

    def write_out(t):
        toks = pl.ds(t * TOK_STEP, TOK_STEP)
        return [pltpu.make_async_copy(buf.at[toks], hbm.at[toks], out_sems.at[kv, t]) for kv, (buf, hbm) in enumerate(zip(bufs, (ko_hbm, vo_hbm)))]

    for h in range(n_heads):
        for c in range(2):
            cols = slice(h * head + c * lanes, h * head + (c + 1) * lanes)
            q_buf.at[c][pl.ds(h, n_tok, stride=2), :] = q_ref[:, cols].astype(F32)
            for kv, ref in enumerate((k_ref, v_ref)):
                new = ref[:, cols].astype(F32)
                for again in range(2):
                    new_buf.at[kv][pl.ds(4 * again + 2 * c + h, n_tok, stride=8), :] = new
    rows2 = n_tok * n_heads
    pos_row = jnp.broadcast_to(pos_ref[...].astype(F32), (rows2, n_tok))
    own = lax.broadcasted_iota(jnp.int32, (rows2, n_tok), 0) // 2 == lax.broadcasted_iota(jnp.int32, (rows2, n_tok), 1)
    pc_buf[...] = jnp.broadcast_to(jnp.sum(jnp.where(own, pos_row, 0.0), axis=1, keepdims=True), (rows2, n_tok))

    tile_row = lax.broadcasted_iota(jnp.int32, (16, lanes), 0)
    sub = TOK_SUB * n_heads
    tok_of = (lax.broadcasted_iota(jnp.int32, (4 * sub, per_tok), 0) % sub) // 2
    row = lax.broadcasted_iota(jnp.int32, (2 * sub, per_tok), 0)
    col = lax.broadcasted_iota(jnp.int32, (2 * sub, per_tok), 1)
    counts = ((col & 2) == 0) & ((col & 1) == (row & 1))
    key_pos = (col >> 2).astype(F32)

    def shift(x, by):
        return jnp.concatenate([pltpu.roll(x[:, i:i + lanes], by % lanes, 1) for i in range(0, per_tok, lanes)], axis=1)

    def pair(buf, b0):
        one, two = (buf[pl.ds(b0 + g * TOK_SUB, TOK_SUB)] for g in range(2))
        return jnp.concatenate([x.reshape(TOK_SUB * per_tok, lanes) for x in (one, two)], axis=1)

    def out_rows(b0):
        return [pl.ds(pl.multiple_of(b0 * n_heads + g * sub, sub), sub) for g in range(2)]

    def mix(t):
        b0 = t * TOK_STEP
        probs = prob_buf[...]
        wide = jnp.concatenate([jnp.where(tok_of == m, probs, 0.0) for m in range(TOK_SUB)], axis=1).astype(BF16)
        out = jnp.dot(wide, pair(v_buf, b0), preferred_element_type=F32).astype(BF16).astype(F32)
        rows = out_rows(b0)
        for g in range(2):
            for c in range(2):
                at = (2 * g + c) * sub
                o_buf[c, rows[g], :] = out[at:at + sub, g * lanes:(g + 1) * lanes]

    def soften():
        total = score_buf[...]
        e = jnp.exp(total - jnp.max(total, axis=1, keepdims=True))
        probs = (e / jnp.sum(e, axis=1, keepdims=True)).astype(BF16).astype(F32)
        moved = shift(probs, 2)
        prob_buf[...] = jnp.concatenate([probs[:sub], moved[:sub], probs[sub:], moved[sub:]], axis=0)

    def score(t):
        b0 = t * TOK_STEP
        for i in range(TOK_STEP):
            b = b0 + i
            pos = pos_smem[0, b]
            tile = pl.ds(pl.multiple_of((pos >> 2) * 16, 16), 16)
            hit = (tile_row >> 2) == (pos & 3)
            for kv in range(2):
                new = new_buf[kv, pl.ds(pl.multiple_of(b * 8, 8), 8), :]
                old = bufs[kv][b, tile, :].astype(F32)
                bufs[kv][b, tile, :] = jnp.where(hit, jnp.concatenate([new, new], axis=0), old).astype(BF16)
        rows = out_rows(b0)
        none = jnp.zeros((sub, lanes), F32)
        q = jnp.concatenate(
            [jnp.concatenate([q_buf[c, rows[0], :], none], axis=1) for c in range(2)] +
            [jnp.concatenate([none, q_buf[c, rows[1], :]], axis=1) for c in range(2)], axis=0).astype(BF16)
        scores = lax.dot_general(q, pair(k_buf, b0), (((1,), (1,)), ((), ())), preferred_element_type=F32)
        mine = scores[:, :per_tok]
        for m in range(1, TOK_SUB):
            mine = jnp.where(tok_of == m, scores[:, m * per_tok:(m + 1) * per_tok], mine)
        first = jnp.concatenate([mine[:sub], mine[2 * sub:3 * sub]], axis=0)
        second = jnp.concatenate([mine[sub:2 * sub], mine[3 * sub:]], axis=0)
        total = (first + shift(second, -2)) * (head ** -0.5)
        pos_of = pc_buf[pl.ds(pl.multiple_of(b0 * n_heads, 2 * sub), 2 * sub), :]
        score_buf[...] = jnp.where(counts & (key_pos <= jnp.concatenate([pos_of] * (per_tok // lanes), axis=1)), total, -1e30)

    def send(t):
        for copy in write_out(t):
            copy.start()

    pos_copy.wait()
    score(0)
    send(0)
    soften()
    score(1)
    send(1)

    def step(t, carry):
        mix(t - 2)
        soften()
        score(t)
        send(t)
        return carry

    lax.fori_loop(2, steps, step, 0)
    mix(steps - 2)
    soften()
    mix(steps - 1)
    attn_ref[...] = jnp.concatenate([o_buf.at[c][pl.ds(h, n_tok, stride=2), :] for h in range(n_heads) for c in range(2)], axis=1).astype(BF16)
    for t in range(steps):
        for copy in write_out(t):
            copy.wait()


class Reducer:
    def __init__(self, part, from_other, chip_sum, far_in, near_in, last_in, send_sems, recv_sems):
        self.part, self.from_other, self.chip_sum = part, from_other, chip_sum
        self.far_in, self.near_in, self.last_in = far_in, near_in, last_in
        self.send_sems, self.recv_sems = send_sems, recv_sems
        self.me, self.core, self.chip, self.other, self.right, self.left = places()
        self.sends = []

    def copy(self, kind, j, cols, way, direct):
        nxt, prv = (self.right, self.left) if way > 0 else (self.left, self.right)
        ahead = lax.rem(self.chip + CHIPS + way, CHIPS)
        behind = lax.rem(self.chip + CHIPS - way, CHIPS)
        opposite = lax.rem(self.chip + 2, CHIPS)
        if kind < 4:
            k = (opposite, behind, ahead, self.chip)[kind]
            src, dst, peer = self.part.at[k, 1 - self.core, :, cols], self.from_other.at[k, :, cols], self.other
        else:
            src, dst, peer = (
                (self.chip_sum.at[opposite, :, cols], self.far_in.at[:, cols], opposite * 2 + self.core if direct else nxt),
                (self.chip_sum.at[behind, :, cols], self.near_in.at[:, cols], prv),
                (self.chip_sum.at[ahead, :, cols], self.last_in.at[:, cols], nxt),
            )[kind - 4]
        return remote(src, dst, self.send_sems.at[kind, j], self.recv_sems.at[kind, j], peer)

    def go(self, kind, j, cols, way, direct):
        copy = self.copy(kind, j, cols, way, direct)
        copy.start()
        self.sends.append(copy)

    def begin(self, j, cols, way, direct):
        for kind in range(4):
            self.go(kind, j, cols, way, direct)

    def pair(self, kind, k, j, cols, way, direct):
        self.copy(kind, j, cols, way, direct).wait_recv()
        return self.part[k, self.core, :, cols].astype(F32) + self.from_other[k, :, cols].astype(F32)

    def far(self, j, cols, way, direct):
        opposite = lax.rem(self.chip + 2, CHIPS)
        self.chip_sum[opposite, :, cols] = self.pair(0, opposite, j, cols, way, direct).astype(BF16)
        self.go(4, j, cols, way, direct)

    def near(self, j, cols, way, direct):
        behind = lax.rem(self.chip + CHIPS - way, CHIPS)
        self.chip_sum[behind, :, cols] = self.pair(1, behind, j, cols, way, direct).astype(BF16)
        self.go(5, j, cols, way, direct)

    def third(self, j, cols, way, direct):
        ahead = lax.rem(self.chip + CHIPS + way, CHIPS)
        mine = self.pair(2, ahead, j, cols, way, direct)
        if not direct:
            self.copy(4, j, cols, way, direct).wait_recv()
            mine = mine + self.far_in[:, cols].astype(F32)
        self.chip_sum[ahead, :, cols] = mine.astype(BF16)
        self.go(6, j, cols, way, direct)

    def last(self, j, cols, way, direct):
        own = self.pair(3, self.chip, j, cols, way, direct)
        self.copy(5, j, cols, way, direct).wait_recv()
        own = own + self.near_in[:, cols].astype(F32)
        if direct:
            self.copy(4, j, cols, way, direct).wait_recv()
            own = own + self.far_in[:, cols].astype(F32)
        self.copy(6, j, cols, way, direct).wait_recv()
        return own + self.last_in[:, cols].astype(F32)

    def finish(self):
        for copy in self.sends:
            copy.wait_send()


def mlp_kernel(attn_ref, x_buf, gain_ref, wo_ref, w1_hbm, w3_hbm, w2_hbm, out_ref,
               part, other_in, chip_sum, far_in, near_in, last_in,
               x1_buf, h_buf, act_buf, w1_buf, w3_buf, w2_buf,
               w_sems, rs1_send, rs1_recv, ag_send, ag_recv, rs2_send, rs2_recv):
    me, core, chip, other, right, left = places()
    knock(other, right, left, lax.rem(chip + 2, CHIPS) * 2 + core)
    width = x_buf.shape[1]
    n_tok = act_buf.shape[0]
    n_chunks = w1_buf.shape[0]
    chunk = w1_buf.shape[2]

    def weight(kind, i):
        src = (w1_hbm, w3_hbm, w2_hbm)[kind]
        dst = (w1_buf, w3_buf, w2_buf)[kind]
        return pltpu.make_async_copy(src.at[0, :, pl.ds(pl.multiple_of(i * chunk, 128), chunk)], dst.at[i], w_sems.at[kind, i])

    for i in range(n_chunks):
        weight(0, i).start()
        weight(1, i).start()

    def plan(pieces, straight=0):
        size = width // pieces
        return [(j, pl.ds(j * size, size), 1 if j % 2 == 0 else -1, j >= pieces - straight) for j in range(pieces)]

    def put_part(cols, value):
        part[:, :, :, cols] = value.astype(BF16).reshape(CHIPS, 2, n_tok // (2 * CHIPS), value.shape[1])

    plan1 = plan(RS1_PIECES)
    rs1 = Reducer(part, other_in, chip_sum, far_in, near_in, last_in, rs1_send, rs1_recv)
    attn = attn_ref[...]
    for item in plan1:
        put_part(item[1], jnp.dot(attn, wo_ref[0, :, item[1]], preferred_element_type=F32))
        if item[0] == 0:
            enter(4)
        rs1.begin(*item)
    for stage in (rs1.far, rs1.near, rs1.third):
        for item in plan1:
            stage(*item)
    for item in plan1:
        cols = item[1]
        x1_buf[:, cols] = (x_buf[:, cols].astype(F32) + rs1.last(*item)).astype(BF16)
    rs1.finish()
    h_buf[me] = norm_rows(x1_buf[...].astype(F32), gain_ref[...].astype(F32))
    gather_rows(h_buf, ag_send, ag_recv)
    for i in range(n_chunks):
        weight(2, i).start()

    def gate_up(i, carry):
        weight(0, i).wait()
        weight(1, i).wait()
        h_all = h_buf[...].reshape(n_tok, width)
        gate = jnp.dot(h_all, w1_buf[i], preferred_element_type=F32)
        up = jnp.dot(h_all, w3_buf[i], preferred_element_type=F32)
        act_buf[:, pl.ds(pl.multiple_of(i * chunk, 128), chunk)] = (gate * jax.nn.sigmoid(gate) * up).astype(BF16)
        return carry

    lax.fori_loop(0, n_chunks, gate_up, 0)

    rs2 = Reducer(part, other_in, chip_sum, far_in, near_in, last_in, rs2_send, rs2_recv)
    plan2 = plan(n_chunks, RS2_STRAIGHT)
    for j in range(n_chunks + RS2_LAG):
        if j < n_chunks:
            weight(2, j).wait()
            put_part(plan2[j][1], jnp.dot(act_buf[...], w2_buf[j], preferred_element_type=F32))
            rs2.begin(*plan2[j])
        if j >= RS2_LAG:
            rs2.far(*plan2[j - RS2_LAG])
            rs2.near(*plan2[j - RS2_LAG])
            if plan2[j - RS2_LAG][3]:
                rs2.third(*plan2[j - RS2_LAG])
    for item in plan2:
        if not item[3]:
            rs2.third(*item)
    for item in plan2:
        cols = item[1]
        out_ref[:, cols] = (x1_buf[:, cols].astype(F32) + rs2.last(*item)).astype(BF16)
    rs2.finish()


def shape(dims, dtype=BF16):
    return jax.ShapeDtypeStruct(dims, dtype)


def to_tiles(cache):
    _, n_tok, n_rows, n_heads, head = cache.shape
    halves = head // LANES
    return cache.reshape(n_tok, n_rows, n_heads, halves, LANES).transpose(0, 1, 3, 2, 4).reshape(n_tok, n_rows * halves * n_heads, LANES)


def from_tiles(tiles, like):
    _, n_tok, n_rows, n_heads, head = like.shape
    halves = head // LANES
    return tiles.reshape(n_tok, n_rows, halves, n_heads, LANES).transpose(0, 1, 3, 2, 4).reshape(like.shape)


def run_qkv(x, gain, pos2, wq, wk, wv, k_tiles, v_tiles):
    n_tok = k_tiles.shape[0]
    rows, width = x.shape
    cols = wq.shape[2]
    blocks = n_tok // rows
    dma = pltpu.SemaphoreType.DMA
    args = (x, gain, pos2, wq, wk, wv, k_tiles, v_tiles)
    return pl.pallas_call(
        qkv_kernel,
        out_shape=[shape((n_tok, cols))] * 3 + [shape(k_tiles.shape)] * 2,
        in_specs=[HBM] * len(args),
        out_specs=[VMEM] * 5,
        scratch_shapes=[
            pltpu.VMEM((rows, width), BF16), pltpu.VMEM(gain.shape, BF16), pltpu.VMEM(pos2.shape, pos2.dtype),
            pltpu.VMEM((blocks, rows, width), BF16), pltpu.VMEM((3, width, cols), BF16),
            dma((6,)), dma((2, 8)), dma((GATHER_SEMS,)), dma((GATHER_SEMS,))],
        compiler_params=pltpu.CompilerParams(collective_id=0, has_side_effects=True, vmem_limit_bytes=36 << 20),
        name='gather_qkv',
    )(*(pltpu.with_memory_space_constraint(a, pltpu.HBM) for a in args))


def run_attn(pos2, q, k, v, k_tiles, v_tiles):
    n_tok = k_tiles.shape[0]
    rows2 = q.shape[1] // (2 * LANES) * n_tok
    dma = pltpu.SemaphoreType.DMA
    wide = pltpu.VMEM((2, rows2, LANES), F32)
    tiles = shape(k_tiles.shape)
    attn, _, _, k_out, v_out = pl.pallas_call(
        attn_kernel,
        out_shape=[shape(q.shape), tiles, tiles, tiles, tiles],
        in_specs=[HBM, VMEM, VMEM, VMEM, VMEM, VMEM, VMEM],
        out_specs=[VMEM, VMEM, VMEM, HBM, HBM],
        scratch_shapes=[
            pltpu.SMEM(pos2.shape, pos2.dtype), pltpu.VMEM((2, n_tok * 8, LANES), F32), wide, wide, pltpu.VMEM((rows2, n_tok), F32),
            pltpu.VMEM((4 * TOK_SUB, k_tiles.shape[1]), F32), pltpu.VMEM((8 * TOK_SUB, k_tiles.shape[1]), F32),
            dma, dma((2, n_tok // TOK_STEP))],
        input_output_aliases={5: 1, 6: 2},
        compiler_params=pltpu.CompilerParams(vmem_limit_bytes=24 << 20),
        name='attention',
    )(pltpu.with_memory_space_constraint(pos2, pltpu.HBM), pos2, q, k, v, k_tiles, v_tiles)
    return attn, k_out, v_out


def run_mlp(attn, x, gain, wo, w1, w3, w2):
    rows, width = x.shape
    n_tok = attn.shape[0]
    ffn = w1.shape[2]
    chunk = MLP_CHUNK
    n_chunks = ffn // chunk
    dma = pltpu.SemaphoreType.DMA
    block = pltpu.VMEM((rows, width), BF16)
    chips = pltpu.VMEM((CHIPS, rows, width), BF16)
    return pl.pallas_call(
        mlp_kernel,
        out_shape=shape((rows, width)),
        in_specs=[VMEM, VMEM, VMEM, VMEM, HBM, HBM, HBM],
        out_specs=VMEM,
        scratch_shapes=[
            pltpu.VMEM((CHIPS, 2, rows, width), BF16), chips, chips, block, block, block,
            block, pltpu.VMEM((n_tok // rows, rows, width), BF16), pltpu.VMEM((n_tok, ffn), BF16),
            pltpu.VMEM((n_chunks, width, chunk), BF16), pltpu.VMEM((n_chunks, width, chunk), BF16), pltpu.VMEM((width // chunk, ffn, chunk), BF16),
            dma((3, n_chunks)), dma((7, RS1_PIECES)), dma((7, RS1_PIECES)), dma((GATHER_SEMS,)), dma((GATHER_SEMS,)),
            dma((7, n_chunks)), dma((7, n_chunks))],
        compiler_params=pltpu.CompilerParams(collective_id=1, has_side_effects=True, vmem_limit_bytes=MLP_VMEM),
        name='reduce_mlp',
    )(*(pltpu.with_memory_space_constraint(a, pltpu.VMEM) for a in (attn, x, gain, wo)), w1, w3, w2)


def solution(mesh):
    row_spec = P(('data', 'model'), None)
    cache_spec = P(None, 'data', None, 'model', None)
    col_spec = P(None, None, 'model')
    inner_spec = P(None, 'model', None)
    in_specs = (row_spec, P('data'), P(), P(), col_spec, col_spec, col_spec, inner_spec, col_spec, col_spec, inner_spec, cache_spec, cache_spec)
    out_specs = (row_spec, cache_spec, cache_spec)

    def device_step(hidden, positions, attn_gain, mlp_gain, w_query, w_key, w_value, w_out, w_gate, w_up, w_down, k_cache, v_cache):
        n_tok = positions.shape[0]
        pos2 = positions.reshape(1, n_tok)
        q, k, v, k_tiles, v_tiles = run_qkv(hidden, attn_gain, pos2, w_query, w_key, w_value, to_tiles(k_cache), to_tiles(v_cache))
        attn, k_out, v_out = run_attn(pos2, q, k, v, k_tiles, v_tiles)
        out = run_mlp(attn, hidden, mlp_gain, w_out, w_gate, w_up, w_down)
        return out, from_tiles(k_out, k_cache), from_tiles(v_out, v_cache)

    return jax.shard_map(device_step, mesh=mesh, in_specs=in_specs, out_specs=out_specs, check_vma=False)
```

```python
import functools
import math
import jax
import jax.numpy as jnp
from jax import lax
from jax.experimental import pallas as pl
from jax.experimental.pallas import tpu as pltpu
from jax.sharding import PartitionSpec as P

NORM_EPS = 1e-5
ROPE_BASE = 10000.0
BF16 = jnp.bfloat16
F32 = jnp.float32
VMEM = pl.BlockSpec(memory_space=pltpu.VMEM)
HBM = pl.BlockSpec(memory_space=pltpu.HBM)
MLP_VMEM = 63400000
CHIPS = 4
MLP_CHUNK = 512
RS1_PIECES = 4
RS2_LAG = 3
RS2_STRAIGHT = 2
GATHER_SEMS = 21


def places():
    me = lax.axis_index('model')
    core = lax.rem(me, 2)
    chip = lax.div(me, 2)
    other = me + 1 - 2 * core
    right = lax.rem(chip + 1, CHIPS) * 2 + core
    left = lax.rem(chip + CHIPS - 1, CHIPS) * 2 + core
    return me, core, chip, other, right, left


def knock(*peers):
    barrier = pltpu.get_barrier_semaphore()
    for peer in peers:
        pl.semaphore_signal(barrier, inc=1, device_id={'model': peer})


def enter(peers):
    pl.semaphore_wait(pltpu.get_barrier_semaphore(), peers)


def remote(src, dst, send_sem, recv_sem, peer):
    return pltpu.make_async_remote_copy(src_ref=src, dst_ref=dst, send_sem=send_sem, recv_sem=recv_sem, device_id={'model': peer})


def norm_rows(x_f, gain_f):
    inv_rms = lax.rsqrt(jnp.mean(x_f * x_f, axis=-1, keepdims=True) + NORM_EPS)
    return (x_f * inv_rms * gain_f).astype(BF16)


def gather_rows(buf, send_sems, recv_sems, behind=(), meanwhile=None):
    me, core, chip, other, right, left = places()
    width = buf.shape[2]
    quarter = width // 4
    q0, q1, q2, q3 = (pl.ds(i * quarter, quarter) for i in range(4))
    lo, hi, full = pl.ds(0, 2 * quarter), pl.ds(2 * quarter, 2 * quarter), pl.ds(0, width)
    far = lax.rem(chip + 2, CHIPS) * 2 + core
    sends = []

    def hop(blk, cols, idx, peer):
        view = buf.at[blk, :, cols]
        return remote(view, view, send_sems.at[idx], recv_sems.at[idx], peer)

    def arrive(blk, cols, idx):
        hop(blk, cols, idx, other).wait_recv()

    def send(blk, cols, idx, peer):
        copy = hop(blk, cols, idx, peer)
        copy.start()
        sends.append(copy)

    for cols, idx, peer in ((q0, 0, right), (q2, 1, left), (q1, 2, right), (q3, 3, left), (hi, 4, right), (lo, 5, left), (full, 6, other)):
        send(me, cols, idx, peer)
    across = []
    behind = list(behind)
    share = -(-len(behind) // 8)
    for copy in behind[:2 * share]:
        copy.start()
    behind = behind[2 * share:]
    if meanwhile is not None:
        meanwhile()
    for blk, cols, idx, onward, peer in (
            (left, q0, 0, 7, right), (right, q2, 1, 8, left), (left, q1, 2, 9, right), (right, q3, 3, 10, left),
            (left, hi, 4, None, None), (right, lo, 5, None, None),
            (far, q0, 7, None, None), (far, q2, 8, None, None), (far, q1, 9, None, None), (far, q3, 10, None, None)):
        arrive(blk, cols, idx)
        if onward is not None:
            send(blk, cols, onward, peer)
        send(blk, cols, 11 + len(across), other)
        across.append((blk + 1 - 2 * core, cols, 11 + len(across)))
        for copy in behind[:share]:
            copy.start()
        behind = behind[share:]
    arrive(other, full, 6)
    for item in across:
        arrive(*item)
    for copy in sends:
        copy.wait_send()


LANES = 128


def qkv_kernel(x_hbm, gain_hbm, pos_hbm, wq_hbm, wk_hbm, wv_hbm, kc_hbm, vc_hbm, q_ref, k_ref, v_ref, kb_ref, vb_ref, pc_ref,
               trig_buf, x_buf, gain_ref, pos_ref, h_buf, w_buf, load_sems, cache_sems, send_sems, recv_sems):
    me, core, chip, other, right, left = places()
    knock(other, right, left)
    loads = [pltpu.make_async_copy(src, dst, load_sems.at[3 + i]) for i, (src, dst) in enumerate(((x_hbm, x_buf), (gain_hbm, gain_ref), (pos_hbm, pos_ref)))]
    w_copies = [pltpu.make_async_copy(w.at[0], w_buf.at[i], load_sems.at[i]) for i, w in enumerate((wq_hbm, wk_hbm, wv_hbm))]
    pieces = cache_sems.shape[1]
    piece = kb_ref.shape[0] // pieces
    cache_in = []
    for kv, (hbm, buf) in enumerate(((kc_hbm, kb_ref), (vc_hbm, vb_ref))):
        for p in range(pieces):
            toks = pl.ds(p * piece, piece)
            cache_in.append(pltpu.make_async_copy(hbm.at[toks], buf.at[toks], cache_sems.at[kv, p]))
    for copy in loads:
        copy.start()
    for copy in loads:
        copy.wait()
    h_buf[me] = norm_rows(x_buf[...].astype(F32), gain_ref[...].astype(F32))
    enter(3)
    n_tok = pos_ref.shape[1]
    half = LANES
    head = 2 * half
    pos_f = pos_ref[...].astype(F32)

    def pick(rows, per):
        own = lax.broadcasted_iota(jnp.int32, (rows, n_tok), 0) // per == lax.broadcasted_iota(jnp.int32, (rows, n_tok), 1)
        return jnp.sum(jnp.where(own, jnp.broadcast_to(pos_f, (rows, n_tok)), 0.0), axis=1, keepdims=True)

    def tables():
        lane = lax.broadcasted_iota(jnp.int32, (n_tok, half), 1).astype(F32)
        angles = pick(n_tok, 1) * jnp.exp(lane * (-2.0 * math.log(ROPE_BASE) / head))
        trig_buf[0] = jnp.cos(angles)
        trig_buf[1] = jnp.sin(angles)
        rows2 = pc_ref.shape[0]
        pc_ref[...] = jnp.broadcast_to(pick(rows2, rows2 // n_tok), pc_ref.shape)

    gather_rows(h_buf, send_sems, recv_sems, w_copies + cache_in, tables)
    cos_tab, sin_tab = trig_buf[0], trig_buf[1]
    h_all = h_buf[...].reshape(n_tok, h_buf.shape[2])
    for i, out_ref in enumerate((q_ref, k_ref, v_ref)):
        w_copies[i].wait()
        proj = jnp.dot(h_all, w_buf[i], preferred_element_type=F32).astype(BF16)
        if i == 2:
            out_ref[...] = proj
            continue
        for h0 in range(0, proj.shape[1], head):
            front = proj[:, h0:h0 + half].astype(F32)
            back = proj[:, h0 + half:h0 + head].astype(F32)
            out_ref[:, h0:h0 + half] = (front * cos_tab - back * sin_tab).astype(BF16)
            out_ref[:, h0 + half:h0 + head] = (back * cos_tab + front * sin_tab).astype(BF16)
    for copy in cache_in:
        copy.wait()


TOK_STEP = 16
TOK_UNIT = 8
TOK_SUB = 4


def attn_kernel(pos_hbm, pc_buf, q_ref, k_ref, v_ref, kb_in, vb_in, attn_ref, k_buf, v_buf, ko_hbm, vo_hbm,
                pos_smem, new_buf, q_buf, o_buf, score_buf, prob_buf, pos_sem, out_sems):
    n_tok, per_tok, lanes = k_buf.shape
    n_heads = 2
    head = q_ref.shape[1] // n_heads
    steps = n_tok // TOK_STEP
    bufs = (k_buf, v_buf)
    pos_copy = pltpu.make_async_copy(pos_hbm, pos_smem, pos_sem)
    pos_copy.start()

    def write_out(t):
        toks = pl.ds(t * TOK_STEP, TOK_STEP)
        return [pltpu.make_async_copy(buf.at[toks], hbm.at[toks], out_sems.at[kv, t]) for kv, (buf, hbm) in enumerate(zip(bufs, (ko_hbm, vo_hbm)))]

    for h in range(n_heads):
        for c in range(2):
            cols = slice(h * head + c * lanes, h * head + (c + 1) * lanes)
            q_buf.at[c][pl.ds(h, n_tok, stride=2), :] = q_ref[:, cols].astype(F32)
            for kv, ref in enumerate((k_ref, v_ref)):
                new = ref[:, cols].astype(F32)
                for again in range(2):
                    new_buf.at[kv][pl.ds(4 * again + 2 * c + h, n_tok, stride=8), :] = new
    tile_row = lax.broadcasted_iota(jnp.int32, (16, lanes), 0)
    sub = TOK_SUB * n_heads
    tok_of = (lax.broadcasted_iota(jnp.int32, (4 * sub, per_tok), 0) % sub) // 2
    row = lax.broadcasted_iota(jnp.int32, (2 * sub, per_tok), 0)
    col = lax.broadcasted_iota(jnp.int32, (2 * sub, per_tok), 1)
    counts = ((col & 2) == 0) & ((col & 1) == (row & 1))
    key_pos = (col >> 2).astype(F32)

    def shift(x, by):
        return jnp.concatenate([pltpu.roll(x[:, i:i + lanes], by % lanes, 1) for i in range(0, per_tok, lanes)], axis=1)

    def pair(buf, b0):
        one, two = (buf[pl.ds(b0 + g * TOK_SUB, TOK_SUB)] for g in range(2))
        return jnp.concatenate([x.reshape(TOK_SUB * per_tok, lanes) for x in (one, two)], axis=1)

    def out_rows(b0):
        return [pl.ds(pl.multiple_of(b0 * n_heads + g * sub, sub), sub) for g in range(2)]

    units = TOK_STEP // TOK_UNIT

    def mix(t, u):
        b0 = t * TOK_STEP + u * TOK_UNIT
        probs = prob_buf[u]
        wide = jnp.concatenate([jnp.where(tok_of == m, probs, 0.0) for m in range(TOK_SUB)], axis=1).astype(BF16)
        out = jnp.dot(wide, pair(v_buf, b0), preferred_element_type=F32).astype(BF16).astype(F32)
        rows = out_rows(b0)
        for g in range(2):
            for c in range(2):
                at = (2 * g + c) * sub
                o_buf[c, rows[g], :] = out[at:at + sub, g * lanes:(g + 1) * lanes]

    def soften(u):
        total = score_buf[u]
        e = jnp.exp(total - jnp.max(total, axis=1, keepdims=True))
        probs = (e / jnp.sum(e, axis=1, keepdims=True)).astype(BF16).astype(F32)
        moved = shift(probs, 2)
        prob_buf[u] = jnp.concatenate([probs[:sub], moved[:sub], probs[sub:], moved[sub:]], axis=0)

    def score(t, u):
        b0 = t * TOK_STEP + u * TOK_UNIT
        for i in range(TOK_UNIT):
            b = b0 + i
            pos = pos_smem[0, b]
            tile = pl.ds(pl.multiple_of((pos >> 2) * 16, 16), 16)
            hit = (tile_row >> 2) == (pos & 3)
            for kv in range(2):
                new = new_buf[kv, pl.ds(pl.multiple_of(b * 8, 8), 8), :]
                old = bufs[kv][b, tile, :].astype(F32)
                bufs[kv][b, tile, :] = jnp.where(hit, jnp.concatenate([new, new], axis=0), old).astype(BF16)
        rows = out_rows(b0)
        none = jnp.zeros((sub, lanes), F32)
        q = jnp.concatenate(
            [jnp.concatenate([q_buf[c, rows[0], :], none], axis=1) for c in range(2)] +
            [jnp.concatenate([none, q_buf[c, rows[1], :]], axis=1) for c in range(2)], axis=0).astype(BF16)
        scores = lax.dot_general(q, pair(k_buf, b0), (((1,), (1,)), ((), ())), preferred_element_type=F32)
        mine = scores[:, :per_tok]
        for m in range(1, TOK_SUB):
            mine = jnp.where(tok_of == m, scores[:, m * per_tok:(m + 1) * per_tok], mine)
        first = jnp.concatenate([mine[:sub], mine[2 * sub:3 * sub]], axis=0)
        second = jnp.concatenate([mine[sub:2 * sub], mine[3 * sub:]], axis=0)
        total = (first + shift(second, -2)) * (head ** -0.5)
        pos_of = pc_buf[pl.ds(pl.multiple_of(b0 * n_heads, 2 * sub), 2 * sub), :]
        score_buf[u] = jnp.where(counts & (key_pos <= jnp.concatenate([pos_of] * (per_tok // lanes), axis=1)), total, -1e30)

    def send(t):
        for copy in write_out(t):
            copy.start()

    def each(stage, *args):
        for u in range(units):
            stage(*args, u)

    pos_copy.wait()
    each(score, 0)
    send(0)
    each(soften)
    each(score, 1)
    send(1)

    def step(t, carry):
        each(mix, t - 2)
        each(soften)
        each(score, t)
        send(t)
        return carry

    lax.fori_loop(2, steps, step, 0)
    each(mix, steps - 2)
    each(soften)
    each(mix, steps - 1)
    attn_ref[...] = jnp.concatenate([o_buf.at[c][pl.ds(h, n_tok, stride=2), :] for h in range(n_heads) for c in range(2)], axis=1).astype(BF16)
    for t in range(steps):
        for copy in write_out(t):
            copy.wait()


class Reducer:
    def __init__(self, part, from_other, chip_sum, far_in, near_in, last_in, send_sems, recv_sems):
        self.part, self.from_other, self.chip_sum = part, from_other, chip_sum
        self.far_in, self.near_in, self.last_in = far_in, near_in, last_in
        self.send_sems, self.recv_sems = send_sems, recv_sems
        self.me, self.core, self.chip, self.other, self.right, self.left = places()
        self.sends = []

    def copy(self, kind, j, cols, way, direct):
        nxt, prv = (self.right, self.left) if way > 0 else (self.left, self.right)
        ahead = lax.rem(self.chip + CHIPS + way, CHIPS)
        behind = lax.rem(self.chip + CHIPS - way, CHIPS)
        opposite = lax.rem(self.chip + 2, CHIPS)
        if kind < 4:
            k = (opposite, behind, ahead, self.chip)[kind]
            src, dst, peer = self.part.at[k, 1 - self.core, :, cols], self.from_other.at[k, :, cols], self.other
        else:
            src, dst, peer = (
                (self.chip_sum.at[opposite, :, cols], self.far_in.at[:, cols], opposite * 2 + self.core if direct else nxt),
                (self.chip_sum.at[behind, :, cols], self.near_in.at[:, cols], prv),
                (self.chip_sum.at[ahead, :, cols], self.last_in.at[:, cols], nxt),
            )[kind - 4]
        return remote(src, dst, self.send_sems.at[kind, j], self.recv_sems.at[kind, j], peer)

    def go(self, kind, j, cols, way, direct):
        copy = self.copy(kind, j, cols, way, direct)
        copy.start()
        self.sends.append(copy)

    def begin(self, j, cols, way, direct):
        for kind in range(4):
            self.go(kind, j, cols, way, direct)

    def pair(self, kind, k, j, cols, way, direct):
        self.copy(kind, j, cols, way, direct).wait_recv()
        return self.part[k, self.core, :, cols].astype(F32) + self.from_other[k, :, cols].astype(F32)

    def far(self, j, cols, way, direct):
        opposite = lax.rem(self.chip + 2, CHIPS)
        self.chip_sum[opposite, :, cols] = self.pair(0, opposite, j, cols, way, direct).astype(BF16)
        self.go(4, j, cols, way, direct)

    def near(self, j, cols, way, direct):
        behind = lax.rem(self.chip + CHIPS - way, CHIPS)
        self.chip_sum[behind, :, cols] = self.pair(1, behind, j, cols, way, direct).astype(BF16)
        self.go(5, j, cols, way, direct)

    def third(self, j, cols, way, direct):
        ahead = lax.rem(self.chip + CHIPS + way, CHIPS)
        mine = self.pair(2, ahead, j, cols, way, direct)
        if not direct:
            self.copy(4, j, cols, way, direct).wait_recv()
            mine = mine + self.far_in[:, cols].astype(F32)
        self.chip_sum[ahead, :, cols] = mine.astype(BF16)
        self.go(6, j, cols, way, direct)

    def last(self, j, cols, way, direct):
        own = self.pair(3, self.chip, j, cols, way, direct)
        self.copy(5, j, cols, way, direct).wait_recv()
        own = own + self.near_in[:, cols].astype(F32)
        if direct:
            self.copy(4, j, cols, way, direct).wait_recv()
            own = own + self.far_in[:, cols].astype(F32)
        self.copy(6, j, cols, way, direct).wait_recv()
        return own + self.last_in[:, cols].astype(F32)

    def finish(self):
        for copy in self.sends:
            copy.wait_send()


def mlp_kernel(attn_ref, x_buf, gain_ref, wo_ref, w1_hbm, w3_hbm, w2_hbm, out_ref,
               part, other_in, chip_sum, far_in, near_in, last_in,
               x1_buf, h_buf, act_buf, w1_buf, w3_buf, w2_buf,
               w_sems, rs1_send, rs1_recv, ag_send, ag_recv, rs2_send, rs2_recv):
    me, core, chip, other, right, left = places()
    knock(other, right, left, lax.rem(chip + 2, CHIPS) * 2 + core)
    width = x_buf.shape[1]
    n_tok = act_buf.shape[0]
    n_chunks = w1_buf.shape[0]
    chunk = w1_buf.shape[2]

    def weight(kind, i):
        src = (w1_hbm, w3_hbm, w2_hbm)[kind]
        dst = (w1_buf, w3_buf, w2_buf)[kind]
        return pltpu.make_async_copy(src.at[0, :, pl.ds(pl.multiple_of(i * chunk, 128), chunk)], dst.at[i], w_sems.at[kind, i])

    queue = [weight(kind, i) for i in range(n_chunks) for kind in range(2)] + [weight(2, i) for i in range(n_chunks)]

    def feed(n):
        for copy in queue[:n]:
            copy.start()
        del queue[:n]

    feed(2)

    def plan(pieces, straight=0):
        size = width // pieces
        return [(j, pl.ds(j * size, size), 1 if j % 2 == 0 else -1, j >= pieces - straight) for j in range(pieces)]

    def put_part(cols, value):
        part[:, :, :, cols] = value.astype(BF16).reshape(CHIPS, 2, n_tok // (2 * CHIPS), value.shape[1])

    plan1 = plan(RS1_PIECES)
    rs1 = Reducer(part, other_in, chip_sum, far_in, near_in, last_in, rs1_send, rs1_recv)
    attn = attn_ref[...]
    for item in plan1:
        put_part(item[1], jnp.dot(attn, wo_ref[0, :, item[1]], preferred_element_type=F32))
        if item[0] == 0:
            enter(4)
        rs1.begin(*item)
    feed(1)
    for stage, n in ((rs1.far, 0), (rs1.near, 4), (rs1.third, 3)):
        for item in plan1:
            stage(*item)
        feed(n)
    for item in plan1:
        cols = item[1]
        x1_buf[:, cols] = (x_buf[:, cols].astype(F32) + rs1.last(*item)).astype(BF16)
    rs1.finish()
    h_buf[me] = norm_rows(x1_buf[...].astype(F32), gain_ref[...].astype(F32))
    gather_rows(h_buf, ag_send, ag_recv, queue)

    def gate_up(i, carry):
        weight(0, i).wait()
        weight(1, i).wait()
        h_all = h_buf[...].reshape(n_tok, width)
        gate = jnp.dot(h_all, w1_buf[i], preferred_element_type=F32)
        up = jnp.dot(h_all, w3_buf[i], preferred_element_type=F32)
        act_buf[:, pl.ds(pl.multiple_of(i * chunk, 128), chunk)] = (gate * jax.nn.sigmoid(gate) * up).astype(BF16)
        return carry

    lax.fori_loop(0, n_chunks, gate_up, 0)

    rs2 = Reducer(part, other_in, chip_sum, far_in, near_in, last_in, rs2_send, rs2_recv)
    plan2 = plan(n_chunks, RS2_STRAIGHT)
    for j in range(n_chunks + RS2_LAG):
        if j < n_chunks:
            weight(2, j).wait()
            put_part(plan2[j][1], jnp.dot(act_buf[...], w2_buf[j], preferred_element_type=F32))
            rs2.begin(*plan2[j])
        if j >= RS2_LAG:
            rs2.far(*plan2[j - RS2_LAG])
            rs2.near(*plan2[j - RS2_LAG])
            if plan2[j - RS2_LAG][3]:
                rs2.third(*plan2[j - RS2_LAG])
    for item in plan2:
        if not item[3]:
            rs2.third(*item)
    for item in plan2:
        cols = item[1]
        out_ref[:, cols] = (x1_buf[:, cols].astype(F32) + rs2.last(*item)).astype(BF16)
    rs2.finish()


def shape(dims, dtype=BF16):
    return jax.ShapeDtypeStruct(dims, dtype)


def to_tiles(cache):
    _, n_tok, n_rows, n_heads, head = cache.shape
    halves = head // LANES
    return cache.reshape(n_tok, n_rows, n_heads, halves, LANES).transpose(0, 1, 3, 2, 4).reshape(n_tok, n_rows * halves * n_heads, LANES)


def from_tiles(tiles, like):
    _, n_tok, n_rows, n_heads, head = like.shape
    halves = head // LANES
    return tiles.reshape(n_tok, n_rows, halves, n_heads, LANES).transpose(0, 1, 3, 2, 4).reshape(like.shape)


def run_qkv(x, gain, pos2, wq, wk, wv, k_tiles, v_tiles):
    n_tok = k_tiles.shape[0]
    rows, width = x.shape
    cols = wq.shape[2]
    blocks = n_tok // rows
    dma = pltpu.SemaphoreType.DMA
    args = (x, gain, pos2, wq, wk, wv, k_tiles, v_tiles)
    return pl.pallas_call(
        qkv_kernel,
        out_shape=[shape((n_tok, cols))] * 3 + [shape(k_tiles.shape)] * 2 + [shape((cols // (2 * LANES) * n_tok, LANES), F32)],
        in_specs=[HBM] * len(args),
        out_specs=[VMEM] * 6,
        scratch_shapes=[
            pltpu.VMEM((2, n_tok, LANES), F32), pltpu.VMEM((rows, width), BF16), pltpu.VMEM(gain.shape, BF16), pltpu.VMEM(pos2.shape, pos2.dtype),
            pltpu.VMEM((blocks, rows, width), BF16), pltpu.VMEM((3, width, cols), BF16),
            dma((6,)), dma((2, 8)), dma((GATHER_SEMS,)), dma((GATHER_SEMS,))],
        compiler_params=pltpu.CompilerParams(collective_id=0, has_side_effects=True, vmem_limit_bytes=36 << 20),
        name='gather_qkv',
    )(*(pltpu.with_memory_space_constraint(a, pltpu.HBM) for a in args))


def run_attn(pos2, pos_rows, q, k, v, k_tiles, v_tiles):
    n_tok = k_tiles.shape[0]
    rows2 = q.shape[1] // (2 * LANES) * n_tok
    dma = pltpu.SemaphoreType.DMA
    wide = pltpu.VMEM((2, rows2, LANES), F32)
    tiles = shape(k_tiles.shape)
    attn, _, _, k_out, v_out = pl.pallas_call(
        attn_kernel,
        out_shape=[shape(q.shape), tiles, tiles, tiles, tiles],
        in_specs=[HBM, VMEM, VMEM, VMEM, VMEM, VMEM, VMEM],
        out_specs=[VMEM, VMEM, VMEM, HBM, HBM],
        scratch_shapes=[
            pltpu.SMEM(pos2.shape, pos2.dtype), pltpu.VMEM((2, n_tok * 8, LANES), F32), wide, wide,
            pltpu.VMEM((TOK_STEP // TOK_UNIT, 4 * TOK_SUB, k_tiles.shape[1]), F32), pltpu.VMEM((TOK_STEP // TOK_UNIT, 8 * TOK_SUB, k_tiles.shape[1]), F32),
            dma, dma((2, n_tok // TOK_STEP))],
        input_output_aliases={5: 1, 6: 2},
        compiler_params=pltpu.CompilerParams(vmem_limit_bytes=24 << 20),
        name='attention',
    )(pltpu.with_memory_space_constraint(pos2, pltpu.HBM), pos_rows, q, k, v, k_tiles, v_tiles)
    return attn, k_out, v_out


def run_mlp(attn, x, gain, wo, w1, w3, w2):
    rows, width = x.shape
    n_tok = attn.shape[0]
    ffn = w1.shape[2]
    chunk = MLP_CHUNK
    n_chunks = ffn // chunk
    dma = pltpu.SemaphoreType.DMA
    block = pltpu.VMEM((rows, width), BF16)
    chips = pltpu.VMEM((CHIPS, rows, width), BF16)
    return pl.pallas_call(
        mlp_kernel,
        out_shape=pltpu.VMEM((rows, width), BF16),
        in_specs=[VMEM, VMEM, VMEM, VMEM, HBM, HBM, HBM],
        out_specs=VMEM,
        scratch_shapes=[
            pltpu.VMEM((CHIPS, 2, rows, width), BF16), chips, chips, block, block, block,
            block, pltpu.VMEM((n_tok // rows, rows, width), BF16), pltpu.VMEM((n_tok, ffn), BF16),
            pltpu.VMEM((n_chunks, width, chunk), BF16), pltpu.VMEM((n_chunks, width, chunk), BF16), pltpu.VMEM((width // chunk, ffn, chunk), BF16),
            dma((3, n_chunks)), dma((7, RS1_PIECES)), dma((7, RS1_PIECES)), dma((GATHER_SEMS,)), dma((GATHER_SEMS,)),
            dma((7, n_chunks)), dma((7, n_chunks))],
        compiler_params=pltpu.CompilerParams(collective_id=1, has_side_effects=True, vmem_limit_bytes=MLP_VMEM),
        name='reduce_mlp',
    )(*(pltpu.with_memory_space_constraint(a, pltpu.VMEM) for a in (attn, x, gain, wo)), w1, w3, w2)


def solution(mesh):
    row_spec = P(('data', 'model'), None)
    cache_spec = P(None, 'data', None, 'model', None)
    col_spec = P(None, None, 'model')
    inner_spec = P(None, 'model', None)
    in_specs = (row_spec, P('data'), P(), P(), col_spec, col_spec, col_spec, inner_spec, col_spec, col_spec, inner_spec, cache_spec, cache_spec)
    out_specs = (row_spec, cache_spec, cache_spec)

    def device_step(hidden, positions, attn_gain, mlp_gain, w_query, w_key, w_value, w_out, w_gate, w_up, w_down, k_cache, v_cache):
        n_tok = positions.shape[0]
        pos2 = positions.reshape(1, n_tok)
        q, k, v, k_tiles, v_tiles, pos_rows = run_qkv(hidden, attn_gain, pos2, w_query, w_key, w_value, to_tiles(k_cache), to_tiles(v_cache))
        attn, k_out, v_out = run_attn(pos2, pos_rows, q, k, v, k_tiles, v_tiles)
        out = run_mlp(attn, hidden, mlp_gain, w_out, w_gate, w_up, w_down)
        return out, from_tiles(k_out, k_cache), from_tiles(v_out, v_cache)

    return jax.shard_map(device_step, mesh=mesh, in_specs=in_specs, out_specs=out_specs, check_vma=False)
```

```python
import functools
import math
import jax
import jax.numpy as jnp
from jax import lax
from jax.experimental import pallas as pl
from jax.experimental.pallas import tpu as pltpu
from jax.sharding import PartitionSpec as P

NORM_EPS = 1e-5
ROPE_BASE = 10000.0
BF16 = jnp.bfloat16
F32 = jnp.float32
VMEM = pl.BlockSpec(memory_space=pltpu.VMEM)
HBM = pl.BlockSpec(memory_space=pltpu.HBM)
MLP_VMEM = 61600000
CHIPS = 4
MLP_CHUNK = 512
RS1_PIECES = 4
RS2_LAG = 2
RS2_STRAIGHT = 3
GATHER_SEMS = 21


def places():
    me = lax.axis_index('model')
    core = lax.rem(me, 2)
    chip = lax.div(me, 2)
    other = me + 1 - 2 * core
    right = lax.rem(chip + 1, CHIPS) * 2 + core
    left = lax.rem(chip + CHIPS - 1, CHIPS) * 2 + core
    return me, core, chip, other, right, left


def knock(*peers):
    barrier = pltpu.get_barrier_semaphore()
    for peer in peers:
        pl.semaphore_signal(barrier, inc=1, device_id={'model': peer})


def enter(peers):
    pl.semaphore_wait(pltpu.get_barrier_semaphore(), peers)


def remote(src, dst, send_sem, recv_sem, peer):
    return pltpu.make_async_remote_copy(src_ref=src, dst_ref=dst, send_sem=send_sem, recv_sem=recv_sem, device_id={'model': peer})


def norm_rows(x_f, gain_f):
    inv_rms = lax.rsqrt(jnp.mean(x_f * x_f, axis=-1, keepdims=True) + NORM_EPS)
    return (x_f * inv_rms * gain_f).astype(BF16)


def gather_rows(buf, send_sems, recv_sems, behind=(), meanwhile=None):
    me, core, chip, other, right, left = places()
    width = buf.shape[2]
    quarter = width // 4
    q0, q1, q2, q3 = (pl.ds(i * quarter, quarter) for i in range(4))
    lo, hi, full = pl.ds(0, 2 * quarter), pl.ds(2 * quarter, 2 * quarter), pl.ds(0, width)
    far = lax.rem(chip + 2, CHIPS) * 2 + core
    sends = []

    def hop(blk, cols, idx, peer):
        view = buf.at[blk, :, cols]
        return remote(view, view, send_sems.at[idx], recv_sems.at[idx], peer)

    def arrive(blk, cols, idx):
        hop(blk, cols, idx, other).wait_recv()

    def send(blk, cols, idx, peer):
        copy = hop(blk, cols, idx, peer)
        copy.start()
        sends.append(copy)

    for cols, idx, peer in ((q0, 0, right), (q2, 1, left), (q1, 2, right), (q3, 3, left), (hi, 4, right), (lo, 5, left), (full, 6, other)):
        send(me, cols, idx, peer)
    across = []
    behind = list(behind)
    share = -(-len(behind) // 8)
    for copy in behind[:2 * share]:
        copy.start()
    behind = behind[2 * share:]
    if meanwhile is not None:
        meanwhile()
    for blk, cols, idx, onward, peer in (
            (left, q0, 0, 7, right), (right, q2, 1, 8, left), (left, q1, 2, 9, right), (right, q3, 3, 10, left),
            (left, hi, 4, None, None), (right, lo, 5, None, None),
            (far, q0, 7, None, None), (far, q2, 8, None, None), (far, q1, 9, None, None), (far, q3, 10, None, None)):
        arrive(blk, cols, idx)
        if onward is not None:
            send(blk, cols, onward, peer)
        send(blk, cols, 11 + len(across), other)
        across.append((blk + 1 - 2 * core, cols, 11 + len(across)))
        for copy in behind[:share]:
            copy.start()
        behind = behind[share:]
    arrive(other, full, 6)
    for item in across:
        arrive(*item)
    for copy in sends:
        copy.wait_send()


LANES = 128


def qkv_kernel(x_hbm, gain_hbm, pos_hbm, wq_hbm, wk_hbm, wv_hbm, kc_hbm, vc_hbm, q_ref, k_ref, v_ref, kb_ref, vb_ref, pc_ref,
               trig_buf, x_buf, gain_ref, pos_ref, h_buf, w_buf, load_sems, cache_sems, send_sems, recv_sems):
    me, core, chip, other, right, left = places()
    knock(other, right, left)
    loads = [pltpu.make_async_copy(src, dst, load_sems.at[3 + i]) for i, (src, dst) in enumerate(((x_hbm, x_buf), (gain_hbm, gain_ref), (pos_hbm, pos_ref)))]
    w_copies = [pltpu.make_async_copy(w.at[0], w_buf.at[i], load_sems.at[i]) for i, w in enumerate((wq_hbm, wk_hbm, wv_hbm))]
    pieces = cache_sems.shape[1]
    piece = kb_ref.shape[0] // pieces
    cache_in = []
    for kv, (hbm, buf) in enumerate(((kc_hbm, kb_ref), (vc_hbm, vb_ref))):
        for p in range(pieces):
            toks = pl.ds(p * piece, piece)
            cache_in.append(pltpu.make_async_copy(hbm.at[toks], buf.at[toks], cache_sems.at[kv, p]))
    for copy in loads:
        copy.start()
    for copy in loads:
        copy.wait()
    h_buf[me] = norm_rows(x_buf[...].astype(F32), gain_ref[...].astype(F32))
    enter(3)
    n_tok = pos_ref.shape[1]
    half = LANES
    head = 2 * half
    pos_f = pos_ref[...].astype(F32)

    def pick(rows, per):
        own = lax.broadcasted_iota(jnp.int32, (rows, n_tok), 0) // per == lax.broadcasted_iota(jnp.int32, (rows, n_tok), 1)
        return jnp.sum(jnp.where(own, jnp.broadcast_to(pos_f, (rows, n_tok)), 0.0), axis=1, keepdims=True)

    def tables():
        lane = lax.broadcasted_iota(jnp.int32, (n_tok, half), 1).astype(F32)
        angles = pick(n_tok, 1) * jnp.exp(lane * (-2.0 * math.log(ROPE_BASE) / head))
        trig_buf[0] = jnp.cos(angles)
        trig_buf[1] = jnp.sin(angles)
        rows2 = pc_ref.shape[0]
        pc_ref[...] = jnp.broadcast_to(pick(rows2, rows2 // n_tok), pc_ref.shape)

    gather_rows(h_buf, send_sems, recv_sems, w_copies + cache_in, tables)
    cos_tab, sin_tab = trig_buf[0], trig_buf[1]
    h_all = h_buf[...].reshape(n_tok, h_buf.shape[2])
    for i, out_ref in enumerate((q_ref, k_ref, v_ref)):
        w_copies[i].wait()
        proj = jnp.dot(h_all, w_buf[i], preferred_element_type=F32).astype(BF16)
        if i == 2:
            out_ref[...] = proj
            continue
        for h0 in range(0, proj.shape[1], head):
            front = proj[:, h0:h0 + half].astype(F32)
            back = proj[:, h0 + half:h0 + head].astype(F32)
            out_ref[:, h0:h0 + half] = (front * cos_tab - back * sin_tab).astype(BF16)
            out_ref[:, h0 + half:h0 + head] = (back * cos_tab + front * sin_tab).astype(BF16)
    for copy in cache_in:
        copy.wait()


TOK_STEP = 16
TOK_UNIT = 8
TOK_SUB = 4


def attn_kernel(pos_hbm, pc_buf, q_ref, k_ref, v_ref, kb_in, vb_in, attn_ref, k_buf, v_buf, ko_hbm, vo_hbm,
                pos_smem, new_buf, q_buf, o_buf, score_buf, prob_buf, pos_sem, out_sems):
    n_tok, per_tok, lanes = k_buf.shape
    n_heads = 2
    head = q_ref.shape[1] // n_heads
    steps = n_tok // TOK_STEP
    bufs = (k_buf, v_buf)
    pos_copy = pltpu.make_async_copy(pos_hbm, pos_smem, pos_sem)
    pos_copy.start()

    def write_out(t):
        toks = pl.ds(t * TOK_STEP, TOK_STEP)
        return [pltpu.make_async_copy(buf.at[toks], hbm.at[toks], out_sems.at[kv, t]) for kv, (buf, hbm) in enumerate(zip(bufs, (ko_hbm, vo_hbm)))]

    for h in range(n_heads):
        for c in range(2):
            cols = slice(h * head + c * lanes, h * head + (c + 1) * lanes)
            q_buf.at[c][pl.ds(h, n_tok, stride=2), :] = q_ref[:, cols].astype(F32)
            for kv, ref in enumerate((k_ref, v_ref)):
                new = ref[:, cols].astype(F32)
                for again in range(2):
                    new_buf.at[kv][pl.ds(4 * again + 2 * c + h, n_tok, stride=8), :] = new
    tile_row = lax.broadcasted_iota(jnp.int32, (16, lanes), 0)
    sub = TOK_SUB * n_heads
    tok_of = (lax.broadcasted_iota(jnp.int32, (4 * sub, per_tok), 0) % sub) // 2
    row = lax.broadcasted_iota(jnp.int32, (2 * sub, per_tok), 0)
    col = lax.broadcasted_iota(jnp.int32, (2 * sub, per_tok), 1)
    counts = ((col & 2) == 0) & ((col & 1) == (row & 1))
    key_pos = (col >> 2).astype(F32)

    def shift(x, by):
        return jnp.concatenate([pltpu.roll(x[:, i:i + lanes], by % lanes, 1) for i in range(0, per_tok, lanes)], axis=1)

    def pair(buf, b0):
        one, two = (buf[pl.ds(b0 + g * TOK_SUB, TOK_SUB)] for g in range(2))
        return jnp.concatenate([x.reshape(TOK_SUB * per_tok, lanes) for x in (one, two)], axis=1)

    def out_rows(b0):
        return [pl.ds(pl.multiple_of(b0 * n_heads + g * sub, sub), sub) for g in range(2)]

    units = TOK_STEP // TOK_UNIT

    def mix(t, u):
        b0 = t * TOK_STEP + u * TOK_UNIT
        probs = prob_buf[u]
        wide = jnp.concatenate([jnp.where(tok_of == m, probs, 0.0) for m in range(TOK_SUB)], axis=1).astype(BF16)
        out = jnp.dot(wide, pair(v_buf, b0), preferred_element_type=F32).astype(BF16).astype(F32)
        rows = out_rows(b0)
        for g in range(2):
            for c in range(2):
                at = (2 * g + c) * sub
                o_buf[c, rows[g], :] = out[at:at + sub, g * lanes:(g + 1) * lanes]

    def soften(u):
        total = score_buf[u]
        e = jnp.exp(total - jnp.max(total, axis=1, keepdims=True))
        probs = (e / jnp.sum(e, axis=1, keepdims=True)).astype(BF16).astype(F32)
        moved = shift(probs, 2)
        prob_buf[u] = jnp.concatenate([probs[:sub], moved[:sub], probs[sub:], moved[sub:]], axis=0)

    def insert(t):
        for i in range(TOK_STEP):
            b = t * TOK_STEP + i
            pos = pos_smem[0, b]
            tile = pl.ds(pl.multiple_of((pos >> 2) * 16, 16), 16)
            hit = (tile_row >> 2) == (pos & 3)
            for kv in range(2):
                new = new_buf[kv, pl.ds(pl.multiple_of(b * 8, 8), 8), :]
                old = bufs[kv][b, tile, :].astype(F32)
                bufs[kv][b, tile, :] = jnp.where(hit, jnp.concatenate([new, new], axis=0), old).astype(BF16)

    def score(t, u):
        b0 = t * TOK_STEP + u * TOK_UNIT
        rows = out_rows(b0)
        none = jnp.zeros((sub, lanes), F32)
        q = jnp.concatenate(
            [jnp.concatenate([q_buf[c, rows[0], :], none], axis=1) for c in range(2)] +
            [jnp.concatenate([none, q_buf[c, rows[1], :]], axis=1) for c in range(2)], axis=0).astype(BF16)
        scores = lax.dot_general(q, pair(k_buf, b0), (((1,), (1,)), ((), ())), preferred_element_type=F32)
        mine = scores[:, :per_tok]
        for m in range(1, TOK_SUB):
            mine = jnp.where(tok_of == m, scores[:, m * per_tok:(m + 1) * per_tok], mine)
        first = jnp.concatenate([mine[:sub], mine[2 * sub:3 * sub]], axis=0)
        second = jnp.concatenate([mine[sub:2 * sub], mine[3 * sub:]], axis=0)
        total = (first + shift(second, -2)) * (head ** -0.5)
        pos_of = pc_buf[pl.ds(pl.multiple_of(b0 * n_heads, 2 * sub), 2 * sub), :]
        score_buf[u] = jnp.where(counts & (key_pos <= jnp.concatenate([pos_of] * (per_tok // lanes), axis=1)), total, -1e30)

    def send(t):
        for copy in write_out(t):
            copy.start()

    def each(stage, *args):
        for u in range(units):
            stage(*args, u)

    pos_copy.wait()
    insert(0)

    def place(t, carry):
        insert(t)
        send(t - 1)
        return carry

    lax.fori_loop(1, steps, place, 0)
    each(score, 0)
    send(steps - 1)
    each(soften)
    each(score, 1)

    def step(t, carry):
        each(mix, t - 2)
        each(soften)
        each(score, t)
        return carry

    lax.fori_loop(2, steps, step, 0)
    each(mix, steps - 2)
    each(soften)
    each(mix, steps - 1)
    attn_ref[...] = jnp.concatenate([o_buf.at[c][pl.ds(h, n_tok, stride=2), :] for h in range(n_heads) for c in range(2)], axis=1).astype(BF16)
    for t in range(steps):
        for copy in write_out(t):
            copy.wait()


class Reducer:
    def __init__(self, part, from_other, chip_sum, far_in, near_in, last_in, send_sems, recv_sems):
        self.part, self.from_other, self.chip_sum = part, from_other, chip_sum
        self.far_in, self.near_in, self.last_in = far_in, near_in, last_in
        self.send_sems, self.recv_sems = send_sems, recv_sems
        self.me, self.core, self.chip, self.other, self.right, self.left = places()
        self.sends = []

    def copy(self, kind, j, cols, way, direct):
        nxt, prv = (self.right, self.left) if way > 0 else (self.left, self.right)
        ahead = lax.rem(self.chip + CHIPS + way, CHIPS)
        behind = lax.rem(self.chip + CHIPS - way, CHIPS)
        opposite = lax.rem(self.chip + 2, CHIPS)
        if kind < 4:
            k = (opposite, behind, ahead, self.chip)[kind]
            src, dst, peer = self.part.at[k, 1 - self.core, :, cols], self.from_other.at[k, :, cols], self.other
        else:
            src, dst, peer = (
                (self.chip_sum.at[opposite, :, cols], self.far_in.at[:, cols], opposite * 2 + self.core if direct else nxt),
                (self.chip_sum.at[behind, :, cols], self.near_in.at[:, cols], prv),
                (self.chip_sum.at[ahead, :, cols], self.last_in.at[:, cols], nxt),
            )[kind - 4]
        return remote(src, dst, self.send_sems.at[kind, j], self.recv_sems.at[kind, j], peer)

    def go(self, kind, j, cols, way, direct):
        copy = self.copy(kind, j, cols, way, direct)
        copy.start()
        self.sends.append(copy)

    def begin(self, j, cols, way, direct):
        for kind in range(4):
            self.go(kind, j, cols, way, direct)

    def pair(self, kind, k, j, cols, way, direct):
        self.copy(kind, j, cols, way, direct).wait_recv()
        return self.part[k, self.core, :, cols].astype(F32) + self.from_other[k, :, cols].astype(F32)

    def far(self, j, cols, way, direct):
        opposite = lax.rem(self.chip + 2, CHIPS)
        self.chip_sum[opposite, :, cols] = self.pair(0, opposite, j, cols, way, direct).astype(BF16)
        self.go(4, j, cols, way, direct)

    def near(self, j, cols, way, direct):
        behind = lax.rem(self.chip + CHIPS - way, CHIPS)
        self.chip_sum[behind, :, cols] = self.pair(1, behind, j, cols, way, direct).astype(BF16)
        self.go(5, j, cols, way, direct)

    def third(self, j, cols, way, direct):
        ahead = lax.rem(self.chip + CHIPS + way, CHIPS)
        mine = self.pair(2, ahead, j, cols, way, direct)
        if not direct:
            self.copy(4, j, cols, way, direct).wait_recv()
            mine = mine + self.far_in[:, cols].astype(F32)
        self.chip_sum[ahead, :, cols] = mine.astype(BF16)
        self.go(6, j, cols, way, direct)

    def last(self, j, cols, way, direct):
        own = self.pair(3, self.chip, j, cols, way, direct)
        self.copy(5, j, cols, way, direct).wait_recv()
        own = own + self.near_in[:, cols].astype(F32)
        if direct:
            self.copy(4, j, cols, way, direct).wait_recv()
            own = own + self.far_in[:, cols].astype(F32)
        self.copy(6, j, cols, way, direct).wait_recv()
        return own + self.last_in[:, cols].astype(F32)

    def finish(self):
        for copy in self.sends:
            copy.wait_send()


def mlp_kernel(attn_ref, x_buf, gain_ref, wo_ref, w1_hbm, w3_hbm, w2_hbm, out_ref,
               part, other_in, chip_sum, far_in, near_in, last_in,
               x1_buf, h_buf, act_buf, w1_buf, w3_buf, w2_buf,
               w_sems, rs1_send, rs1_recv, ag_send, ag_recv, rs2_send, rs2_recv):
    me, core, chip, other, right, left = places()
    knock(other, right, left, lax.rem(chip + 2, CHIPS) * 2 + core)
    width = x_buf.shape[1]
    n_tok = act_buf.shape[0]
    n_chunks = w1_buf.shape[0]
    chunk = w1_buf.shape[2]

    def weight(kind, i):
        src = (w1_hbm, w3_hbm, w2_hbm)[kind]
        dst = (w1_buf, w3_buf, w2_buf)[kind]
        return pltpu.make_async_copy(src.at[0, :, pl.ds(pl.multiple_of(i * chunk, 128), chunk)], dst.at[i], w_sems.at[kind, i])

    queue = [weight(kind, i) for i in range(n_chunks) for kind in range(2)] + [weight(2, i) for i in range(n_chunks)]

    def feed(n):
        for copy in queue[:n]:
            copy.start()
        del queue[:n]

    feed(2)

    def plan(pieces, straight=0):
        size = width // pieces
        return [(j, pl.ds(j * size, size), 1 if j % 2 == 0 else -1, j >= pieces - straight) for j in range(pieces)]

    def put_part(cols, value):
        part[:, :, :, cols] = value.astype(BF16).reshape(CHIPS, 2, n_tok // (2 * CHIPS), value.shape[1])

    plan1 = plan(RS1_PIECES)
    rs1 = Reducer(part, other_in, chip_sum, far_in, near_in, last_in, rs1_send, rs1_recv)
    attn = attn_ref[...]
    for item in plan1:
        put_part(item[1], jnp.dot(attn, wo_ref[0, :, item[1]], preferred_element_type=F32))
        if item[0] == 0:
            enter(4)
        rs1.begin(*item)
    feed(1)
    for stage, n in ((rs1.far, 0), (rs1.near, 4), (rs1.third, 3)):
        for item in plan1:
            stage(*item)
        feed(n)
    for item in plan1:
        cols = item[1]
        x1_buf[:, cols] = (x_buf[:, cols].astype(F32) + rs1.last(*item)).astype(BF16)
    rs1.finish()
    h_buf[me] = norm_rows(x1_buf[...].astype(F32), gain_ref[...].astype(F32))
    gather_rows(h_buf, ag_send, ag_recv, queue)

    def gate_up(i, carry):
        weight(0, i).wait()
        weight(1, i).wait()
        h_all = h_buf[...].reshape(n_tok, width)
        gate = jnp.dot(h_all, w1_buf[i], preferred_element_type=F32)
        up = jnp.dot(h_all, w3_buf[i], preferred_element_type=F32)
        act_buf[:, pl.ds(pl.multiple_of(i * chunk, 128), chunk)] = (gate * jax.nn.sigmoid(gate) * up).astype(BF16)
        return carry

    lax.fori_loop(0, n_chunks, gate_up, 0)

    rs2 = Reducer(part, other_in, chip_sum, far_in, near_in, last_in, rs2_send, rs2_recv)
    plan2 = plan(n_chunks, RS2_STRAIGHT)
    for j in range(n_chunks + RS2_LAG):
        if j < n_chunks:
            weight(2, j).wait()
            put_part(plan2[j][1], jnp.dot(act_buf[...], w2_buf[j], preferred_element_type=F32))
            rs2.begin(*plan2[j])
        if j >= RS2_LAG:
            rs2.far(*plan2[j - RS2_LAG])
            rs2.near(*plan2[j - RS2_LAG])
            if plan2[j - RS2_LAG][3]:
                rs2.third(*plan2[j - RS2_LAG])
    for item in plan2:
        if not item[3]:
            rs2.third(*item)
    for item in plan2:
        cols = item[1]
        out_ref[:, cols] = (x1_buf[:, cols].astype(F32) + rs2.last(*item)).astype(BF16)
    rs2.finish()


def shape(dims, dtype=BF16):
    return jax.ShapeDtypeStruct(dims, dtype)


def to_tiles(cache):
    _, n_tok, n_rows, n_heads, head = cache.shape
    halves = head // LANES
    return cache.reshape(n_tok, n_rows, n_heads, halves, LANES).transpose(0, 1, 3, 2, 4).reshape(n_tok, n_rows * halves * n_heads, LANES)


def from_tiles(tiles, like):
    _, n_tok, n_rows, n_heads, head = like.shape
    halves = head // LANES
    return tiles.reshape(n_tok, n_rows, halves, n_heads, LANES).transpose(0, 1, 3, 2, 4).reshape(like.shape)


def run_qkv(x, gain, pos2, wq, wk, wv, k_tiles, v_tiles):
    n_tok = k_tiles.shape[0]
    rows, width = x.shape
    cols = wq.shape[2]
    blocks = n_tok // rows
    dma = pltpu.SemaphoreType.DMA
    args = (x, gain, pos2, wq, wk, wv, k_tiles, v_tiles)
    return pl.pallas_call(
        qkv_kernel,
        out_shape=[shape((n_tok, cols))] * 3 + [shape(k_tiles.shape)] * 2 + [shape((cols // (2 * LANES) * n_tok, LANES), F32)],
        in_specs=[HBM] * len(args),
        out_specs=[VMEM] * 6,
        scratch_shapes=[
            pltpu.VMEM((2, n_tok, LANES), F32), pltpu.VMEM((rows, width), BF16), pltpu.VMEM(gain.shape, BF16), pltpu.VMEM(pos2.shape, pos2.dtype),
            pltpu.VMEM((blocks, rows, width), BF16), pltpu.VMEM((3, width, cols), BF16),
            dma((6,)), dma((2, 8)), dma((GATHER_SEMS,)), dma((GATHER_SEMS,))],
        compiler_params=pltpu.CompilerParams(collective_id=0, has_side_effects=True, vmem_limit_bytes=36 << 20),
        name='gather_qkv',
    )(*(pltpu.with_memory_space_constraint(a, pltpu.HBM) for a in args))


def run_attn(pos2, pos_rows, q, k, v, k_tiles, v_tiles):
    n_tok = k_tiles.shape[0]
    rows2 = q.shape[1] // (2 * LANES) * n_tok
    dma = pltpu.SemaphoreType.DMA
    wide = pltpu.VMEM((2, rows2, LANES), F32)
    tiles = shape(k_tiles.shape)
    attn, _, _, k_out, v_out = pl.pallas_call(
        attn_kernel,
        out_shape=[shape(q.shape), tiles, tiles, tiles, tiles],
        in_specs=[HBM, VMEM, VMEM, VMEM, VMEM, VMEM, VMEM],
        out_specs=[VMEM, VMEM, VMEM, HBM, HBM],
        scratch_shapes=[
            pltpu.SMEM(pos2.shape, pos2.dtype), pltpu.VMEM((2, n_tok * 8, LANES), F32), wide, wide,
            pltpu.VMEM((TOK_STEP // TOK_UNIT, 4 * TOK_SUB, k_tiles.shape[1]), F32), pltpu.VMEM((TOK_STEP // TOK_UNIT, 8 * TOK_SUB, k_tiles.shape[1]), F32),
            dma, dma((2, n_tok // TOK_STEP))],
        input_output_aliases={5: 1, 6: 2},
        compiler_params=pltpu.CompilerParams(vmem_limit_bytes=24 << 20),
        name='attention',
    )(pltpu.with_memory_space_constraint(pos2, pltpu.HBM), pos_rows, q, k, v, k_tiles, v_tiles)
    return attn, k_out, v_out


def run_mlp(attn, x, gain, wo, w1, w3, w2):
    rows, width = x.shape
    n_tok = attn.shape[0]
    ffn = w1.shape[2]
    chunk = MLP_CHUNK
    n_chunks = ffn // chunk
    dma = pltpu.SemaphoreType.DMA
    block = pltpu.VMEM((rows, width), BF16)
    chips = pltpu.VMEM((CHIPS, rows, width), BF16)
    return pl.pallas_call(
        mlp_kernel,
        out_shape=pltpu.VMEM((rows, width), BF16),
        in_specs=[VMEM, VMEM, VMEM, VMEM, HBM, HBM, HBM],
        out_specs=VMEM,
        scratch_shapes=[
            pltpu.VMEM((CHIPS, 2, rows, width), BF16), chips, chips, block, block, block,
            block, pltpu.VMEM((n_tok // rows, rows, width), BF16), pltpu.VMEM((n_tok, ffn), BF16),
            pltpu.VMEM((n_chunks, width, chunk), BF16), pltpu.VMEM((n_chunks, width, chunk), BF16), pltpu.VMEM((width // chunk, ffn, chunk), BF16),
            dma((3, n_chunks)), dma((7, RS1_PIECES)), dma((7, RS1_PIECES)), dma((GATHER_SEMS,)), dma((GATHER_SEMS,)),
            dma((7, n_chunks)), dma((7, n_chunks))],
        compiler_params=pltpu.CompilerParams(collective_id=1, has_side_effects=True, vmem_limit_bytes=MLP_VMEM),
        name='reduce_mlp',
    )(*(pltpu.with_memory_space_constraint(a, pltpu.VMEM) for a in (attn, x, gain, wo)), w1, w3, w2)


def solution(mesh):
    row_spec = P(('data', 'model'), None)
    cache_spec = P(None, 'data', None, 'model', None)
    col_spec = P(None, None, 'model')
    inner_spec = P(None, 'model', None)
    in_specs = (row_spec, P('data'), P(), P(), col_spec, col_spec, col_spec, inner_spec, col_spec, col_spec, inner_spec, cache_spec, cache_spec)
    out_specs = (row_spec, cache_spec, cache_spec)

    def device_step(hidden, positions, attn_gain, mlp_gain, w_query, w_key, w_value, w_out, w_gate, w_up, w_down, k_cache, v_cache):
        n_tok = positions.shape[0]
        pos2 = positions.reshape(1, n_tok)
        q, k, v, k_tiles, v_tiles, pos_rows = run_qkv(hidden, attn_gain, pos2, w_query, w_key, w_value, to_tiles(k_cache), to_tiles(v_cache))
        attn, k_out, v_out = run_attn(pos2, pos_rows, q, k, v, k_tiles, v_tiles)
        out = run_mlp(attn, hidden, mlp_gain, w_out, w_gate, w_up, w_down)
        return out, from_tiles(k_out, k_cache), from_tiles(v_out, v_cache)

    return jax.shard_map(device_step, mesh=mesh, in_specs=in_specs, out_specs=out_specs, check_vma=False)
```

```python
import functools
import math
import jax
import jax.numpy as jnp
from jax import lax
from jax.experimental import pallas as pl
from jax.experimental.pallas import tpu as pltpu
from jax.sharding import PartitionSpec as P

NORM_EPS = 1e-5
ROPE_BASE = 10000.0
BF16 = jnp.bfloat16
F32 = jnp.float32
VMEM = pl.BlockSpec(memory_space=pltpu.VMEM)
HBM = pl.BlockSpec(memory_space=pltpu.HBM)
MLP_VMEM = 61600000
CHIPS = 4
MLP_CHUNK = 512
RS1_PIECES = 4
RS2_LAG = 2
RS2_STRAIGHT = 4
GATHER_SEMS = 21


def places():
    me = lax.axis_index('model')
    core = lax.rem(me, 2)
    chip = lax.div(me, 2)
    other = me + 1 - 2 * core
    right = lax.rem(chip + 1, CHIPS) * 2 + core
    left = lax.rem(chip + CHIPS - 1, CHIPS) * 2 + core
    return me, core, chip, other, right, left


def knock(*peers):
    barrier = pltpu.get_barrier_semaphore()
    for peer in peers:
        pl.semaphore_signal(barrier, inc=1, device_id={'model': peer})


def enter(peers):
    pl.semaphore_wait(pltpu.get_barrier_semaphore(), peers)


def remote(src, dst, send_sem, recv_sem, peer):
    return pltpu.make_async_remote_copy(src_ref=src, dst_ref=dst, send_sem=send_sem, recv_sem=recv_sem, device_id={'model': peer})


def norm_rows(x_f, gain_f):
    inv_rms = lax.rsqrt(jnp.mean(x_f * x_f, axis=-1, keepdims=True) + NORM_EPS)
    return (x_f * inv_rms * gain_f).astype(BF16)


def gather_rows(buf, send_sems, recv_sems, behind=(), meanwhile=None):
    me, core, chip, other, right, left = places()
    width = buf.shape[2]
    quarter = width // 4
    q0, q1, q2, q3 = (pl.ds(i * quarter, quarter) for i in range(4))
    lo, hi, full = pl.ds(0, 2 * quarter), pl.ds(2 * quarter, 2 * quarter), pl.ds(0, width)
    far = lax.rem(chip + 2, CHIPS) * 2 + core
    sends = []

    def hop(blk, cols, idx, peer):
        view = buf.at[blk, :, cols]
        return remote(view, view, send_sems.at[idx], recv_sems.at[idx], peer)

    def arrive(blk, cols, idx):
        hop(blk, cols, idx, other).wait_recv()

    def send(blk, cols, idx, peer):
        copy = hop(blk, cols, idx, peer)
        copy.start()
        sends.append(copy)

    for cols, idx, peer in (
            (q0, 0, right), (q2, 1, left), (q1, 9, far), (q3, 10, far), (q1, 2, right), (q3, 3, left), (hi, 4, right), (lo, 5, left),
            (full, 6, other)):
        send(me, cols, idx, peer)
    across = []
    behind = list(behind)
    share = -(-len(behind) // 8)
    for copy in behind[:2 * share]:
        copy.start()
    behind = behind[2 * share:]
    if meanwhile is not None:
        meanwhile()
    for blk, cols, idx, onward, peer in (
            (left, q0, 0, 7, right), (right, q2, 1, 8, left), (left, q1, 2, None, None), (right, q3, 3, None, None),
            (left, hi, 4, None, None), (right, lo, 5, None, None),
            (far, q1, 9, None, None), (far, q3, 10, None, None), (far, q0, 7, None, None), (far, q2, 8, None, None)):
        arrive(blk, cols, idx)
        if onward is not None:
            send(blk, cols, onward, peer)
        send(blk, cols, 11 + len(across), other)
        across.append((blk + 1 - 2 * core, cols, 11 + len(across)))
        for copy in behind[:share]:
            copy.start()
        behind = behind[share:]
    arrive(other, full, 6)
    for item in across:
        arrive(*item)
    for copy in sends:
        copy.wait_send()


LANES = 128


def qkv_kernel(x_hbm, gain_hbm, pos_hbm, wq_hbm, wk_hbm, wv_hbm, kc_hbm, vc_hbm, q_ref, k_ref, v_ref, kb_ref, vb_ref, pc_ref,
               trig_buf, x_buf, gain_ref, pos_ref, h_buf, w_buf, load_sems, cache_sems, send_sems, recv_sems):
    me, core, chip, other, right, left = places()
    knock(other, right, left, lax.rem(chip + 2, CHIPS) * 2 + core)
    loads = [pltpu.make_async_copy(src, dst, load_sems.at[3 + i]) for i, (src, dst) in enumerate(((x_hbm, x_buf), (gain_hbm, gain_ref), (pos_hbm, pos_ref)))]
    w_copies = [pltpu.make_async_copy(w.at[0], w_buf.at[i], load_sems.at[i]) for i, w in enumerate((wq_hbm, wk_hbm, wv_hbm))]
    pieces = cache_sems.shape[1]
    piece = kb_ref.shape[0] // pieces
    cache_in = []
    for kv, (hbm, buf) in enumerate(((kc_hbm, kb_ref), (vc_hbm, vb_ref))):
        for p in range(pieces):
            toks = pl.ds(p * piece, piece)
            cache_in.append(pltpu.make_async_copy(hbm.at[toks], buf.at[toks], cache_sems.at[kv, p]))
    for copy in loads:
        copy.start()
    for copy in loads:
        copy.wait()
    h_buf[me] = norm_rows(x_buf[...].astype(F32), gain_ref[...].astype(F32))
    enter(4)
    n_tok = pos_ref.shape[1]
    half = LANES
    head = 2 * half
    pos_f = pos_ref[...].astype(F32)

    def pick(rows, per):
        own = lax.broadcasted_iota(jnp.int32, (rows, n_tok), 0) // per == lax.broadcasted_iota(jnp.int32, (rows, n_tok), 1)
        return jnp.sum(jnp.where(own, jnp.broadcast_to(pos_f, (rows, n_tok)), 0.0), axis=1, keepdims=True)

    def tables():
        lane = lax.broadcasted_iota(jnp.int32, (n_tok, half), 1).astype(F32)
        angles = pick(n_tok, 1) * jnp.exp(lane * (-2.0 * math.log(ROPE_BASE) / head))
        trig_buf[0] = jnp.cos(angles)
        trig_buf[1] = jnp.sin(angles)
        rows2 = pc_ref.shape[0]
        pc_ref[...] = jnp.broadcast_to(pick(rows2, rows2 // n_tok), pc_ref.shape)

    gather_rows(h_buf, send_sems, recv_sems, w_copies + cache_in, tables)
    cos_tab, sin_tab = trig_buf[0], trig_buf[1]
    h_all = h_buf[...].reshape(n_tok, h_buf.shape[2])
    for i, out_ref in enumerate((q_ref, k_ref, v_ref)):
        w_copies[i].wait()
        proj = jnp.dot(h_all, w_buf[i], preferred_element_type=F32).astype(BF16)
        if i == 2:
            out_ref[...] = proj
            continue
        for h0 in range(0, proj.shape[1], head):
            front = proj[:, h0:h0 + half].astype(F32)
            back = proj[:, h0 + half:h0 + head].astype(F32)
            out_ref[:, h0:h0 + half] = (front * cos_tab - back * sin_tab).astype(BF16)
            out_ref[:, h0 + half:h0 + head] = (back * cos_tab + front * sin_tab).astype(BF16)
    for copy in cache_in:
        copy.wait()


TOK_STEP = 16
TOK_UNIT = 8
TOK_SUB = 4


def attn_kernel(pos_hbm, pc_buf, q_ref, k_ref, v_ref, kb_in, vb_in, attn_ref, k_buf, v_buf, ko_hbm, vo_hbm,
                pos_smem, new_buf, q_buf, o_buf, score_buf, prob_buf, pos_sem, out_sems):
    n_tok, per_tok, lanes = k_buf.shape
    n_heads = 2
    head = q_ref.shape[1] // n_heads
    steps = n_tok // TOK_STEP
    bufs = (k_buf, v_buf)
    pos_copy = pltpu.make_async_copy(pos_hbm, pos_smem, pos_sem)
    pos_copy.start()

    def write_out(t):
        toks = pl.ds(t * TOK_STEP, TOK_STEP)
        return [pltpu.make_async_copy(buf.at[toks], hbm.at[toks], out_sems.at[kv, t]) for kv, (buf, hbm) in enumerate(zip(bufs, (ko_hbm, vo_hbm)))]

    for h in range(n_heads):
        for c in range(2):
            cols = slice(h * head + c * lanes, h * head + (c + 1) * lanes)
            q_buf.at[c][pl.ds(h, n_tok, stride=2), :] = q_ref[:, cols].astype(F32)
            for kv, ref in enumerate((k_ref, v_ref)):
                new = ref[:, cols].astype(F32)
                for again in range(2):
                    new_buf.at[kv][pl.ds(4 * again + 2 * c + h, n_tok, stride=8), :] = new
    tile_row = lax.broadcasted_iota(jnp.int32, (16, lanes), 0)
    sub = TOK_SUB * n_heads
    tok_of = (lax.broadcasted_iota(jnp.int32, (4 * sub, per_tok), 0) % sub) // 2
    row = lax.broadcasted_iota(jnp.int32, (2 * sub, per_tok), 0)
    col = lax.broadcasted_iota(jnp.int32, (2 * sub, per_tok), 1)
    counts = ((col & 2) == 0) & ((col & 1) == (row & 1))
    key_pos = (col >> 2).astype(F32)

    def shift(x, by):
        return jnp.concatenate([pltpu.roll(x[:, i:i + lanes], by % lanes, 1) for i in range(0, per_tok, lanes)], axis=1)

    def pair(buf, b0):
        one, two = (buf[pl.ds(b0 + g * TOK_SUB, TOK_SUB)] for g in range(2))
        return jnp.concatenate([x.reshape(TOK_SUB * per_tok, lanes) for x in (one, two)], axis=1)

    def out_rows(b0):
        return [pl.ds(pl.multiple_of(b0 * n_heads + g * sub, sub), sub) for g in range(2)]

    units = TOK_STEP // TOK_UNIT

    def mix(t, u):
        b0 = t * TOK_STEP + u * TOK_UNIT
        probs = prob_buf[u]
        wide = jnp.concatenate([jnp.where(tok_of == m, probs, 0.0) for m in range(TOK_SUB)], axis=1).astype(BF16)
        out = jnp.dot(wide, pair(v_buf, b0), preferred_element_type=F32).astype(BF16).astype(F32)
        rows = out_rows(b0)
        for g in range(2):
            for c in range(2):
                at = (2 * g + c) * sub
                o_buf[c, rows[g], :] = out[at:at + sub, g * lanes:(g + 1) * lanes]

    def soften(u):
        total = score_buf[u]
        e = jnp.exp(total - jnp.max(total, axis=1, keepdims=True))
        probs = (e / jnp.sum(e, axis=1, keepdims=True)).astype(BF16).astype(F32)
        moved = shift(probs, 2)
        prob_buf[u] = jnp.concatenate([probs[:sub], moved[:sub], probs[sub:], moved[sub:]], axis=0)

    def insert(t):
        for i in range(TOK_STEP):
            b = t * TOK_STEP + i
            pos = pos_smem[0, b]
            tile = pl.ds(pl.multiple_of((pos >> 2) * 16, 16), 16)
            hit = (tile_row >> 2) == (pos & 3)
            for kv in range(2):
                new = new_buf[kv, pl.ds(pl.multiple_of(b * 8, 8), 8), :]
                old = bufs[kv][b, tile, :].astype(F32)
                bufs[kv][b, tile, :] = jnp.where(hit, jnp.concatenate([new, new], axis=0), old).astype(BF16)

    def score(t, u):
        b0 = t * TOK_STEP + u * TOK_UNIT
        rows = out_rows(b0)
        none = jnp.zeros((sub, lanes), F32)
        q = jnp.concatenate(
            [jnp.concatenate([q_buf[c, rows[0], :], none], axis=1) for c in range(2)] +
            [jnp.concatenate([none, q_buf[c, rows[1], :]], axis=1) for c in range(2)], axis=0).astype(BF16)
        scores = lax.dot_general(q, pair(k_buf, b0), (((1,), (1,)), ((), ())), preferred_element_type=F32)
        mine = scores[:, :per_tok]
        for m in range(1, TOK_SUB):
            mine = jnp.where(tok_of == m, scores[:, m * per_tok:(m + 1) * per_tok], mine)
        first = jnp.concatenate([mine[:sub], mine[2 * sub:3 * sub]], axis=0)
        second = jnp.concatenate([mine[sub:2 * sub], mine[3 * sub:]], axis=0)
        total = (first + shift(second, -2)) * (head ** -0.5)
        pos_of = pc_buf[pl.ds(pl.multiple_of(b0 * n_heads, 2 * sub), 2 * sub), :]
        score_buf[u] = jnp.where(counts & (key_pos <= jnp.concatenate([pos_of] * (per_tok // lanes), axis=1)), total, -1e30)

    def send(t):
        for copy in write_out(t):
            copy.start()

    def each(stage, *args):
        for u in range(units):
            stage(*args, u)

    pos_copy.wait()
    insert(0)

    def place(t, carry):
        insert(t)
        send(t - 1)
        return carry

    lax.fori_loop(1, steps, place, 0)
    each(score, 0)
    send(steps - 1)
    each(soften)
    each(score, 1)

    def step(t, carry):
        each(mix, t - 2)
        each(soften)
        each(score, t)
        return carry

    lax.fori_loop(2, steps, step, 0)
    each(mix, steps - 2)
    each(soften)
    each(mix, steps - 1)
    attn_ref[...] = jnp.concatenate([o_buf.at[c][pl.ds(h, n_tok, stride=2), :] for h in range(n_heads) for c in range(2)], axis=1).astype(BF16)
    for t in range(steps):
        for copy in write_out(t):
            copy.wait()


class Reducer:
    def __init__(self, part, from_other, chip_sum, far_in, near_in, last_in, send_sems, recv_sems):
        self.part, self.from_other, self.chip_sum = part, from_other, chip_sum
        self.far_in, self.near_in, self.last_in = far_in, near_in, last_in
        self.send_sems, self.recv_sems = send_sems, recv_sems
        self.me, self.core, self.chip, self.other, self.right, self.left = places()
        self.sends = []

    def copy(self, kind, j, cols, way, direct):
        nxt, prv = (self.right, self.left) if way > 0 else (self.left, self.right)
        ahead = lax.rem(self.chip + CHIPS + way, CHIPS)
        behind = lax.rem(self.chip + CHIPS - way, CHIPS)
        opposite = lax.rem(self.chip + 2, CHIPS)
        if kind < 4:
            k = (opposite, behind, ahead, self.chip)[kind]
            src, dst, peer = self.part.at[k, 1 - self.core, :, cols], self.from_other.at[k, :, cols], self.other
        else:
            src, dst, peer = (
                (self.chip_sum.at[opposite, :, cols], self.far_in.at[:, cols], opposite * 2 + self.core if direct else nxt),
                (self.chip_sum.at[behind, :, cols], self.near_in.at[:, cols], prv),
                (self.chip_sum.at[ahead, :, cols], self.last_in.at[:, cols], nxt),
            )[kind - 4]
        return remote(src, dst, self.send_sems.at[kind, j], self.recv_sems.at[kind, j], peer)

    def go(self, kind, j, cols, way, direct):
        copy = self.copy(kind, j, cols, way, direct)
        copy.start()
        self.sends.append(copy)

    def begin(self, j, cols, way, direct):
        for kind in range(4):
            self.go(kind, j, cols, way, direct)

    def pair(self, kind, k, j, cols, way, direct):
        self.copy(kind, j, cols, way, direct).wait_recv()
        return self.part[k, self.core, :, cols].astype(F32) + self.from_other[k, :, cols].astype(F32)

    def far(self, j, cols, way, direct):
        opposite = lax.rem(self.chip + 2, CHIPS)
        self.chip_sum[opposite, :, cols] = self.pair(0, opposite, j, cols, way, direct).astype(BF16)
        self.go(4, j, cols, way, direct)

    def near(self, j, cols, way, direct):
        behind = lax.rem(self.chip + CHIPS - way, CHIPS)
        self.chip_sum[behind, :, cols] = self.pair(1, behind, j, cols, way, direct).astype(BF16)
        self.go(5, j, cols, way, direct)

    def third(self, j, cols, way, direct):
        ahead = lax.rem(self.chip + CHIPS + way, CHIPS)
        mine = self.pair(2, ahead, j, cols, way, direct)
        if not direct:
            self.copy(4, j, cols, way, direct).wait_recv()
            mine = mine + self.far_in[:, cols].astype(F32)
        self.chip_sum[ahead, :, cols] = mine.astype(BF16)
        self.go(6, j, cols, way, direct)

    def last(self, j, cols, way, direct):
        own = self.pair(3, self.chip, j, cols, way, direct)
        self.copy(5, j, cols, way, direct).wait_recv()
        own = own + self.near_in[:, cols].astype(F32)
        if direct:
            self.copy(4, j, cols, way, direct).wait_recv()
            own = own + self.far_in[:, cols].astype(F32)
        self.copy(6, j, cols, way, direct).wait_recv()
        return own + self.last_in[:, cols].astype(F32)

    def finish(self):
        for copy in self.sends:
            copy.wait_send()


def mlp_kernel(attn_ref, x_buf, gain_ref, wo_ref, w1_hbm, w3_hbm, w2_hbm, out_ref,
               part, other_in, chip_sum, far_in, near_in, last_in,
               x1_buf, h_buf, act_buf, w1_buf, w3_buf, w2_buf,
               w_sems, rs1_send, rs1_recv, ag_send, ag_recv, rs2_send, rs2_recv):
    me, core, chip, other, right, left = places()
    knock(other, right, left, lax.rem(chip + 2, CHIPS) * 2 + core)
    width = x_buf.shape[1]
    n_tok = act_buf.shape[0]
    n_chunks = w1_buf.shape[0]
    chunk = w1_buf.shape[2]

    def weight(kind, i):
        src = (w1_hbm, w3_hbm, w2_hbm)[kind]
        dst = (w1_buf, w3_buf, w2_buf)[kind]
        return pltpu.make_async_copy(src.at[0, :, pl.ds(pl.multiple_of(i * chunk, 128), chunk)], dst.at[i], w_sems.at[kind, i])

    queue = [weight(kind, i) for i in range(n_chunks) for kind in range(2)] + [weight(2, i) for i in range(n_chunks)]

    def feed(n):
        for copy in queue[:n]:
            copy.start()
        del queue[:n]

    feed(2)

    def plan(pieces, straight=0):
        size = width // pieces
        return [(j, pl.ds(j * size, size), 1 if j % 2 == 0 else -1, j >= pieces - straight) for j in range(pieces)]

    def put_part(cols, value):
        part[:, :, :, cols] = value.astype(BF16).reshape(CHIPS, 2, n_tok // (2 * CHIPS), value.shape[1])

    plan1 = plan(RS1_PIECES)
    rs1 = Reducer(part, other_in, chip_sum, far_in, near_in, last_in, rs1_send, rs1_recv)
    attn = attn_ref[...]
    for item in plan1:
        put_part(item[1], jnp.dot(attn, wo_ref[0, :, item[1]], preferred_element_type=F32))
        if item[0] == 0:
            enter(4)
        rs1.begin(*item)
    feed(1)
    for stage, n in ((rs1.far, 0), (rs1.near, 4), (rs1.third, 3)):
        for item in plan1:
            stage(*item)
        feed(n)
    for item in plan1:
        cols = item[1]
        x1_buf[:, cols] = (x_buf[:, cols].astype(F32) + rs1.last(*item)).astype(BF16)
    rs1.finish()
    h_buf[me] = norm_rows(x1_buf[...].astype(F32), gain_ref[...].astype(F32))
    gather_rows(h_buf, ag_send, ag_recv, queue)

    def gate_up(i, carry):
        weight(0, i).wait()
        weight(1, i).wait()
        h_all = h_buf[...].reshape(n_tok, width)
        gate = jnp.dot(h_all, w1_buf[i], preferred_element_type=F32)
        up = jnp.dot(h_all, w3_buf[i], preferred_element_type=F32)
        act_buf[:, pl.ds(pl.multiple_of(i * chunk, 128), chunk)] = (gate * jax.nn.sigmoid(gate) * up).astype(BF16)
        return carry

    lax.fori_loop(0, n_chunks, gate_up, 0)

    rs2 = Reducer(part, other_in, chip_sum, far_in, near_in, last_in, rs2_send, rs2_recv)
    plan2 = plan(n_chunks, RS2_STRAIGHT)
    for j in range(n_chunks + RS2_LAG):
        if j < n_chunks:
            weight(2, j).wait()
            put_part(plan2[j][1], jnp.dot(act_buf[...], w2_buf[j], preferred_element_type=F32))
            rs2.begin(*plan2[j])
        if j >= RS2_LAG:
            rs2.far(*plan2[j - RS2_LAG])
            rs2.near(*plan2[j - RS2_LAG])
            if plan2[j - RS2_LAG][3]:
                rs2.third(*plan2[j - RS2_LAG])
    for item in plan2:
        if not item[3]:
            rs2.third(*item)
    for item in plan2:
        cols = item[1]
        out_ref[:, cols] = (x1_buf[:, cols].astype(F32) + rs2.last(*item)).astype(BF16)
    rs2.finish()


def shape(dims, dtype=BF16):
    return jax.ShapeDtypeStruct(dims, dtype)


def to_tiles(cache):
    _, n_tok, n_rows, n_heads, head = cache.shape
    halves = head // LANES
    return cache.reshape(n_tok, n_rows, n_heads, halves, LANES).transpose(0, 1, 3, 2, 4).reshape(n_tok, n_rows * halves * n_heads, LANES)


def from_tiles(tiles, like):
    _, n_tok, n_rows, n_heads, head = like.shape
    halves = head // LANES
    return tiles.reshape(n_tok, n_rows, halves, n_heads, LANES).transpose(0, 1, 3, 2, 4).reshape(like.shape)


def run_qkv(x, gain, pos2, wq, wk, wv, k_tiles, v_tiles):
    n_tok = k_tiles.shape[0]
    rows, width = x.shape
    cols = wq.shape[2]
    blocks = n_tok // rows
    dma = pltpu.SemaphoreType.DMA
    args = (x, gain, pos2, wq, wk, wv, k_tiles, v_tiles)
    return pl.pallas_call(
        qkv_kernel,
        out_shape=[shape((n_tok, cols))] * 3 + [shape(k_tiles.shape)] * 2 + [shape((cols // (2 * LANES) * n_tok, LANES), F32)],
        in_specs=[HBM] * len(args),
        out_specs=[VMEM] * 6,
        scratch_shapes=[
            pltpu.VMEM((2, n_tok, LANES), F32), pltpu.VMEM((rows, width), BF16), pltpu.VMEM(gain.shape, BF16), pltpu.VMEM(pos2.shape, pos2.dtype),
            pltpu.VMEM((blocks, rows, width), BF16), pltpu.VMEM((3, width, cols), BF16),
            dma((6,)), dma((2, 8)), dma((GATHER_SEMS,)), dma((GATHER_SEMS,))],
        compiler_params=pltpu.CompilerParams(collective_id=0, has_side_effects=True, vmem_limit_bytes=16 << 20),
        name='gather_qkv',
    )(*(pltpu.with_memory_space_constraint(a, pltpu.HBM) for a in args))


def run_attn(pos2, pos_rows, q, k, v, k_tiles, v_tiles):
    n_tok = k_tiles.shape[0]
    rows2 = q.shape[1] // (2 * LANES) * n_tok
    dma = pltpu.SemaphoreType.DMA
    wide = pltpu.VMEM((2, rows2, LANES), F32)
    tiles = shape(k_tiles.shape)
    attn, _, _, k_out, v_out = pl.pallas_call(
        attn_kernel,
        out_shape=[shape(q.shape), tiles, tiles, tiles, tiles],
        in_specs=[HBM, VMEM, VMEM, VMEM, VMEM, VMEM, VMEM],
        out_specs=[VMEM, VMEM, VMEM, HBM, HBM],
        scratch_shapes=[
            pltpu.SMEM(pos2.shape, pos2.dtype), pltpu.VMEM((2, n_tok * 8, LANES), F32), wide, wide,
            pltpu.VMEM((TOK_STEP // TOK_UNIT, 4 * TOK_SUB, k_tiles.shape[1]), F32), pltpu.VMEM((TOK_STEP // TOK_UNIT, 8 * TOK_SUB, k_tiles.shape[1]), F32),
            dma, dma((2, n_tok // TOK_STEP))],
        input_output_aliases={5: 1, 6: 2},
        compiler_params=pltpu.CompilerParams(vmem_limit_bytes=8 << 20),
        name='attention',
    )(pltpu.with_memory_space_constraint(pos2, pltpu.HBM), pos_rows, q, k, v, k_tiles, v_tiles)
    return attn, k_out, v_out


def run_mlp(attn, x, gain, wo, w1, w3, w2):
    rows, width = x.shape
    n_tok = attn.shape[0]
    ffn = w1.shape[2]
    chunk = MLP_CHUNK
    n_chunks = ffn // chunk
    dma = pltpu.SemaphoreType.DMA
    block = pltpu.VMEM((rows, width), BF16)
    chips = pltpu.VMEM((CHIPS, rows, width), BF16)
    return pl.pallas_call(
        mlp_kernel,
        out_shape=pltpu.VMEM((rows, width), BF16),
        in_specs=[VMEM, VMEM, VMEM, VMEM, HBM, HBM, HBM],
        out_specs=VMEM,
        scratch_shapes=[
            pltpu.VMEM((CHIPS, 2, rows, width), BF16), chips, chips, block, block, block,
            block, pltpu.VMEM((n_tok // rows, rows, width), BF16), pltpu.VMEM((n_tok, ffn), BF16),
            pltpu.VMEM((n_chunks, width, chunk), BF16), pltpu.VMEM((n_chunks, width, chunk), BF16), pltpu.VMEM((width // chunk, ffn, chunk), BF16),
            dma((3, n_chunks)), dma((7, RS1_PIECES)), dma((7, RS1_PIECES)), dma((GATHER_SEMS,)), dma((GATHER_SEMS,)),
            dma((7, n_chunks)), dma((7, n_chunks))],
        compiler_params=pltpu.CompilerParams(collective_id=1, has_side_effects=True, vmem_limit_bytes=MLP_VMEM),
        name='reduce_mlp',
    )(*(pltpu.with_memory_space_constraint(a, pltpu.VMEM) for a in (attn, x, gain, wo)), w1, w3, w2)


def solution(mesh):
    row_spec = P(('data', 'model'), None)
    cache_spec = P(None, 'data', None, 'model', None)
    col_spec = P(None, None, 'model')
    inner_spec = P(None, 'model', None)
    in_specs = (row_spec, P('data'), P(), P(), col_spec, col_spec, col_spec, inner_spec, col_spec, col_spec, inner_spec, cache_spec, cache_spec)
    out_specs = (row_spec, cache_spec, cache_spec)

    def device_step(hidden, positions, attn_gain, mlp_gain, w_query, w_key, w_value, w_out, w_gate, w_up, w_down, k_cache, v_cache):
        n_tok = positions.shape[0]
        pos2 = positions.reshape(1, n_tok)
        q, k, v, k_tiles, v_tiles, pos_rows = run_qkv(hidden, attn_gain, pos2, w_query, w_key, w_value, to_tiles(k_cache), to_tiles(v_cache))
        attn, k_out, v_out = run_attn(pos2, pos_rows, q, k, v, k_tiles, v_tiles)
        out = run_mlp(attn, hidden, mlp_gain, w_out, w_gate, w_up, w_down)
        return out, from_tiles(k_out, k_cache), from_tiles(v_out, v_cache)

    return jax.shard_map(device_step, mesh=mesh, in_specs=in_specs, out_specs=out_specs, check_vma=False)
```

```python
import functools
import math
import jax
import jax.numpy as jnp
from jax import lax
from jax.experimental import pallas as pl
from jax.experimental.pallas import tpu as pltpu
from jax.sharding import PartitionSpec as P

NORM_EPS = 1e-5
ROPE_BASE = 10000.0
BF16 = jnp.bfloat16
F32 = jnp.float32
VMEM = pl.BlockSpec(memory_space=pltpu.VMEM)
HBM = pl.BlockSpec(memory_space=pltpu.HBM)
MLP_VMEM = 61600000
CHIPS = 4
MLP_CHUNK = 512
RS1_PIECES = 4
RS2_LAG = 2
RS2_STRAIGHT = 4
GATHER_SEMS = 21


def places():
    me = lax.axis_index('model')
    core = lax.rem(me, 2)
    chip = lax.div(me, 2)
    other = me + 1 - 2 * core
    right = lax.rem(chip + 1, CHIPS) * 2 + core
    left = lax.rem(chip + CHIPS - 1, CHIPS) * 2 + core
    return me, core, chip, other, right, left


def knock(*peers):
    barrier = pltpu.get_barrier_semaphore()
    for peer in peers:
        pl.semaphore_signal(barrier, inc=1, device_id={'model': peer})


def enter(peers):
    pl.semaphore_wait(pltpu.get_barrier_semaphore(), peers)


def remote(src, dst, send_sem, recv_sem, peer):
    return pltpu.make_async_remote_copy(src_ref=src, dst_ref=dst, send_sem=send_sem, recv_sem=recv_sem, device_id={'model': peer})


def norm_rows(x_f, gain_f):
    inv_rms = lax.rsqrt(jnp.mean(x_f * x_f, axis=-1, keepdims=True) + NORM_EPS)
    return (x_f * inv_rms * gain_f).astype(BF16)


def gather_rows(buf, send_sems, recv_sems, behind=(), meanwhile=None):
    me, core, chip, other, right, left = places()
    width = buf.shape[2]
    quarter = width // 4
    q0, q1, q2, q3 = (pl.ds(i * quarter, quarter) for i in range(4))
    lo, hi, full = pl.ds(0, 2 * quarter), pl.ds(2 * quarter, 2 * quarter), pl.ds(0, width)
    far = lax.rem(chip + 2, CHIPS) * 2 + core
    sends = []

    def hop(blk, cols, idx, peer):
        view = buf.at[blk, :, cols]
        return remote(view, view, send_sems.at[idx], recv_sems.at[idx], peer)

    def arrive(blk, cols, idx):
        hop(blk, cols, idx, other).wait_recv()

    def send(blk, cols, idx, peer):
        copy = hop(blk, cols, idx, peer)
        copy.start()
        sends.append(copy)

    for cols, idx, peer in (
            (q0, 0, right), (q2, 1, left), (q1, 9, far), (q3, 10, far), (q1, 2, right), (q3, 3, left), (hi, 4, right), (lo, 5, left),
            (full, 6, other)):
        send(me, cols, idx, peer)
    across = []
    behind = list(behind)
    share = -(-len(behind) // 8)
    for copy in behind[:2 * share]:
        copy.start()
    behind = behind[2 * share:]
    if meanwhile is not None:
        meanwhile()
    for blk, cols, idx, onward, peer in (
            (left, q0, 0, 7, right), (right, q2, 1, 8, left), (left, q1, 2, None, None), (right, q3, 3, None, None),
            (left, hi, 4, None, None), (right, lo, 5, None, None),
            (far, q1, 9, None, None), (far, q3, 10, None, None), (far, q0, 7, None, None), (far, q2, 8, None, None)):
        arrive(blk, cols, idx)
        if onward is not None:
            send(blk, cols, onward, peer)
        send(blk, cols, 11 + len(across), other)
        across.append((blk + 1 - 2 * core, cols, 11 + len(across)))
        for copy in behind[:share]:
            copy.start()
        behind = behind[share:]
    arrive(other, full, 6)
    for item in across:
        arrive(*item)
    for copy in sends:
        copy.wait_send()


LANES = 128


def qkv_kernel(x_hbm, gain_hbm, pos_hbm, wq_hbm, wk_hbm, wv_hbm, kc_hbm, vc_hbm, q_ref, k_ref, v_ref, kb_ref, vb_ref, pc_ref,
               trig_buf, x_buf, gain_ref, pos_ref, h_buf, w_buf, load_sems, cache_sems, send_sems, recv_sems):
    me, core, chip, other, right, left = places()
    knock(other, right, left, lax.rem(chip + 2, CHIPS) * 2 + core)
    loads = [pltpu.make_async_copy(src, dst, load_sems.at[3 + i]) for i, (src, dst) in enumerate(((x_hbm, x_buf), (gain_hbm, gain_ref), (pos_hbm, pos_ref)))]
    w_copies = [pltpu.make_async_copy(w.at[0], w_buf.at[i], load_sems.at[i]) for i, w in enumerate((wq_hbm, wk_hbm, wv_hbm))]
    pieces = cache_sems.shape[1]
    piece = kb_ref.shape[0] // pieces
    cache_in = []
    for kv, (hbm, buf) in enumerate(((kc_hbm, kb_ref), (vc_hbm, vb_ref))):
        for p in range(pieces):
            toks = pl.ds(p * piece, piece)
            cache_in.append(pltpu.make_async_copy(hbm.at[toks], buf.at[toks], cache_sems.at[kv, p]))
    for copy in loads:
        copy.start()
    for copy in loads:
        copy.wait()
    h_buf[me] = norm_rows(x_buf[...].astype(F32), gain_ref[...].astype(F32))
    enter(4)
    n_tok = pos_ref.shape[1]
    half = LANES
    head = 2 * half
    pos_f = pos_ref[...].astype(F32)

    def pick(rows, per):
        own = lax.broadcasted_iota(jnp.int32, (rows, n_tok), 0) // per == lax.broadcasted_iota(jnp.int32, (rows, n_tok), 1)
        return jnp.sum(jnp.where(own, jnp.broadcast_to(pos_f, (rows, n_tok)), 0.0), axis=1, keepdims=True)

    def tables():
        lane = lax.broadcasted_iota(jnp.int32, (n_tok, half), 1).astype(F32)
        angles = pick(n_tok, 1) * jnp.exp(lane * (-2.0 * math.log(ROPE_BASE) / head))
        trig_buf[0] = jnp.cos(angles)
        trig_buf[1] = jnp.sin(angles)
        rows2 = pc_ref.shape[0]
        pc_ref[...] = jnp.broadcast_to(pick(rows2, rows2 // n_tok), pc_ref.shape)

    gather_rows(h_buf, send_sems, recv_sems, w_copies + cache_in, tables)
    cos_tab, sin_tab = trig_buf[0], trig_buf[1]
    h_all = h_buf[...].reshape(n_tok, h_buf.shape[2])
    for i, out_ref in enumerate((q_ref, k_ref, v_ref)):
        w_copies[i].wait()
        proj = jnp.dot(h_all, w_buf[i], preferred_element_type=F32).astype(BF16)
        if i == 2:
            out_ref[...] = proj
            continue
        for h0 in range(0, proj.shape[1], head):
            front = proj[:, h0:h0 + half].astype(F32)
            back = proj[:, h0 + half:h0 + head].astype(F32)
            out_ref[:, h0:h0 + half] = (front * cos_tab - back * sin_tab).astype(BF16)
            out_ref[:, h0 + half:h0 + head] = (back * cos_tab + front * sin_tab).astype(BF16)
    for copy in cache_in:
        copy.wait()


TOK_STEP = 16
TOK_UNIT = 8
TOK_SUB = 4


def attn_kernel(pos_hbm, pc_buf, q_ref, k_ref, v_ref, kb_in, vb_in, attn_ref, k_buf, v_buf, ko_hbm, vo_hbm,
                pos_smem, new_buf, q_buf, o_buf, score_buf, prob_buf, pos_sem, out_sems):
    n_tok, per_tok, lanes = k_buf.shape
    n_heads = 2
    head = q_ref.shape[1] // n_heads
    steps = n_tok // TOK_STEP
    bufs = (k_buf, v_buf)
    pos_copy = pltpu.make_async_copy(pos_hbm, pos_smem, pos_sem)
    pos_copy.start()

    def write_out(t):
        toks = pl.ds(t * TOK_STEP, TOK_STEP)
        return [pltpu.make_async_copy(buf.at[toks], hbm.at[toks], out_sems.at[kv, t]) for kv, (buf, hbm) in enumerate(zip(bufs, (ko_hbm, vo_hbm)))]

    for h in range(n_heads):
        for c in range(2):
            cols = slice(h * head + c * lanes, h * head + (c + 1) * lanes)
            q_buf.at[c][pl.ds(h, n_tok, stride=2), :] = q_ref[:, cols].astype(F32)
            for kv, ref in enumerate((k_ref, v_ref)):
                new = ref[:, cols].astype(F32)
                for again in range(2):
                    new_buf.at[kv][pl.ds(4 * again + 2 * c + h, n_tok, stride=8), :] = new
    tile_row = lax.broadcasted_iota(jnp.int32, (16, lanes), 0)
    sub = TOK_SUB * n_heads
    tok_of = (lax.broadcasted_iota(jnp.int32, (4 * sub, per_tok), 0) % sub) // 2
    row = lax.broadcasted_iota(jnp.int32, (2 * sub, per_tok), 0)
    col = lax.broadcasted_iota(jnp.int32, (2 * sub, per_tok), 1)
    counts = ((col & 2) == 0) & ((col & 1) == (row & 1))
    key_pos = (col >> 2).astype(F32)

    def shift(x, by):
        return jnp.concatenate([pltpu.roll(x[:, i:i + lanes], by % lanes, 1) for i in range(0, per_tok, lanes)], axis=1)

    def pair(buf, b0):
        one, two = (buf[pl.ds(b0 + g * TOK_SUB, TOK_SUB)] for g in range(2))
        return jnp.concatenate([x.reshape(TOK_SUB * per_tok, lanes) for x in (one, two)], axis=1)

    def out_rows(b0):
        return [pl.ds(pl.multiple_of(b0 * n_heads + g * sub, sub), sub) for g in range(2)]

    units = TOK_STEP // TOK_UNIT

    def mix(t, u):
        b0 = t * TOK_STEP + u * TOK_UNIT
        probs = prob_buf[u]
        wide = jnp.concatenate([jnp.where(tok_of == m, probs, 0.0) for m in range(TOK_SUB)], axis=1).astype(BF16)
        out = jnp.dot(wide, pair(v_buf, b0), preferred_element_type=F32).astype(BF16).astype(F32)
        rows = out_rows(b0)
        for g in range(2):
            for c in range(2):
                at = (2 * g + c) * sub
                o_buf[c, rows[g], :] = out[at:at + sub, g * lanes:(g + 1) * lanes]

    def soften(u):
        total = score_buf[u]
        e = jnp.exp(total - jnp.max(total, axis=1, keepdims=True))
        probs = (e / jnp.sum(e, axis=1, keepdims=True)).astype(BF16).astype(F32)
        moved = shift(probs, 2)
        prob_buf[u] = jnp.concatenate([probs[:sub], moved[:sub], probs[sub:], moved[sub:]], axis=0)

    def insert(t):
        for i in range(TOK_STEP):
            b = t * TOK_STEP + i
            pos = pos_smem[0, b]
            tile = pl.ds(pl.multiple_of((pos >> 2) * 16, 16), 16)
            hit = (tile_row >> 2) == (pos & 3)
            for kv in range(2):
                new = new_buf[kv, pl.ds(pl.multiple_of(b * 8, 8), 8), :]
                old = bufs[kv][b, tile, :].astype(F32)
                bufs[kv][b, tile, :] = jnp.where(hit, jnp.concatenate([new, new], axis=0), old).astype(BF16)

    def score(t, u):
        b0 = t * TOK_STEP + u * TOK_UNIT
        rows = out_rows(b0)
        none = jnp.zeros((sub, lanes), F32)
        q = jnp.concatenate(
            [jnp.concatenate([q_buf[c, rows[0], :], none], axis=1) for c in range(2)] +
            [jnp.concatenate([none, q_buf[c, rows[1], :]], axis=1) for c in range(2)], axis=0).astype(BF16)
        scores = lax.dot_general(q, pair(k_buf, b0), (((1,), (1,)), ((), ())), preferred_element_type=F32)
        mine = scores[:, :per_tok]
        for m in range(1, TOK_SUB):
            mine = jnp.where(tok_of == m, scores[:, m * per_tok:(m + 1) * per_tok], mine)
        first = jnp.concatenate([mine[:sub], mine[2 * sub:3 * sub]], axis=0)
        second = jnp.concatenate([mine[sub:2 * sub], mine[3 * sub:]], axis=0)
        total = (first + shift(second, -2)) * (head ** -0.5)
        pos_of = pc_buf[pl.ds(pl.multiple_of(b0 * n_heads, 2 * sub), 2 * sub), :]
        score_buf[u] = jnp.where(counts & (key_pos <= jnp.concatenate([pos_of] * (per_tok // lanes), axis=1)), total, -1e30)

    def send(t):
        for copy in write_out(t):
            copy.start()

    def each(stage, *args):
        for u in range(units):
            stage(*args, u)

    pos_copy.wait()
    for t in range(3):
        insert(t)
    send(0)
    each(score, 0)
    send(1)
    send(2)
    each(soften)
    each(score, 1)

    def stages(t):
        each(mix, t - 2)
        each(soften)
        each(score, t)

    def step(t, carry):
        insert(t + 1)
        stages(t)
        send(t + 1)
        return carry

    lax.fori_loop(2, steps - 1, step, 0)
    stages(steps - 1)
    each(mix, steps - 2)
    each(soften)
    each(mix, steps - 1)
    attn_ref[...] = jnp.concatenate([o_buf.at[c][pl.ds(h, n_tok, stride=2), :] for h in range(n_heads) for c in range(2)], axis=1).astype(BF16)
    for t in range(steps):
        for copy in write_out(t):
            copy.wait()


class Reducer:
    def __init__(self, part, from_other, chip_sum, far_in, near_in, last_in, send_sems, recv_sems):
        self.part, self.from_other, self.chip_sum = part, from_other, chip_sum
        self.far_in, self.near_in, self.last_in = far_in, near_in, last_in
        self.send_sems, self.recv_sems = send_sems, recv_sems
        self.me, self.core, self.chip, self.other, self.right, self.left = places()
        self.sends = []

    def copy(self, kind, j, cols, way, direct):
        nxt, prv = (self.right, self.left) if way > 0 else (self.left, self.right)
        ahead = lax.rem(self.chip + CHIPS + way, CHIPS)
        behind = lax.rem(self.chip + CHIPS - way, CHIPS)
        opposite = lax.rem(self.chip + 2, CHIPS)
        if kind < 4:
            k = (opposite, behind, ahead, self.chip)[kind]
            src, dst, peer = self.part.at[k, 1 - self.core, :, cols], self.from_other.at[k, :, cols], self.other
        else:
            src, dst, peer = (
                (self.chip_sum.at[opposite, :, cols], self.far_in.at[:, cols], opposite * 2 + self.core if direct else nxt),
                (self.chip_sum.at[behind, :, cols], self.near_in.at[:, cols], prv),
                (self.chip_sum.at[ahead, :, cols], self.last_in.at[:, cols], nxt),
            )[kind - 4]
        return remote(src, dst, self.send_sems.at[kind, j], self.recv_sems.at[kind, j], peer)

    def go(self, kind, j, cols, way, direct):
        copy = self.copy(kind, j, cols, way, direct)
        copy.start()
        self.sends.append(copy)

    def begin(self, j, cols, way, direct):
        for kind in range(4):
            self.go(kind, j, cols, way, direct)

    def pair(self, kind, k, j, cols, way, direct):
        self.copy(kind, j, cols, way, direct).wait_recv()
        return self.part[k, self.core, :, cols].astype(F32) + self.from_other[k, :, cols].astype(F32)

    def far(self, j, cols, way, direct):
        opposite = lax.rem(self.chip + 2, CHIPS)
        self.chip_sum[opposite, :, cols] = self.pair(0, opposite, j, cols, way, direct).astype(BF16)
        self.go(4, j, cols, way, direct)

    def near(self, j, cols, way, direct):
        behind = lax.rem(self.chip + CHIPS - way, CHIPS)
        self.chip_sum[behind, :, cols] = self.pair(1, behind, j, cols, way, direct).astype(BF16)
        self.go(5, j, cols, way, direct)

    def third(self, j, cols, way, direct):
        ahead = lax.rem(self.chip + CHIPS + way, CHIPS)
        mine = self.pair(2, ahead, j, cols, way, direct)
        if not direct:
            self.copy(4, j, cols, way, direct).wait_recv()
            mine = mine + self.far_in[:, cols].astype(F32)
        self.chip_sum[ahead, :, cols] = mine.astype(BF16)
        self.go(6, j, cols, way, direct)

    def last(self, j, cols, way, direct):
        own = self.pair(3, self.chip, j, cols, way, direct)
        self.copy(5, j, cols, way, direct).wait_recv()
        own = own + self.near_in[:, cols].astype(F32)
        if direct:
            self.copy(4, j, cols, way, direct).wait_recv()
            own = own + self.far_in[:, cols].astype(F32)
        self.copy(6, j, cols, way, direct).wait_recv()
        return own + self.last_in[:, cols].astype(F32)

    def finish(self):
        for copy in self.sends:
            copy.wait_send()


def mlp_kernel(attn_ref, x_buf, gain_ref, wo_ref, w1_hbm, w3_hbm, w2_hbm, out_ref,
               part, other_in, chip_sum, far_in, near_in, last_in,
               x1_buf, h_buf, act_buf, w1_buf, w3_buf, w2_buf,
               w_sems, rs1_send, rs1_recv, ag_send, ag_recv, rs2_send, rs2_recv):
    me, core, chip, other, right, left = places()
    knock(other, right, left, lax.rem(chip + 2, CHIPS) * 2 + core)
    width = x_buf.shape[1]
    n_tok = act_buf.shape[0]
    n_chunks = w1_buf.shape[0]
    chunk = w1_buf.shape[2]

    def weight(kind, i):
        src = (w1_hbm, w3_hbm, w2_hbm)[kind]
        dst = (w1_buf, w3_buf, w2_buf)[kind]
        return pltpu.make_async_copy(src.at[0, :, pl.ds(pl.multiple_of(i * chunk, 128), chunk)], dst.at[i], w_sems.at[kind, i])

    queue = [weight(kind, i) for i in range(n_chunks) for kind in range(2)] + [weight(2, i) for i in range(n_chunks)]

    def feed(n):
        for copy in queue[:n]:
            copy.start()
        del queue[:n]

    feed(2)

    def plan(pieces, straight=0):
        size = width // pieces
        return [(j, pl.ds(j * size, size), 1 if j % 2 == 0 else -1, j >= pieces - straight) for j in range(pieces)]

    def put_part(cols, value):
        part[:, :, :, cols] = value.astype(BF16).reshape(CHIPS, 2, n_tok // (2 * CHIPS), value.shape[1])

    plan1 = plan(RS1_PIECES)
    rs1 = Reducer(part, other_in, chip_sum, far_in, near_in, last_in, rs1_send, rs1_recv)
    attn = attn_ref[...]
    for item in plan1:
        put_part(item[1], jnp.dot(attn, wo_ref[0, :, item[1]], preferred_element_type=F32))
    enter(4)
    for kind in range(4):
        for item in plan1:
            rs1.go(kind, *item)
    feed(1)
    for stage, n in ((rs1.far, 0), (rs1.near, 4), (rs1.third, 3)):
        for item in plan1:
            stage(*item)
        feed(n)
    for item in plan1:
        cols = item[1]
        x1_buf[:, cols] = (x_buf[:, cols].astype(F32) + rs1.last(*item)).astype(BF16)
    rs1.finish()
    h_buf[me] = norm_rows(x1_buf[...].astype(F32), gain_ref[...].astype(F32))
    gather_rows(h_buf, ag_send, ag_recv, queue)

    def gate_up(i, carry):
        weight(0, i).wait()
        weight(1, i).wait()
        h_all = h_buf[...].reshape(n_tok, width)
        gate = jnp.dot(h_all, w1_buf[i], preferred_element_type=F32)
        up = jnp.dot(h_all, w3_buf[i], preferred_element_type=F32)
        act_buf[:, pl.ds(pl.multiple_of(i * chunk, 128), chunk)] = (gate * jax.nn.sigmoid(gate) * up).astype(BF16)
        return carry

    lax.fori_loop(0, n_chunks, gate_up, 0)

    rs2 = Reducer(part, other_in, chip_sum, far_in, near_in, last_in, rs2_send, rs2_recv)
    plan2 = plan(n_chunks, RS2_STRAIGHT)
    for j in range(n_chunks + RS2_LAG):
        if j < n_chunks:
            weight(2, j).wait()
            put_part(plan2[j][1], jnp.dot(act_buf[...], w2_buf[j], preferred_element_type=F32))
            rs2.begin(*plan2[j])
        if j >= RS2_LAG:
            rs2.far(*plan2[j - RS2_LAG])
            rs2.near(*plan2[j - RS2_LAG])
            if plan2[j - RS2_LAG][3]:
                rs2.third(*plan2[j - RS2_LAG])
    for item in plan2:
        if not item[3]:
            rs2.third(*item)
    for item in plan2:
        cols = item[1]
        out_ref[:, cols] = (x1_buf[:, cols].astype(F32) + rs2.last(*item)).astype(BF16)
    rs2.finish()


def shape(dims, dtype=BF16):
    return jax.ShapeDtypeStruct(dims, dtype)


def to_tiles(cache):
    _, n_tok, n_rows, n_heads, head = cache.shape
    halves = head // LANES
    return cache.reshape(n_tok, n_rows, n_heads, halves, LANES).transpose(0, 1, 3, 2, 4).reshape(n_tok, n_rows * halves * n_heads, LANES)


def from_tiles(tiles, like):
    _, n_tok, n_rows, n_heads, head = like.shape
    halves = head // LANES
    return tiles.reshape(n_tok, n_rows, halves, n_heads, LANES).transpose(0, 1, 3, 2, 4).reshape(like.shape)


def run_qkv(x, gain, pos2, wq, wk, wv, k_tiles, v_tiles):
    n_tok = k_tiles.shape[0]
    rows, width = x.shape
    cols = wq.shape[2]
    blocks = n_tok // rows
    dma = pltpu.SemaphoreType.DMA
    args = (x, gain, pos2, wq, wk, wv, k_tiles, v_tiles)
    return pl.pallas_call(
        qkv_kernel,
        out_shape=[shape((n_tok, cols))] * 3 + [shape(k_tiles.shape)] * 2 + [shape((cols // (2 * LANES) * n_tok, LANES), F32)],
        in_specs=[HBM] * len(args),
        out_specs=[VMEM] * 6,
        scratch_shapes=[
            pltpu.VMEM((2, n_tok, LANES), F32), pltpu.VMEM((rows, width), BF16), pltpu.VMEM(gain.shape, BF16), pltpu.VMEM(pos2.shape, pos2.dtype),
            pltpu.VMEM((blocks, rows, width), BF16), pltpu.VMEM((3, width, cols), BF16),
            dma((6,)), dma((2, 8)), dma((GATHER_SEMS,)), dma((GATHER_SEMS,))],
        compiler_params=pltpu.CompilerParams(collective_id=0, has_side_effects=True, vmem_limit_bytes=16 << 20),
        name='gather_qkv',
    )(*(pltpu.with_memory_space_constraint(a, pltpu.HBM) for a in args))


def run_attn(pos2, pos_rows, q, k, v, k_tiles, v_tiles):
    n_tok = k_tiles.shape[0]
    rows2 = q.shape[1] // (2 * LANES) * n_tok
    dma = pltpu.SemaphoreType.DMA
    wide = pltpu.VMEM((2, rows2, LANES), F32)
    tiles = shape(k_tiles.shape)
    attn, _, _, k_out, v_out = pl.pallas_call(
        attn_kernel,
        out_shape=[shape(q.shape), tiles, tiles, tiles, tiles],
        in_specs=[HBM, VMEM, VMEM, VMEM, VMEM, VMEM, VMEM],
        out_specs=[VMEM, VMEM, VMEM, HBM, HBM],
        scratch_shapes=[
            pltpu.SMEM(pos2.shape, pos2.dtype), pltpu.VMEM((2, n_tok * 8, LANES), F32), wide, wide,
            pltpu.VMEM((TOK_STEP // TOK_UNIT, 4 * TOK_SUB, k_tiles.shape[1]), F32), pltpu.VMEM((TOK_STEP // TOK_UNIT, 8 * TOK_SUB, k_tiles.shape[1]), F32),
            dma, dma((2, n_tok // TOK_STEP))],
        input_output_aliases={5: 1, 6: 2},
        compiler_params=pltpu.CompilerParams(vmem_limit_bytes=8 << 20),
        name='attention',
    )(pltpu.with_memory_space_constraint(pos2, pltpu.HBM), pos_rows, q, k, v, k_tiles, v_tiles)
    return attn, k_out, v_out


def run_mlp(attn, x, gain, wo, w1, w3, w2):
    rows, width = x.shape
    n_tok = attn.shape[0]
    ffn = w1.shape[2]
    chunk = MLP_CHUNK
    n_chunks = ffn // chunk
    dma = pltpu.SemaphoreType.DMA
    block = pltpu.VMEM((rows, width), BF16)
    chips = pltpu.VMEM((CHIPS, rows, width), BF16)
    return pl.pallas_call(
        mlp_kernel,
        out_shape=pltpu.VMEM((rows, width), BF16),
        in_specs=[VMEM, VMEM, VMEM, VMEM, HBM, HBM, HBM],
        out_specs=VMEM,
        scratch_shapes=[
            pltpu.VMEM((CHIPS, 2, rows, width), BF16), chips, chips, block, block, block,
            block, pltpu.VMEM((n_tok // rows, rows, width), BF16), pltpu.VMEM((n_tok, ffn), BF16),
            pltpu.VMEM((n_chunks, width, chunk), BF16), pltpu.VMEM((n_chunks, width, chunk), BF16), pltpu.VMEM((width // chunk, ffn, chunk), BF16),
            dma((3, n_chunks)), dma((7, RS1_PIECES)), dma((7, RS1_PIECES)), dma((GATHER_SEMS,)), dma((GATHER_SEMS,)),
            dma((7, n_chunks)), dma((7, n_chunks))],
        compiler_params=pltpu.CompilerParams(collective_id=1, has_side_effects=True, vmem_limit_bytes=MLP_VMEM),
        name='reduce_mlp',
    )(*(pltpu.with_memory_space_constraint(a, pltpu.VMEM) for a in (attn, x, gain, wo)), w1, w3, w2)


def solution(mesh):
    row_spec = P(('data', 'model'), None)
    cache_spec = P(None, 'data', None, 'model', None)
    col_spec = P(None, None, 'model')
    inner_spec = P(None, 'model', None)
    in_specs = (row_spec, P('data'), P(), P(), col_spec, col_spec, col_spec, inner_spec, col_spec, col_spec, inner_spec, cache_spec, cache_spec)
    out_specs = (row_spec, cache_spec, cache_spec)

    def device_step(hidden, positions, attn_gain, mlp_gain, w_query, w_key, w_value, w_out, w_gate, w_up, w_down, k_cache, v_cache):
        n_tok = positions.shape[0]
        pos2 = positions.reshape(1, n_tok)
        q, k, v, k_tiles, v_tiles, pos_rows = run_qkv(hidden, attn_gain, pos2, w_query, w_key, w_value, to_tiles(k_cache), to_tiles(v_cache))
        attn, k_out, v_out = run_attn(pos2, pos_rows, q, k, v, k_tiles, v_tiles)
        out = run_mlp(attn, hidden, mlp_gain, w_out, w_gate, w_up, w_down)
        return out, from_tiles(k_out, k_cache), from_tiles(v_out, v_cache)

    return jax.shard_map(device_step, mesh=mesh, in_specs=in_specs, out_specs=out_specs, check_vma=False)
```

```python
import functools
import math
import jax
import jax.numpy as jnp
from jax import lax
from jax.experimental import pallas as pl
from jax.experimental.pallas import tpu as pltpu
from jax.sharding import PartitionSpec as P

NORM_EPS = 1e-5
ROPE_BASE = 10000.0
BF16 = jnp.bfloat16
F32 = jnp.float32
VMEM = pl.BlockSpec(memory_space=pltpu.VMEM)
HBM = pl.BlockSpec(memory_space=pltpu.HBM)
MLP_VMEM = 61600000
CHIPS = 4
MLP_CHUNK = 512
RS1_PIECES = 4
RS2_LAG = 2
RS2_STRAIGHT = 4
GATHER_SEMS = 21


def places():
    me = lax.axis_index('model')
    core = lax.rem(me, 2)
    chip = lax.div(me, 2)
    other = me + 1 - 2 * core
    right = lax.rem(chip + 1, CHIPS) * 2 + core
    left = lax.rem(chip + CHIPS - 1, CHIPS) * 2 + core
    return me, core, chip, other, right, left


def knock(*peers):
    barrier = pltpu.get_barrier_semaphore()
    for peer in peers:
        pl.semaphore_signal(barrier, inc=1, device_id={'model': peer})


def enter(peers):
    pl.semaphore_wait(pltpu.get_barrier_semaphore(), peers)


def remote(src, dst, send_sem, recv_sem, peer):
    return pltpu.make_async_remote_copy(src_ref=src, dst_ref=dst, send_sem=send_sem, recv_sem=recv_sem, device_id={'model': peer})


def norm_rows(x_f, gain_f):
    inv_rms = lax.rsqrt(jnp.mean(x_f * x_f, axis=-1, keepdims=True) + NORM_EPS)
    return (x_f * inv_rms * gain_f).astype(BF16)


def gather_rows(buf, send_sems, recv_sems, behind=(), meanwhile=None):
    me, core, chip, other, right, left = places()
    width = buf.shape[2]
    quarter = width // 4
    q0, q1, q2, q3 = (pl.ds(i * quarter, quarter) for i in range(4))
    lo, hi, full = pl.ds(0, 2 * quarter), pl.ds(2 * quarter, 2 * quarter), pl.ds(0, width)
    far = lax.rem(chip + 2, CHIPS) * 2 + core
    sends = []

    def hop(blk, cols, idx, peer):
        view = buf.at[blk, :, cols]
        return remote(view, view, send_sems.at[idx], recv_sems.at[idx], peer)

    def arrive(blk, cols, idx):
        hop(blk, cols, idx, other).wait_recv()

    def send(blk, cols, idx, peer):
        copy = hop(blk, cols, idx, peer)
        copy.start()
        sends.append(copy)

    for cols, idx, peer in (
            (q0, 0, right), (q2, 1, left), (q1, 9, far), (q3, 10, far), (q1, 2, right), (q3, 3, left), (hi, 4, right), (lo, 5, left),
            (full, 6, other)):
        send(me, cols, idx, peer)
    across = []
    behind = list(behind)
    share = -(-len(behind) // 8)
    for copy in behind[:2 * share]:
        copy.start()
    behind = behind[2 * share:]
    if meanwhile is not None:
        meanwhile()
    for blk, cols, idx, onward, peer in (
            (left, q0, 0, 7, right), (right, q2, 1, 8, left), (left, q1, 2, None, None), (right, q3, 3, None, None),
            (left, hi, 4, None, None), (right, lo, 5, None, None),
            (far, q1, 9, None, None), (far, q3, 10, None, None), (far, q0, 7, None, None), (far, q2, 8, None, None)):
        arrive(blk, cols, idx)
        if onward is not None:
            send(blk, cols, onward, peer)
        send(blk, cols, 11 + len(across), other)
        across.append((blk + 1 - 2 * core, cols, 11 + len(across)))
        for copy in behind[:share]:
            copy.start()
        behind = behind[share:]
    arrive(other, full, 6)
    for item in across:
        arrive(*item)
    for copy in sends:
        copy.wait_send()


LANES = 128


def qkv_kernel(x_hbm, gain_hbm, pos_hbm, wq_hbm, wk_hbm, wv_hbm, kc_hbm, vc_hbm, wo_hbm, q_ref, k_ref, v_ref, kb_ref, vb_ref, pc_ref, wo_ref,
               trig_buf, x_buf, gain_ref, pos_ref, h_buf, w_buf, load_sems, cache_sems, send_sems, recv_sems):
    me, core, chip, other, right, left = places()
    knock(other, right, left, lax.rem(chip + 2, CHIPS) * 2 + core)
    loads = [pltpu.make_async_copy(src, dst, load_sems.at[3 + i]) for i, (src, dst) in enumerate(((x_hbm, x_buf), (gain_hbm, gain_ref), (pos_hbm, pos_ref)))]
    w_copies = [pltpu.make_async_copy(w.at[0], w_buf.at[i], load_sems.at[i]) for i, w in enumerate((wq_hbm, wk_hbm, wv_hbm))]
    pieces = cache_sems.shape[1]
    piece = kb_ref.shape[0] // pieces
    cache_in = []
    for kv, (hbm, buf) in enumerate(((kc_hbm, kb_ref), (vc_hbm, vb_ref))):
        for p in range(pieces):
            toks = pl.ds(p * piece, piece)
            cache_in.append(pltpu.make_async_copy(hbm.at[toks], buf.at[toks], cache_sems.at[kv, p]))
    cache_in.append(pltpu.make_async_copy(wo_hbm, wo_ref, load_sems.at[6]))
    for copy in loads:
        copy.start()
    for copy in loads:
        copy.wait()
    h_buf[me] = norm_rows(x_buf[...].astype(F32), gain_ref[...].astype(F32))
    enter(4)
    n_tok = pos_ref.shape[1]
    half = LANES
    head = 2 * half
    pos_f = pos_ref[...].astype(F32)

    def pick(rows, per):
        own = lax.broadcasted_iota(jnp.int32, (rows, n_tok), 0) // per == lax.broadcasted_iota(jnp.int32, (rows, n_tok), 1)
        return jnp.sum(jnp.where(own, jnp.broadcast_to(pos_f, (rows, n_tok)), 0.0), axis=1, keepdims=True)

    def tables():
        lane = lax.broadcasted_iota(jnp.int32, (n_tok, half), 1).astype(F32)
        angles = pick(n_tok, 1) * jnp.exp(lane * (-2.0 * math.log(ROPE_BASE) / head))
        trig_buf[0] = jnp.cos(angles)
        trig_buf[1] = jnp.sin(angles)
        rows2 = pc_ref.shape[0]
        pc_ref[...] = jnp.broadcast_to(pick(rows2, rows2 // n_tok), pc_ref.shape)

    gather_rows(h_buf, send_sems, recv_sems, w_copies + cache_in, tables)
    cos_tab, sin_tab = trig_buf[0], trig_buf[1]
    h_all = h_buf[...].reshape(n_tok, h_buf.shape[2])
    for i, out_ref in enumerate((q_ref, k_ref, v_ref)):
        w_copies[i].wait()
        proj = jnp.dot(h_all, w_buf[i], preferred_element_type=F32).astype(BF16)
        if i == 2:
            out_ref[...] = proj
            continue
        for h0 in range(0, proj.shape[1], head):
            front = proj[:, h0:h0 + half].astype(F32)
            back = proj[:, h0 + half:h0 + head].astype(F32)
            out_ref[:, h0:h0 + half] = (front * cos_tab - back * sin_tab).astype(BF16)
            out_ref[:, h0 + half:h0 + head] = (back * cos_tab + front * sin_tab).astype(BF16)
    for copy in cache_in:
        copy.wait()


TOK_STEP = 16
TOK_UNIT = 8
TOK_SUB = 4


def attn_kernel(pos_hbm, pc_buf, q_ref, k_ref, v_ref, kb_in, vb_in, attn_ref, k_buf, v_buf, ko_hbm, vo_hbm,
                pos_smem, new_buf, q_buf, o_buf, score_buf, prob_buf, pos_sem, out_sems):
    n_tok, per_tok, lanes = k_buf.shape
    n_heads = 2
    head = q_ref.shape[1] // n_heads
    steps = n_tok // TOK_STEP
    bufs = (k_buf, v_buf)
    pos_copy = pltpu.make_async_copy(pos_hbm, pos_smem, pos_sem)
    pos_copy.start()

    def write_out(t):
        toks = pl.ds(t * TOK_STEP, TOK_STEP)
        return [pltpu.make_async_copy(buf.at[toks], hbm.at[toks], out_sems.at[kv, t]) for kv, (buf, hbm) in enumerate(zip(bufs, (ko_hbm, vo_hbm)))]

    for h in range(n_heads):
        for c in range(2):
            cols = slice(h * head + c * lanes, h * head + (c + 1) * lanes)
            q_buf.at[c][pl.ds(h, n_tok, stride=2), :] = q_ref[:, cols].astype(F32)
            for kv, ref in enumerate((k_ref, v_ref)):
                new = ref[:, cols].astype(F32)
                for again in range(2):
                    new_buf.at[kv][pl.ds(4 * again + 2 * c + h, n_tok, stride=8), :] = new
    tile_row = lax.broadcasted_iota(jnp.int32, (16, lanes), 0)
    sub = TOK_SUB * n_heads
    tok_of = (lax.broadcasted_iota(jnp.int32, (4 * sub, per_tok), 0) % sub) // 2
    row = lax.broadcasted_iota(jnp.int32, (2 * sub, per_tok), 0)
    col = lax.broadcasted_iota(jnp.int32, (2 * sub, per_tok), 1)
    counts = ((col & 2) == 0) & ((col & 1) == (row & 1))
    key_pos = (col >> 2).astype(F32)

    def shift(x, by):
        return jnp.concatenate([pltpu.roll(x[:, i:i + lanes], by % lanes, 1) for i in range(0, per_tok, lanes)], axis=1)

    def pair(buf, b0):
        one, two = (buf[pl.ds(b0 + g * TOK_SUB, TOK_SUB)] for g in range(2))
        return jnp.concatenate([x.reshape(TOK_SUB * per_tok, lanes) for x in (one, two)], axis=1)

    def out_rows(b0):
        return [pl.ds(pl.multiple_of(b0 * n_heads + g * sub, sub), sub) for g in range(2)]

    units = TOK_STEP // TOK_UNIT

    def mix(t, u):
        b0 = t * TOK_STEP + u * TOK_UNIT
        probs = prob_buf[u]
        wide = jnp.concatenate([jnp.where(tok_of == m, probs, 0.0) for m in range(TOK_SUB)], axis=1).astype(BF16)
        out = jnp.dot(wide, pair(v_buf, b0), preferred_element_type=F32).astype(BF16).astype(F32)
        rows = out_rows(b0)
        for g in range(2):
            for c in range(2):
                at = (2 * g + c) * sub
                o_buf[c, rows[g], :] = out[at:at + sub, g * lanes:(g + 1) * lanes]

    def soften(u):
        total = score_buf[u]
        e = jnp.exp(total - jnp.max(total, axis=1, keepdims=True))
        probs = (e / jnp.sum(e, axis=1, keepdims=True)).astype(BF16).astype(F32)
        moved = shift(probs, 2)
        prob_buf[u] = jnp.concatenate([probs[:sub], moved[:sub], probs[sub:], moved[sub:]], axis=0)

    def insert(t):
        for i in range(TOK_STEP):
            b = t * TOK_STEP + i
            pos = pos_smem[0, b]
            tile = pl.ds(pl.multiple_of((pos >> 2) * 16, 16), 16)
            hit = (tile_row >> 2) == (pos & 3)
            for kv in range(2):
                new = new_buf[kv, pl.ds(pl.multiple_of(b * 8, 8), 8), :]
                old = bufs[kv][b, tile, :].astype(F32)
                bufs[kv][b, tile, :] = jnp.where(hit, jnp.concatenate([new, new], axis=0), old).astype(BF16)

    def score(t, u):
        b0 = t * TOK_STEP + u * TOK_UNIT
        rows = out_rows(b0)
        none = jnp.zeros((sub, lanes), F32)
        q = jnp.concatenate(
            [jnp.concatenate([q_buf[c, rows[0], :], none], axis=1) for c in range(2)] +
            [jnp.concatenate([none, q_buf[c, rows[1], :]], axis=1) for c in range(2)], axis=0).astype(BF16)
        scores = lax.dot_general(q, pair(k_buf, b0), (((1,), (1,)), ((), ())), preferred_element_type=F32)
        mine = scores[:, :per_tok]
        for m in range(1, TOK_SUB):
            mine = jnp.where(tok_of == m, scores[:, m * per_tok:(m + 1) * per_tok], mine)
        first = jnp.concatenate([mine[:sub], mine[2 * sub:3 * sub]], axis=0)
        second = jnp.concatenate([mine[sub:2 * sub], mine[3 * sub:]], axis=0)
        total = (first + shift(second, -2)) * (head ** -0.5)
        pos_of = pc_buf[pl.ds(pl.multiple_of(b0 * n_heads, 2 * sub), 2 * sub), :]
        score_buf[u] = jnp.where(counts & (key_pos <= jnp.concatenate([pos_of] * (per_tok // lanes), axis=1)), total, -1e30)

    def send(t):
        for copy in write_out(t):
            copy.start()

    def each(stage, *args):
        for u in range(units):
            stage(*args, u)

    pos_copy.wait()
    insert(0)

    def place(t, carry):
        insert(t)
        send(t - 1)
        return carry

    lax.fori_loop(1, steps, place, 0)
    each(score, 0)
    send(steps - 1)
    each(soften)
    each(score, 1)

    def step(t, carry):
        each(mix, t - 2)
        each(soften)
        each(score, t)
        return carry

    lax.fori_loop(2, steps, step, 0)
    each(mix, steps - 2)
    each(soften)
    each(mix, steps - 1)
    attn_ref[...] = jnp.concatenate([o_buf.at[c][pl.ds(h, n_tok, stride=2), :] for h in range(n_heads) for c in range(2)], axis=1).astype(BF16)
    for t in range(steps):
        for copy in write_out(t):
            copy.wait()


class Reducer:
    def __init__(self, part, from_other, chip_sum, far_in, near_in, last_in, send_sems, recv_sems, joint=False):
        self.joint = joint
        self.part, self.from_other, self.chip_sum = part, from_other, chip_sum
        self.far_in, self.near_in, self.last_in = far_in, near_in, last_in
        self.send_sems, self.recv_sems = send_sems, recv_sems
        self.me, self.core, self.chip, self.other, self.right, self.left = places()
        self.sends = []

    def copy(self, kind, j, cols, way, direct):
        nxt, prv = (self.right, self.left) if way > 0 else (self.left, self.right)
        ahead = lax.rem(self.chip + CHIPS + way, CHIPS)
        behind = lax.rem(self.chip + CHIPS - way, CHIPS)
        opposite = lax.rem(self.chip + 2, CHIPS)
        if kind < 4:
            k = (opposite, behind, ahead, self.chip)[kind]
            k = slice(None) if self.joint else k
            src, dst, peer = self.part.at[k, 1 - self.core, :, cols], self.from_other.at[k, :, cols], self.other
        else:
            src, dst, peer = (
                (self.chip_sum.at[opposite, :, cols], self.far_in.at[:, cols], opposite * 2 + self.core if direct else nxt),
                (self.chip_sum.at[behind, :, cols], self.near_in.at[:, cols], prv),
                (self.chip_sum.at[ahead, :, cols], self.last_in.at[:, cols], nxt),
            )[kind - 4]
        return remote(src, dst, self.send_sems.at[kind, j], self.recv_sems.at[kind, j], peer)

    def go(self, kind, j, cols, way, direct):
        copy = self.copy(kind, j, cols, way, direct)
        copy.start()
        self.sends.append(copy)

    def begin(self, j, cols, way, direct):
        for kind in range(1 if self.joint else 4):
            self.go(kind, j, cols, way, direct)

    def pair(self, kind, k, j, cols, way, direct):
        if kind == 0 or not self.joint:
            self.copy(kind, j, cols, way, direct).wait_recv()
        return self.part[k, self.core, :, cols].astype(F32) + self.from_other[k, :, cols].astype(F32)

    def far(self, j, cols, way, direct):
        opposite = lax.rem(self.chip + 2, CHIPS)
        self.chip_sum[opposite, :, cols] = self.pair(0, opposite, j, cols, way, direct).astype(BF16)
        self.go(4, j, cols, way, direct)

    def near(self, j, cols, way, direct):
        behind = lax.rem(self.chip + CHIPS - way, CHIPS)
        self.chip_sum[behind, :, cols] = self.pair(1, behind, j, cols, way, direct).astype(BF16)
        self.go(5, j, cols, way, direct)

    def third(self, j, cols, way, direct):
        ahead = lax.rem(self.chip + CHIPS + way, CHIPS)
        mine = self.pair(2, ahead, j, cols, way, direct)
        if not direct:
            self.copy(4, j, cols, way, direct).wait_recv()
            mine = mine + self.far_in[:, cols].astype(F32)
        self.chip_sum[ahead, :, cols] = mine.astype(BF16)
        self.go(6, j, cols, way, direct)

    def last(self, j, cols, way, direct):
        own = self.pair(3, self.chip, j, cols, way, direct)
        self.copy(5, j, cols, way, direct).wait_recv()
        own = own + self.near_in[:, cols].astype(F32)
        if direct:
            self.copy(4, j, cols, way, direct).wait_recv()
            own = own + self.far_in[:, cols].astype(F32)
        self.copy(6, j, cols, way, direct).wait_recv()
        return own + self.last_in[:, cols].astype(F32)

    def finish(self):
        for copy in self.sends:
            copy.wait_send()


def mlp_kernel(attn_ref, x_buf, gain_ref, wo_ref, w1_hbm, w3_hbm, w2_hbm, out_ref,
               part, other_in, chip_sum, far_in, near_in, last_in,
               x1_buf, h_buf, act_buf, w1_buf, w3_buf, w2_buf,
               w_sems, rs1_send, rs1_recv, ag_send, ag_recv, rs2_send, rs2_recv):
    me, core, chip, other, right, left = places()
    knock(other, right, left, lax.rem(chip + 2, CHIPS) * 2 + core)
    width = x_buf.shape[1]
    n_tok = act_buf.shape[0]
    n_chunks = w1_buf.shape[0]
    chunk = w1_buf.shape[2]

    def weight(kind, i):
        src = (w1_hbm, w3_hbm, w2_hbm)[kind]
        dst = (w1_buf, w3_buf, w2_buf)[kind]
        return pltpu.make_async_copy(src.at[0, :, pl.ds(pl.multiple_of(i * chunk, 128), chunk)], dst.at[i], w_sems.at[kind, i])

    queue = [weight(kind, i) for i in range(n_chunks) for kind in range(2)] + [weight(2, i) for i in range(n_chunks)]

    def feed(n):
        for copy in queue[:n]:
            copy.start()
        del queue[:n]

    feed(2)

    def plan(pieces, straight=0):
        size = width // pieces
        return [(j, pl.ds(j * size, size), 1 if j % 2 == 0 else -1, j >= pieces - straight) for j in range(pieces)]

    def put_part(cols, value):
        part[:, :, :, cols] = value.astype(BF16).reshape(CHIPS, 2, n_tok // (2 * CHIPS), value.shape[1])

    plan1 = plan(RS1_PIECES)
    rs1 = Reducer(part, other_in, chip_sum, far_in, near_in, last_in, rs1_send, rs1_recv)
    attn = attn_ref[...]
    for item in plan1:
        put_part(item[1], jnp.dot(attn, wo_ref[0, :, item[1]], preferred_element_type=F32))
    enter(4)
    for kind in range(4):
        for item in plan1:
            rs1.go(kind, *item)
    feed(1)
    for stage, n in ((rs1.far, 0), (rs1.near, 4), (rs1.third, 3)):
        for item in plan1:
            stage(*item)
        feed(n)
    for item in plan1:
        cols = item[1]
        x1_buf[:, cols] = (x_buf[:, cols].astype(F32) + rs1.last(*item)).astype(BF16)
    rs1.finish()
    h_buf[me] = norm_rows(x1_buf[...].astype(F32), gain_ref[...].astype(F32))
    gather_rows(h_buf, ag_send, ag_recv, queue)

    def gate_up(i, carry):
        weight(0, i).wait()
        weight(1, i).wait()
        h_all = h_buf[...].reshape(n_tok, width)
        gate = jnp.dot(h_all, w1_buf[i], preferred_element_type=F32)
        up = jnp.dot(h_all, w3_buf[i], preferred_element_type=F32)
        act_buf[:, pl.ds(pl.multiple_of(i * chunk, 128), chunk)] = (gate * jax.nn.sigmoid(gate) * up).astype(BF16)
        return carry

    lax.fori_loop(0, n_chunks, gate_up, 0)

    rs2 = Reducer(part, other_in, chip_sum, far_in, near_in, last_in, rs2_send, rs2_recv, joint=True)
    plan2 = plan(n_chunks, RS2_STRAIGHT)
    for j in range(n_chunks + RS2_LAG):
        if j < n_chunks:
            weight(2, j).wait()
            put_part(plan2[j][1], jnp.dot(act_buf[...], w2_buf[j], preferred_element_type=F32))
            rs2.begin(*plan2[j])
        if j >= RS2_LAG:
            rs2.far(*plan2[j - RS2_LAG])
            rs2.near(*plan2[j - RS2_LAG])
            if plan2[j - RS2_LAG][3]:
                rs2.third(*plan2[j - RS2_LAG])
    for item in plan2:
        if not item[3]:
            rs2.third(*item)
    for item in plan2:
        cols = item[1]
        out_ref[:, cols] = (x1_buf[:, cols].astype(F32) + rs2.last(*item)).astype(BF16)
    rs2.finish()


def shape(dims, dtype=BF16):
    return jax.ShapeDtypeStruct(dims, dtype)


def to_tiles(cache):
    _, n_tok, n_rows, n_heads, head = cache.shape
    halves = head // LANES
    return cache.reshape(n_tok, n_rows, n_heads, halves, LANES).transpose(0, 1, 3, 2, 4).reshape(n_tok, n_rows * halves * n_heads, LANES)


def from_tiles(tiles, like):
    _, n_tok, n_rows, n_heads, head = like.shape
    halves = head // LANES
    return tiles.reshape(n_tok, n_rows, halves, n_heads, LANES).transpose(0, 1, 3, 2, 4).reshape(like.shape)


def run_qkv(x, gain, pos2, wq, wk, wv, k_tiles, v_tiles, wo):
    n_tok = k_tiles.shape[0]
    rows, width = x.shape
    cols = wq.shape[2]
    blocks = n_tok // rows
    dma = pltpu.SemaphoreType.DMA
    args = (x, gain, pos2, wq, wk, wv, k_tiles, v_tiles, wo)
    return pl.pallas_call(
        qkv_kernel,
        out_shape=[shape((n_tok, cols))] * 3 + [shape(k_tiles.shape)] * 2 + [shape((cols // (2 * LANES) * n_tok, LANES), F32), shape(wo.shape)],
        in_specs=[HBM] * len(args),
        out_specs=[VMEM] * 7,
        scratch_shapes=[
            pltpu.VMEM((2, n_tok, LANES), F32), pltpu.VMEM((rows, width), BF16), pltpu.VMEM(gain.shape, BF16), pltpu.VMEM(pos2.shape, pos2.dtype),
            pltpu.VMEM((blocks, rows, width), BF16), pltpu.VMEM((3, width, cols), BF16),
            dma((7,)), dma((2, 8)), dma((GATHER_SEMS,)), dma((GATHER_SEMS,))],
        compiler_params=pltpu.CompilerParams(collective_id=0, has_side_effects=True, vmem_limit_bytes=16 << 20),
        name='gather_qkv',
    )(*(pltpu.with_memory_space_constraint(a, pltpu.HBM) for a in args))


def run_attn(pos2, pos_rows, q, k, v, k_tiles, v_tiles):
    n_tok = k_tiles.shape[0]
    rows2 = q.shape[1] // (2 * LANES) * n_tok
    dma = pltpu.SemaphoreType.DMA
    wide = pltpu.VMEM((2, rows2, LANES), F32)
    tiles = shape(k_tiles.shape)
    attn, _, _, k_out, v_out = pl.pallas_call(
        attn_kernel,
        out_shape=[shape(q.shape), tiles, tiles, tiles, tiles],
        in_specs=[HBM, VMEM, VMEM, VMEM, VMEM, VMEM, VMEM],
        out_specs=[VMEM, VMEM, VMEM, HBM, HBM],
        scratch_shapes=[
            pltpu.SMEM(pos2.shape, pos2.dtype), pltpu.VMEM((2, n_tok * 8, LANES), F32), wide, wide,
            pltpu.VMEM((TOK_STEP // TOK_UNIT, 4 * TOK_SUB, k_tiles.shape[1]), F32), pltpu.VMEM((TOK_STEP // TOK_UNIT, 8 * TOK_SUB, k_tiles.shape[1]), F32),
            dma, dma((2, n_tok // TOK_STEP))],
        input_output_aliases={5: 1, 6: 2},
        compiler_params=pltpu.CompilerParams(vmem_limit_bytes=8 << 20),
        name='attention',
    )(pltpu.with_memory_space_constraint(pos2, pltpu.HBM), pos_rows, q, k, v, k_tiles, v_tiles)
    return attn, k_out, v_out


def run_mlp(attn, x, gain, wo, w1, w3, w2):
    rows, width = x.shape
    n_tok = attn.shape[0]
    ffn = w1.shape[2]
    chunk = MLP_CHUNK
    n_chunks = ffn // chunk
    dma = pltpu.SemaphoreType.DMA
    block = pltpu.VMEM((rows, width), BF16)
    chips = pltpu.VMEM((CHIPS, rows, width), BF16)
    return pl.pallas_call(
        mlp_kernel,
        out_shape=pltpu.VMEM((rows, width), BF16),
        in_specs=[VMEM, VMEM, VMEM, VMEM, HBM, HBM, HBM],
        out_specs=VMEM,
        scratch_shapes=[
            pltpu.VMEM((CHIPS, 2, rows, width), BF16), chips, chips, block, block, block,
            block, pltpu.VMEM((n_tok // rows, rows, width), BF16), pltpu.VMEM((n_tok, ffn), BF16),
            pltpu.VMEM((n_chunks, width, chunk), BF16), pltpu.VMEM((n_chunks, width, chunk), BF16), pltpu.VMEM((width // chunk, ffn, chunk), BF16),
            dma((3, n_chunks)), dma((7, RS1_PIECES)), dma((7, RS1_PIECES)), dma((GATHER_SEMS,)), dma((GATHER_SEMS,)),
            dma((7, n_chunks)), dma((7, n_chunks))],
        compiler_params=pltpu.CompilerParams(collective_id=1, has_side_effects=True, vmem_limit_bytes=MLP_VMEM),
        name='reduce_mlp',
    )(*(pltpu.with_memory_space_constraint(a, pltpu.VMEM) for a in (attn, x, gain, wo)), w1, w3, w2)


def solution(mesh):
    row_spec = P(('data', 'model'), None)
    cache_spec = P(None, 'data', None, 'model', None)
    col_spec = P(None, None, 'model')
    inner_spec = P(None, 'model', None)
    in_specs = (row_spec, P('data'), P(), P(), col_spec, col_spec, col_spec, inner_spec, col_spec, col_spec, inner_spec, cache_spec, cache_spec)
    out_specs = (row_spec, cache_spec, cache_spec)

    def device_step(hidden, positions, attn_gain, mlp_gain, w_query, w_key, w_value, w_out, w_gate, w_up, w_down, k_cache, v_cache):
        n_tok = positions.shape[0]
        pos2 = positions.reshape(1, n_tok)
        q, k, v, k_tiles, v_tiles, pos_rows, wo = run_qkv(hidden, attn_gain, pos2, w_query, w_key, w_value, to_tiles(k_cache), to_tiles(v_cache), w_out)
        attn, k_out, v_out = run_attn(pos2, pos_rows, q, k, v, k_tiles, v_tiles)
        out = run_mlp(attn, hidden, mlp_gain, wo, w_gate, w_up, w_down)
        return out, from_tiles(k_out, k_cache), from_tiles(v_out, v_cache)

    return jax.shard_map(device_step, mesh=mesh, in_specs=in_specs, out_specs=out_specs, check_vma=False)
```

```python
import functools
import math
import jax
import jax.numpy as jnp
from jax import lax
from jax.experimental import pallas as pl
from jax.experimental.pallas import tpu as pltpu
from jax.sharding import PartitionSpec as P

NORM_EPS = 1e-5
ROPE_BASE = 10000.0
BF16 = jnp.bfloat16
F32 = jnp.float32
VMEM = pl.BlockSpec(memory_space=pltpu.VMEM)
HBM = pl.BlockSpec(memory_space=pltpu.HBM)
MLP_VMEM = 61600000
CHIPS = 4
MLP_CHUNK = 512
RS1_PIECES = 4
RS2_LAG = 2
RS2_STRAIGHT = 4
GATHER_SEMS = 21


def places():
    me = lax.axis_index('model')
    core = lax.rem(me, 2)
    chip = lax.div(me, 2)
    other = me + 1 - 2 * core
    right = lax.rem(chip + 1, CHIPS) * 2 + core
    left = lax.rem(chip + CHIPS - 1, CHIPS) * 2 + core
    return me, core, chip, other, right, left


def knock(*peers):
    barrier = pltpu.get_barrier_semaphore()
    for peer in peers:
        pl.semaphore_signal(barrier, inc=1, device_id={'model': peer})


def enter(peers):
    pl.semaphore_wait(pltpu.get_barrier_semaphore(), peers)


def remote(src, dst, send_sem, recv_sem, peer):
    return pltpu.make_async_remote_copy(src_ref=src, dst_ref=dst, send_sem=send_sem, recv_sem=recv_sem, device_id={'model': peer})


def norm_rows(x_f, gain_f):
    inv_rms = lax.rsqrt(jnp.mean(x_f * x_f, axis=-1, keepdims=True) + NORM_EPS)
    return (x_f * inv_rms * gain_f).astype(BF16)


def gather_rows(buf, send_sems, recv_sems, behind=(), meanwhile=None):
    me, core, chip, other, right, left = places()
    width = buf.shape[2]
    quarter = width // 4
    q0, q1, q2, q3 = (pl.ds(i * quarter, quarter) for i in range(4))
    lo, hi, full = pl.ds(0, 2 * quarter), pl.ds(2 * quarter, 2 * quarter), pl.ds(0, width)
    far = lax.rem(chip + 2, CHIPS) * 2 + core
    sends = []

    def hop(blk, cols, idx, peer):
        view = buf.at[blk, :, cols]
        return remote(view, view, send_sems.at[idx], recv_sems.at[idx], peer)

    def arrive(blk, cols, idx):
        hop(blk, cols, idx, other).wait_recv()

    def send(blk, cols, idx, peer):
        copy = hop(blk, cols, idx, peer)
        copy.start()
        sends.append(copy)

    for cols, idx, peer in (
            (q0, 0, right), (q2, 1, left), (q1, 9, far), (q3, 10, far), (q1, 2, right), (q3, 3, left), (hi, 4, right), (lo, 5, left),
            (full, 6, other)):
        send(me, cols, idx, peer)
    across = []
    behind = list(behind)
    share = -(-len(behind) // 8)
    for copy in behind[:2 * share]:
        copy.start()
    behind = behind[2 * share:]
    if meanwhile is not None:
        meanwhile()
    for blk, cols, idx, onward, peer in (
            (left, q0, 0, 7, right), (right, q2, 1, 8, left), (left, q1, 2, None, None), (right, q3, 3, None, None),
            (left, hi, 4, None, None), (right, lo, 5, None, None),
            (far, q1, 9, None, None), (far, q3, 10, None, None), (far, q0, 7, None, None), (far, q2, 8, None, None)):
        arrive(blk, cols, idx)
        if onward is not None:
            send(blk, cols, onward, peer)
        send(blk, cols, 11 + len(across), other)
        across.append((blk + 1 - 2 * core, cols, 11 + len(across)))
        for copy in behind[:share]:
            copy.start()
        behind = behind[share:]
    arrive(other, full, 6)
    for item in across:
        arrive(*item)
    for copy in sends:
        copy.wait_send()


LANES = 128


def qkv_kernel(x_hbm, gain_hbm, pos_hbm, wq_hbm, wk_hbm, wv_hbm, kc_hbm, vc_hbm, wo_hbm, q_ref, k_ref, v_ref, kb_ref, vb_ref, pc_ref, wo_ref,
               trig_buf, x_buf, gain_ref, pos_ref, h_buf, w_buf, load_sems, cache_sems, send_sems, recv_sems):
    me, core, chip, other, right, left = places()
    knock(other, right, left, lax.rem(chip + 2, CHIPS) * 2 + core)
    loads = [pltpu.make_async_copy(src, dst, load_sems.at[3 + i]) for i, (src, dst) in enumerate(((x_hbm, x_buf), (gain_hbm, gain_ref), (pos_hbm, pos_ref)))]
    w_copies = [pltpu.make_async_copy(w.at[0], w_buf.at[i], load_sems.at[i]) for i, w in enumerate((wq_hbm, wk_hbm, wv_hbm))]
    pieces = cache_sems.shape[1]
    piece = kb_ref.shape[0] // pieces
    cache_in = []
    for kv, (hbm, buf) in enumerate(((kc_hbm, kb_ref), (vc_hbm, vb_ref))):
        for p in range(pieces):
            toks = pl.ds(p * piece, piece)
            cache_in.append(pltpu.make_async_copy(hbm.at[toks], buf.at[toks], cache_sems.at[kv, p]))
    cache_in.append(pltpu.make_async_copy(wo_hbm, wo_ref, load_sems.at[6]))
    for copy in loads + w_copies[:1]:
        copy.start()
    for copy in loads:
        copy.wait()
    h_buf[me] = norm_rows(x_buf[...].astype(F32), gain_ref[...].astype(F32))
    enter(4)
    n_tok = pos_ref.shape[1]
    half = LANES
    head = 2 * half
    pos_f = pos_ref[...].astype(F32)

    def pick(rows, per):
        own = lax.broadcasted_iota(jnp.int32, (rows, n_tok), 0) // per == lax.broadcasted_iota(jnp.int32, (rows, n_tok), 1)
        return jnp.sum(jnp.where(own, jnp.broadcast_to(pos_f, (rows, n_tok)), 0.0), axis=1, keepdims=True)

    def tables():
        lane = lax.broadcasted_iota(jnp.int32, (n_tok, half), 1).astype(F32)
        angles = pick(n_tok, 1) * jnp.exp(lane * (-2.0 * math.log(ROPE_BASE) / head))
        trig_buf[0] = jnp.cos(angles)
        trig_buf[1] = jnp.sin(angles)
        rows2 = pc_ref.shape[0]
        pc_ref[...] = jnp.broadcast_to(pick(rows2, rows2 // n_tok), pc_ref.shape)

    gather_rows(h_buf, send_sems, recv_sems, w_copies[1:] + cache_in, tables)
    cos_tab, sin_tab = trig_buf[0], trig_buf[1]
    h_all = h_buf[...].reshape(n_tok, h_buf.shape[2])
    for i, out_ref in enumerate((q_ref, k_ref, v_ref)):
        w_copies[i].wait()
        proj = jnp.dot(h_all, w_buf[i], preferred_element_type=F32).astype(BF16)
        if i == 2:
            out_ref[...] = proj
            continue
        for h0 in range(0, proj.shape[1], head):
            front = proj[:, h0:h0 + half].astype(F32)
            back = proj[:, h0 + half:h0 + head].astype(F32)
            out_ref[:, h0:h0 + half] = (front * cos_tab - back * sin_tab).astype(BF16)
            out_ref[:, h0 + half:h0 + head] = (back * cos_tab + front * sin_tab).astype(BF16)
    for copy in cache_in:
        copy.wait()


TOK_STEP = 16
TOK_UNIT = 8
TOK_SUB = 4


def attn_kernel(pos_hbm, pc_buf, q_ref, k_ref, v_ref, kb_in, vb_in, attn_ref, k_buf, v_buf, ko_hbm, vo_hbm,
                pos_smem, new_buf, q_buf, o_buf, score_buf, prob_buf, pos_sem, out_sems):
    n_tok, per_tok, lanes = k_buf.shape
    n_heads = 2
    head = q_ref.shape[1] // n_heads
    steps = n_tok // TOK_STEP
    bufs = (k_buf, v_buf)
    pos_copy = pltpu.make_async_copy(pos_hbm, pos_smem, pos_sem)
    pos_copy.start()

    def write_out(t):
        toks = pl.ds(t * TOK_STEP, TOK_STEP)
        return [pltpu.make_async_copy(buf.at[toks], hbm.at[toks], out_sems.at[kv, t]) for kv, (buf, hbm) in enumerate(zip(bufs, (ko_hbm, vo_hbm)))]

    for h in range(n_heads):
        for c in range(2):
            cols = slice(h * head + c * lanes, h * head + (c + 1) * lanes)
            q_buf.at[c][pl.ds(h, n_tok, stride=2), :] = q_ref[:, cols].astype(F32)
            for kv, ref in enumerate((k_ref, v_ref)):
                new = ref[:, cols].astype(F32)
                for again in range(2):
                    new_buf.at[kv][pl.ds(4 * again + 2 * c + h, n_tok, stride=8), :] = new
    tile_row = lax.broadcasted_iota(jnp.int32, (16, lanes), 0)
    sub = TOK_SUB * n_heads
    tok_of = (lax.broadcasted_iota(jnp.int32, (4 * sub, per_tok), 0) % sub) // 2
    row = lax.broadcasted_iota(jnp.int32, (2 * sub, per_tok), 0)
    col = lax.broadcasted_iota(jnp.int32, (2 * sub, per_tok), 1)
    counts = ((col & 2) == 0) & ((col & 1) == (row & 1))
    key_pos = (col >> 2).astype(F32)

    def shift(x, by):
        return jnp.concatenate([pltpu.roll(x[:, i:i + lanes], by % lanes, 1) for i in range(0, per_tok, lanes)], axis=1)

    def pair(buf, b0):
        one, two = (buf[pl.ds(b0 + g * TOK_SUB, TOK_SUB)] for g in range(2))
        return jnp.concatenate([x.reshape(TOK_SUB * per_tok, lanes) for x in (one, two)], axis=1)

    def out_rows(b0):
        return [pl.ds(pl.multiple_of(b0 * n_heads + g * sub, sub), sub) for g in range(2)]

    units = TOK_STEP // TOK_UNIT

    def mix(t, u):
        b0 = t * TOK_STEP + u * TOK_UNIT
        probs = prob_buf[u]
        wide = jnp.concatenate([jnp.where(tok_of == m, probs, 0.0) for m in range(TOK_SUB)], axis=1).astype(BF16)
        out = jnp.dot(wide, pair(v_buf, b0), preferred_element_type=F32).astype(BF16).astype(F32)
        rows = out_rows(b0)
        for g in range(2):
            for c in range(2):
                at = (2 * g + c) * sub
                o_buf[c, rows[g], :] = out[at:at + sub, g * lanes:(g + 1) * lanes]

    def soften(u):
        total = score_buf[u]
        e = jnp.exp(total - jnp.max(total, axis=1, keepdims=True))
        probs = (e / jnp.sum(e, axis=1, keepdims=True)).astype(BF16).astype(F32)
        moved = shift(probs, 2)
        prob_buf[u] = jnp.concatenate([probs[:sub], moved[:sub], probs[sub:], moved[sub:]], axis=0)

    def insert(t):
        for i in range(TOK_STEP):
            b = t * TOK_STEP + i
            pos = pos_smem[0, b]
            tile = pl.ds(pl.multiple_of((pos >> 2) * 16, 16), 16)
            hit = (tile_row >> 2) == (pos & 3)
            for kv in range(2):
                new = new_buf[kv, pl.ds(pl.multiple_of(b * 8, 8), 8), :]
                old = bufs[kv][b, tile, :].astype(F32)
                bufs[kv][b, tile, :] = jnp.where(hit, jnp.concatenate([new, new], axis=0), old).astype(BF16)

    def score(t, u):
        b0 = t * TOK_STEP + u * TOK_UNIT
        rows = out_rows(b0)
        none = jnp.zeros((sub, lanes), F32)
        q = jnp.concatenate(
            [jnp.concatenate([q_buf[c, rows[0], :], none], axis=1) for c in range(2)] +
            [jnp.concatenate([none, q_buf[c, rows[1], :]], axis=1) for c in range(2)], axis=0).astype(BF16)
        scores = lax.dot_general(q, pair(k_buf, b0), (((1,), (1,)), ((), ())), preferred_element_type=F32)
        mine = scores[:, :per_tok]
        for m in range(1, TOK_SUB):
            mine = jnp.where(tok_of == m, scores[:, m * per_tok:(m + 1) * per_tok], mine)
        first = jnp.concatenate([mine[:sub], mine[2 * sub:3 * sub]], axis=0)
        second = jnp.concatenate([mine[sub:2 * sub], mine[3 * sub:]], axis=0)
        total = (first + shift(second, -2)) * (head ** -0.5)
        pos_of = pc_buf[pl.ds(pl.multiple_of(b0 * n_heads, 2 * sub), 2 * sub), :]
        score_buf[u] = jnp.where(counts & (key_pos <= jnp.concatenate([pos_of] * (per_tok // lanes), axis=1)), total, -1e30)

    def send(t):
        for copy in write_out(t):
            copy.start()

    def each(stage, *args):
        for u in range(units):
            stage(*args, u)

    pos_copy.wait()
    insert(0)

    def place(t, carry):
        insert(t)
        send(t - 1)
        return carry

    lax.fori_loop(1, steps, place, 0)
    each(score, 0)
    send(steps - 1)
    each(soften)
    each(score, 1)

    def step(t, carry):
        each(mix, t - 2)
        each(soften)
        each(score, t)
        return carry

    lax.fori_loop(2, steps, step, 0)
    each(mix, steps - 2)
    each(soften)
    each(mix, steps - 1)
    attn_ref[...] = jnp.concatenate([o_buf.at[c][pl.ds(h, n_tok, stride=2), :] for h in range(n_heads) for c in range(2)], axis=1).astype(BF16)
    for t in range(steps):
        for copy in write_out(t):
            copy.wait()


class Reducer:
    def __init__(self, part, from_other, chip_sum, far_in, near_in, last_in, send_sems, recv_sems, joint=False):
        self.joint = joint
        self.part, self.from_other, self.chip_sum = part, from_other, chip_sum
        self.far_in, self.near_in, self.last_in = far_in, near_in, last_in
        self.send_sems, self.recv_sems = send_sems, recv_sems
        self.me, self.core, self.chip, self.other, self.right, self.left = places()
        self.sends = []

    def copy(self, kind, j, cols, way, direct):
        nxt, prv = (self.right, self.left) if way > 0 else (self.left, self.right)
        ahead = lax.rem(self.chip + CHIPS + way, CHIPS)
        behind = lax.rem(self.chip + CHIPS - way, CHIPS)
        opposite = lax.rem(self.chip + 2, CHIPS)
        if kind < 4:
            k = (opposite, behind, ahead, self.chip)[kind]
            k = slice(None) if self.joint else k
            src, dst, peer = self.part.at[k, 1 - self.core, :, cols], self.from_other.at[k, :, cols], self.other
        else:
            src, dst, peer = (
                (self.chip_sum.at[opposite, :, cols], self.far_in.at[:, cols], opposite * 2 + self.core if direct else nxt),
                (self.chip_sum.at[behind, :, cols], self.near_in.at[:, cols], prv),
                (self.chip_sum.at[ahead, :, cols], self.last_in.at[:, cols], nxt),
            )[kind - 4]
        return remote(src, dst, self.send_sems.at[kind, j], self.recv_sems.at[kind, j], peer)

    def go(self, kind, j, cols, way, direct):
        copy = self.copy(kind, j, cols, way, direct)
        copy.start()
        self.sends.append(copy)

    def begin(self, j, cols, way, direct):
        for kind in range(1 if self.joint else 4):
            self.go(kind, j, cols, way, direct)

    def pair(self, kind, k, j, cols, way, direct):
        if kind == 0 or not self.joint:
            self.copy(kind, j, cols, way, direct).wait_recv()
        return self.part[k, self.core, :, cols].astype(F32) + self.from_other[k, :, cols].astype(F32)

    def far(self, j, cols, way, direct):
        opposite = lax.rem(self.chip + 2, CHIPS)
        self.chip_sum[opposite, :, cols] = self.pair(0, opposite, j, cols, way, direct).astype(BF16)
        self.go(4, j, cols, way, direct)

    def near(self, j, cols, way, direct):
        behind = lax.rem(self.chip + CHIPS - way, CHIPS)
        self.chip_sum[behind, :, cols] = self.pair(1, behind, j, cols, way, direct).astype(BF16)
        self.go(5, j, cols, way, direct)

    def third(self, j, cols, way, direct):
        ahead = lax.rem(self.chip + CHIPS + way, CHIPS)
        mine = self.pair(2, ahead, j, cols, way, direct)
        if not direct:
            self.copy(4, j, cols, way, direct).wait_recv()
            mine = mine + self.far_in[:, cols].astype(F32)
        self.chip_sum[ahead, :, cols] = mine.astype(BF16)
        self.go(6, j, cols, way, direct)

    def last(self, j, cols, way, direct):
        own = self.pair(3, self.chip, j, cols, way, direct)
        self.copy(5, j, cols, way, direct).wait_recv()
        own = own + self.near_in[:, cols].astype(F32)
        if direct:
            self.copy(4, j, cols, way, direct).wait_recv()
            own = own + self.far_in[:, cols].astype(F32)
        self.copy(6, j, cols, way, direct).wait_recv()
        return own + self.last_in[:, cols].astype(F32)

    def finish(self):
        for copy in self.sends:
            copy.wait_send()


def mlp_kernel(attn_ref, x_buf, gain_ref, wo_ref, w1_hbm, w3_hbm, w2_hbm, out_ref,
               part, other_in, chip_sum, far_in, near_in, last_in,
               x1_buf, h_buf, act_buf, w1_buf, w3_buf, w2_buf,
               w_sems, rs1_send, rs1_recv, ag_send, ag_recv, rs2_send, rs2_recv):
    me, core, chip, other, right, left = places()
    knock(other, right, left, lax.rem(chip + 2, CHIPS) * 2 + core)
    width = x_buf.shape[1]
    n_tok = act_buf.shape[0]
    n_chunks = w1_buf.shape[0]
    chunk = w1_buf.shape[2]

    def weight(kind, i):
        src = (w1_hbm, w3_hbm, w2_hbm)[kind]
        dst = (w1_buf, w3_buf, w2_buf)[kind]
        return pltpu.make_async_copy(src.at[0, :, pl.ds(pl.multiple_of(i * chunk, 128), chunk)], dst.at[i], w_sems.at[kind, i])

    queue = [weight(kind, i) for i in range(n_chunks) for kind in range(2)] + [weight(2, i) for i in range(n_chunks)]

    def feed(n):
        for copy in queue[:n]:
            copy.start()
        del queue[:n]

    feed(2)

    def plan(pieces, straight=0):
        size = width // pieces
        return [(j, pl.ds(j * size, size), 1 if j % 2 == 0 else -1, j >= pieces - straight) for j in range(pieces)]

    def put_part(cols, value):
        part[:, :, :, cols] = value.astype(BF16).reshape(CHIPS, 2, n_tok // (2 * CHIPS), value.shape[1])

    plan1 = plan(RS1_PIECES)
    rs1 = Reducer(part, other_in, chip_sum, far_in, near_in, last_in, rs1_send, rs1_recv)
    attn = attn_ref[...]
    for item in plan1:
        put_part(item[1], jnp.dot(attn, wo_ref[0, :, item[1]], preferred_element_type=F32))
    enter(4)
    for kind in range(4):
        for item in plan1:
            rs1.go(kind, *item)
    feed(1)
    for stage, n in ((rs1.far, 0), (rs1.near, 4), (rs1.third, 3)):
        for item in plan1:
            stage(*item)
        feed(n)
    for item in plan1:
        cols = item[1]
        x1_buf[:, cols] = (x_buf[:, cols].astype(F32) + rs1.last(*item)).astype(BF16)
    rs1.finish()
    h_buf[me] = norm_rows(x1_buf[...].astype(F32), gain_ref[...].astype(F32))
    gather_rows(h_buf, ag_send, ag_recv, queue)

    def gate_up(i, carry):
        weight(0, i).wait()
        weight(1, i).wait()
        h_all = h_buf[...].reshape(n_tok, width)
        gate = jnp.dot(h_all, w1_buf[i], preferred_element_type=F32)
        up = jnp.dot(h_all, w3_buf[i], preferred_element_type=F32)
        act_buf[:, pl.ds(pl.multiple_of(i * chunk, 128), chunk)] = (gate * jax.nn.sigmoid(gate) * up).astype(BF16)
        return carry

    lax.fori_loop(0, n_chunks, gate_up, 0)

    rs2 = Reducer(part, other_in, chip_sum, far_in, near_in, last_in, rs2_send, rs2_recv, joint=True)
    plan2 = plan(n_chunks, RS2_STRAIGHT)
    for j in range(n_chunks + RS2_LAG):
        if j < n_chunks:
            weight(2, j).wait()
            put_part(plan2[j][1], jnp.dot(act_buf[...], w2_buf[j], preferred_element_type=F32))
            rs2.begin(*plan2[j])
        if j >= RS2_LAG:
            rs2.far(*plan2[j - RS2_LAG])
            rs2.near(*plan2[j - RS2_LAG])
            if plan2[j - RS2_LAG][3]:
                rs2.third(*plan2[j - RS2_LAG])
    for item in plan2:
        if not item[3]:
            rs2.third(*item)
    for item in plan2:
        cols = item[1]
        out_ref[:, cols] = (x1_buf[:, cols].astype(F32) + rs2.last(*item)).astype(BF16)
    rs2.finish()


def shape(dims, dtype=BF16):
    return jax.ShapeDtypeStruct(dims, dtype)


def to_tiles(cache):
    _, n_tok, n_rows, n_heads, head = cache.shape
    halves = head // LANES
    return cache.reshape(n_tok, n_rows, n_heads, halves, LANES).transpose(0, 1, 3, 2, 4).reshape(n_tok, n_rows * halves * n_heads, LANES)


def from_tiles(tiles, like):
    _, n_tok, n_rows, n_heads, head = like.shape
    halves = head // LANES
    return tiles.reshape(n_tok, n_rows, halves, n_heads, LANES).transpose(0, 1, 3, 2, 4).reshape(like.shape)


def run_qkv(x, gain, pos2, wq, wk, wv, k_tiles, v_tiles, wo):
    n_tok = k_tiles.shape[0]
    rows, width = x.shape
    cols = wq.shape[2]
    blocks = n_tok // rows
    dma = pltpu.SemaphoreType.DMA
    args = (x, gain, pos2, wq, wk, wv, k_tiles, v_tiles, wo)
    return pl.pallas_call(
        qkv_kernel,
        out_shape=[shape((n_tok, cols))] * 3 + [shape(k_tiles.shape)] * 2 + [shape((cols // (2 * LANES) * n_tok, LANES), F32), shape(wo.shape)],
        in_specs=[HBM] * len(args),
        out_specs=[VMEM] * 7,
        scratch_shapes=[
            pltpu.VMEM((2, n_tok, LANES), F32), pltpu.VMEM((rows, width), BF16), pltpu.VMEM(gain.shape, BF16), pltpu.VMEM(pos2.shape, pos2.dtype),
            pltpu.VMEM((blocks, rows, width), BF16), pltpu.VMEM((3, width, cols), BF16),
            dma((7,)), dma((2, 8)), dma((GATHER_SEMS,)), dma((GATHER_SEMS,))],
        compiler_params=pltpu.CompilerParams(collective_id=0, has_side_effects=True, vmem_limit_bytes=16 << 20),
        name='gather_qkv',
    )(*(pltpu.with_memory_space_constraint(a, pltpu.HBM) for a in args))


def run_attn(pos2, pos_rows, q, k, v, k_tiles, v_tiles):
    n_tok = k_tiles.shape[0]
    rows2 = q.shape[1] // (2 * LANES) * n_tok
    dma = pltpu.SemaphoreType.DMA
    wide = pltpu.VMEM((2, rows2, LANES), F32)
    tiles = shape(k_tiles.shape)
    attn, _, _, k_out, v_out = pl.pallas_call(
        attn_kernel,
        out_shape=[shape(q.shape), tiles, tiles, tiles, tiles],
        in_specs=[HBM, VMEM, VMEM, VMEM, VMEM, VMEM, VMEM],
        out_specs=[VMEM, VMEM, VMEM, HBM, HBM],
        scratch_shapes=[
            pltpu.SMEM(pos2.shape, pos2.dtype), pltpu.VMEM((2, n_tok * 8, LANES), F32), wide, wide,
            pltpu.VMEM((TOK_STEP // TOK_UNIT, 4 * TOK_SUB, k_tiles.shape[1]), F32), pltpu.VMEM((TOK_STEP // TOK_UNIT, 8 * TOK_SUB, k_tiles.shape[1]), F32),
            dma, dma((2, n_tok // TOK_STEP))],
        input_output_aliases={5: 1, 6: 2},
        compiler_params=pltpu.CompilerParams(vmem_limit_bytes=8 << 20),
        name='attention',
    )(pltpu.with_memory_space_constraint(pos2, pltpu.HBM), pos_rows, q, k, v, k_tiles, v_tiles)
    return attn, k_out, v_out


def run_mlp(attn, x, gain, wo, w1, w3, w2):
    rows, width = x.shape
    n_tok = attn.shape[0]
    ffn = w1.shape[2]
    chunk = MLP_CHUNK
    n_chunks = ffn // chunk
    dma = pltpu.SemaphoreType.DMA
    block = pltpu.VMEM((rows, width), BF16)
    chips = pltpu.VMEM((CHIPS, rows, width), BF16)
    return pl.pallas_call(
        mlp_kernel,
        out_shape=pltpu.VMEM((rows, width), BF16),
        in_specs=[VMEM, VMEM, VMEM, VMEM, HBM, HBM, HBM],
        out_specs=VMEM,
        scratch_shapes=[
            pltpu.VMEM((CHIPS, 2, rows, width), BF16), chips, chips, block, block, block,
            block, pltpu.VMEM((n_tok // rows, rows, width), BF16), pltpu.VMEM((n_tok, ffn), BF16),
            pltpu.VMEM((n_chunks, width, chunk), BF16), pltpu.VMEM((n_chunks, width, chunk), BF16), pltpu.VMEM((width // chunk, ffn, chunk), BF16),
            dma((3, n_chunks)), dma((7, RS1_PIECES)), dma((7, RS1_PIECES)), dma((GATHER_SEMS,)), dma((GATHER_SEMS,)),
            dma((7, n_chunks)), dma((7, n_chunks))],
        compiler_params=pltpu.CompilerParams(collective_id=1, has_side_effects=True, vmem_limit_bytes=MLP_VMEM),
        name='reduce_mlp',
    )(*(pltpu.with_memory_space_constraint(a, pltpu.VMEM) for a in (attn, x, gain, wo)), w1, w3, w2)


def solution(mesh):
    row_spec = P(('data', 'model'), None)
    cache_spec = P(None, 'data', None, 'model', None)
    col_spec = P(None, None, 'model')
    inner_spec = P(None, 'model', None)
    in_specs = (row_spec, P('data'), P(), P(), col_spec, col_spec, col_spec, inner_spec, col_spec, col_spec, inner_spec, cache_spec, cache_spec)
    out_specs = (row_spec, cache_spec, cache_spec)

    def device_step(hidden, positions, attn_gain, mlp_gain, w_query, w_key, w_value, w_out, w_gate, w_up, w_down, k_cache, v_cache):
        n_tok = positions.shape[0]
        pos2 = positions.reshape(1, n_tok)
        q, k, v, k_tiles, v_tiles, pos_rows, wo = run_qkv(hidden, attn_gain, pos2, w_query, w_key, w_value, to_tiles(k_cache), to_tiles(v_cache), w_out)
        attn, k_out, v_out = run_attn(pos2, pos_rows, q, k, v, k_tiles, v_tiles)
        out = run_mlp(attn, hidden, mlp_gain, wo, w_gate, w_up, w_down)
        return out, from_tiles(k_out, k_cache), from_tiles(v_out, v_cache)

    return jax.shard_map(device_step, mesh=mesh, in_specs=in_specs, out_specs=out_specs, check_vma=False)
```

```python
import functools
import math
import jax
import jax.numpy as jnp
from jax import lax
from jax.experimental import pallas as pl
from jax.experimental.pallas import tpu as pltpu
from jax.sharding import PartitionSpec as P

NORM_EPS = 1e-5
ROPE_BASE = 10000.0
BF16 = jnp.bfloat16
F32 = jnp.float32
VMEM = pl.BlockSpec(memory_space=pltpu.VMEM)
HBM = pl.BlockSpec(memory_space=pltpu.HBM)
MLP_VMEM = 61600000
CHIPS = 4
MLP_CHUNK = 512
RS1_PIECES = 4
RS2_LAG = 2
RS2_STRAIGHT = 5
GATHER_SEMS = 21


def places():
    me = lax.axis_index('model')
    core = lax.rem(me, 2)
    chip = lax.div(me, 2)
    other = me + 1 - 2 * core
    right = lax.rem(chip + 1, CHIPS) * 2 + core
    left = lax.rem(chip + CHIPS - 1, CHIPS) * 2 + core
    return me, core, chip, other, right, left


def knock(*peers):
    barrier = pltpu.get_barrier_semaphore()
    for peer in peers:
        pl.semaphore_signal(barrier, inc=1, device_id={'model': peer})


def enter(peers):
    pl.semaphore_wait(pltpu.get_barrier_semaphore(), peers)


def remote(src, dst, send_sem, recv_sem, peer):
    return pltpu.make_async_remote_copy(src_ref=src, dst_ref=dst, send_sem=send_sem, recv_sem=recv_sem, device_id={'model': peer})


def norm_rows(x_f, gain_f):
    inv_rms = lax.rsqrt(jnp.mean(x_f * x_f, axis=-1, keepdims=True) + NORM_EPS)
    return (x_f * inv_rms * gain_f).astype(BF16)


def gather_rows(buf, send_sems, recv_sems, behind=(), meanwhile=None):
    me, core, chip, other, right, left = places()
    width = buf.shape[2]
    quarter = width // 4
    q0, q1, q2, q3 = (pl.ds(i * quarter, quarter) for i in range(4))
    lo, hi, full = pl.ds(0, 2 * quarter), pl.ds(2 * quarter, 2 * quarter), pl.ds(0, width)
    far = lax.rem(chip + 2, CHIPS) * 2 + core
    sends = []

    def hop(blk, cols, idx, peer):
        view = buf.at[blk, :, cols]
        return remote(view, view, send_sems.at[idx], recv_sems.at[idx], peer)

    def arrive(blk, cols, idx):
        hop(blk, cols, idx, other).wait_recv()

    def send(blk, cols, idx, peer):
        copy = hop(blk, cols, idx, peer)
        copy.start()
        sends.append(copy)

    for cols, idx, peer in (
            (q0, 0, right), (q2, 1, left), (q1, 9, far), (q3, 10, far), (q1, 2, right), (q3, 3, left), (hi, 4, right), (lo, 5, left),
            (full, 6, other)):
        send(me, cols, idx, peer)
    across = []
    behind = list(behind)
    share = -(-len(behind) // 8)
    for copy in behind[:2 * share]:
        copy.start()
    behind = behind[2 * share:]
    if meanwhile is not None:
        meanwhile()
    for blk, cols, idx, onward, peer in (
            (left, q0, 0, 7, right), (right, q2, 1, 8, left), (left, q1, 2, None, None), (right, q3, 3, None, None),
            (left, hi, 4, None, None), (right, lo, 5, None, None),
            (far, q1, 9, None, None), (far, q3, 10, None, None), (far, q0, 7, None, None), (far, q2, 8, None, None)):
        arrive(blk, cols, idx)
        if onward is not None:
            send(blk, cols, onward, peer)
        send(blk, cols, 11 + len(across), other)
        across.append((blk + 1 - 2 * core, cols, 11 + len(across)))
        for copy in behind[:share]:
            copy.start()
        behind = behind[share:]
    arrive(other, full, 6)
    for item in across:
        arrive(*item)
    for copy in sends:
        copy.wait_send()


LANES = 128


def qkv_kernel(x_hbm, gain_hbm, pos_hbm, wq_hbm, wk_hbm, wv_hbm, kc_hbm, vc_hbm, wo_hbm, q_ref, k_ref, v_ref, kb_ref, vb_ref, pc_ref, wo_ref,
               trig_buf, x_buf, gain_ref, pos_ref, h_buf, w_buf, load_sems, cache_sems, send_sems, recv_sems):
    me, core, chip, other, right, left = places()
    knock(other, right, left, lax.rem(chip + 2, CHIPS) * 2 + core)
    loads = [pltpu.make_async_copy(src, dst, load_sems.at[3 + i]) for i, (src, dst) in enumerate(((x_hbm, x_buf), (gain_hbm, gain_ref), (pos_hbm, pos_ref)))]
    w_copies = [pltpu.make_async_copy(w.at[0], w_buf.at[i], load_sems.at[i]) for i, w in enumerate((wq_hbm, wk_hbm, wv_hbm))]
    pieces = cache_sems.shape[1]
    piece = kb_ref.shape[0] // pieces
    cache_in = []
    for kv, (hbm, buf) in enumerate(((kc_hbm, kb_ref), (vc_hbm, vb_ref))):
        for p in range(pieces):
            toks = pl.ds(p * piece, piece)
            cache_in.append(pltpu.make_async_copy(hbm.at[toks], buf.at[toks], cache_sems.at[kv, p]))
    cache_in.append(pltpu.make_async_copy(wo_hbm, wo_ref, load_sems.at[6]))
    for copy in loads:
        copy.start()
    for copy in loads:
        copy.wait()
    h_buf[me] = norm_rows(x_buf[...].astype(F32), gain_ref[...].astype(F32))
    enter(4)
    n_tok = pos_ref.shape[1]
    half = LANES
    head = 2 * half
    pos_f = pos_ref[...].astype(F32)

    def pick(rows, per):
        own = lax.broadcasted_iota(jnp.int32, (rows, n_tok), 0) // per == lax.broadcasted_iota(jnp.int32, (rows, n_tok), 1)
        return jnp.sum(jnp.where(own, jnp.broadcast_to(pos_f, (rows, n_tok)), 0.0), axis=1, keepdims=True)

    def tables():
        lane = lax.broadcasted_iota(jnp.int32, (n_tok, half), 1).astype(F32)
        angles = pick(n_tok, 1) * jnp.exp(lane * (-2.0 * math.log(ROPE_BASE) / head))
        trig_buf[0] = jnp.cos(angles)
        trig_buf[1] = jnp.sin(angles)
        rows2 = pc_ref.shape[0]
        pc_ref[...] = jnp.broadcast_to(pick(rows2, rows2 // n_tok), pc_ref.shape)

    gather_rows(h_buf, send_sems, recv_sems, w_copies + cache_in, tables)
    cos_tab, sin_tab = trig_buf[0], trig_buf[1]
    h_all = h_buf[...].reshape(n_tok, h_buf.shape[2])
    for i, out_ref in enumerate((q_ref, k_ref, v_ref)):
        w_copies[i].wait()
        proj = jnp.dot(h_all, w_buf[i], preferred_element_type=F32).astype(BF16)
        if i == 2:
            out_ref[...] = proj
            continue
        for h0 in range(0, proj.shape[1], head):
            front = proj[:, h0:h0 + half].astype(F32)
            back = proj[:, h0 + half:h0 + head].astype(F32)
            out_ref[:, h0:h0 + half] = (front * cos_tab - back * sin_tab).astype(BF16)
            out_ref[:, h0 + half:h0 + head] = (back * cos_tab + front * sin_tab).astype(BF16)
    for copy in cache_in:
        copy.wait()


TOK_STEP = 16
TOK_UNIT = 8
TOK_SUB = 4


def attn_kernel(pos_hbm, pc_buf, q_ref, k_ref, v_ref, kb_in, vb_in, attn_ref, k_buf, v_buf, ko_hbm, vo_hbm,
                pos_smem, new_buf, q_buf, o_buf, score_buf, prob_buf, pos_sem, out_sems):
    n_tok, per_tok, lanes = k_buf.shape
    n_heads = 2
    head = q_ref.shape[1] // n_heads
    steps = n_tok // TOK_STEP
    bufs = (k_buf, v_buf)
    pos_copy = pltpu.make_async_copy(pos_hbm, pos_smem, pos_sem)
    pos_copy.start()

    def write_out(t):
        toks = pl.ds(t * TOK_STEP, TOK_STEP)
        return [pltpu.make_async_copy(buf.at[toks], hbm.at[toks], out_sems.at[kv, t]) for kv, (buf, hbm) in enumerate(zip(bufs, (ko_hbm, vo_hbm)))]

    for h in range(n_heads):
        for c in range(2):
            cols = slice(h * head + c * lanes, h * head + (c + 1) * lanes)
            q_buf.at[c][pl.ds(h, n_tok, stride=2), :] = q_ref[:, cols].astype(F32)
            for kv, ref in enumerate((k_ref, v_ref)):
                new = ref[:, cols].astype(F32)
                for again in range(2):
                    new_buf.at[kv][pl.ds(4 * again + 2 * c + h, n_tok, stride=8), :] = new
    tile_row = lax.broadcasted_iota(jnp.int32, (16, lanes), 0)
    sub = TOK_SUB * n_heads
    tok_of = (lax.broadcasted_iota(jnp.int32, (4 * sub, per_tok), 0) % sub) // 2
    row = lax.broadcasted_iota(jnp.int32, (2 * sub, per_tok), 0)
    col = lax.broadcasted_iota(jnp.int32, (2 * sub, per_tok), 1)
    counts = ((col & 2) == 0) & ((col & 1) == (row & 1))
    key_pos = (col >> 2).astype(F32)

    def shift(x, by):
        return jnp.concatenate([pltpu.roll(x[:, i:i + lanes], by % lanes, 1) for i in range(0, per_tok, lanes)], axis=1)

    def pair(buf, b0):
        one, two = (buf[pl.ds(b0 + g * TOK_SUB, TOK_SUB)] for g in range(2))
        return jnp.concatenate([x.reshape(TOK_SUB * per_tok, lanes) for x in (one, two)], axis=1)

    def out_rows(b0):
        return [pl.ds(pl.multiple_of(b0 * n_heads + g * sub, sub), sub) for g in range(2)]

    units = TOK_STEP // TOK_UNIT

    def mix(t, u):
        b0 = t * TOK_STEP + u * TOK_UNIT
        probs = prob_buf[u]
        wide = jnp.concatenate([jnp.where(tok_of == m, probs, 0.0) for m in range(TOK_SUB)], axis=1).astype(BF16)
        out = jnp.dot(wide, pair(v_buf, b0), preferred_element_type=F32).astype(BF16).astype(F32)
        rows = out_rows(b0)
        for g in range(2):
            for c in range(2):
                at = (2 * g + c) * sub
                o_buf[c, rows[g], :] = out[at:at + sub, g * lanes:(g + 1) * lanes]

    def soften(u):
        total = score_buf[u]
        e = jnp.exp(total - jnp.max(total, axis=1, keepdims=True))
        probs = (e / jnp.sum(e, axis=1, keepdims=True)).astype(BF16).astype(F32)
        moved = shift(probs, 2)
        prob_buf[u] = jnp.concatenate([probs[:sub], moved[:sub], probs[sub:], moved[sub:]], axis=0)

    def insert(t):
        for i in range(TOK_STEP):
            b = t * TOK_STEP + i
            pos = pos_smem[0, b]
            tile = pl.ds(pl.multiple_of((pos >> 2) * 16, 16), 16)
            hit = (tile_row >> 2) == (pos & 3)
            for kv in range(2):
                new = new_buf[kv, pl.ds(pl.multiple_of(b * 8, 8), 8), :]
                old = bufs[kv][b, tile, :].astype(F32)
                bufs[kv][b, tile, :] = jnp.where(hit, jnp.concatenate([new, new], axis=0), old).astype(BF16)

    def score(t, u):
        b0 = t * TOK_STEP + u * TOK_UNIT
        rows = out_rows(b0)
        none = jnp.zeros((sub, lanes), F32)
        q = jnp.concatenate(
            [jnp.concatenate([q_buf[c, rows[0], :], none], axis=1) for c in range(2)] +
            [jnp.concatenate([none, q_buf[c, rows[1], :]], axis=1) for c in range(2)], axis=0).astype(BF16)
        scores = lax.dot_general(q, pair(k_buf, b0), (((1,), (1,)), ((), ())), preferred_element_type=F32)
        mine = scores[:, :per_tok]
        for m in range(1, TOK_SUB):
            mine = jnp.where(tok_of == m, scores[:, m * per_tok:(m + 1) * per_tok], mine)
        first = jnp.concatenate([mine[:sub], mine[2 * sub:3 * sub]], axis=0)
        second = jnp.concatenate([mine[sub:2 * sub], mine[3 * sub:]], axis=0)
        total = (first + shift(second, -2)) * (head ** -0.5)
        pos_of = pc_buf[pl.ds(pl.multiple_of(b0 * n_heads, 2 * sub), 2 * sub), :]
        score_buf[u] = jnp.where(counts & (key_pos <= jnp.concatenate([pos_of] * (per_tok // lanes), axis=1)), total, -1e30)

    def send(t):
        for copy in write_out(t):
            copy.start()

    def each(stage, *args):
        for u in range(units):
            stage(*args, u)

    pos_copy.wait()
    insert(0)

    def place(t, carry):
        insert(t)
        send(t - 1)
        return carry

    lax.fori_loop(1, steps, place, 0)
    each(score, 0)
    send(steps - 1)
    each(soften)
    each(score, 1)

    def step(t, carry):
        each(mix, t - 2)
        each(soften)
        each(score, t)
        return carry

    lax.fori_loop(2, steps, step, 0)
    each(mix, steps - 2)
    each(soften)
    each(mix, steps - 1)
    attn_ref[...] = jnp.concatenate([o_buf.at[c][pl.ds(h, n_tok, stride=2), :] for h in range(n_heads) for c in range(2)], axis=1).astype(BF16)
    for t in range(steps):
        for copy in write_out(t):
            copy.wait()


class Reducer:
    def __init__(self, part, from_other, chip_sum, far_in, near_in, last_in, send_sems, recv_sems, joint=False):
        self.joint = joint
        self.part, self.from_other, self.chip_sum = part, from_other, chip_sum
        self.far_in, self.near_in, self.last_in = far_in, near_in, last_in
        self.send_sems, self.recv_sems = send_sems, recv_sems
        self.me, self.core, self.chip, self.other, self.right, self.left = places()
        self.sends = []

    def copy(self, kind, j, cols, way, direct):
        nxt, prv = (self.right, self.left) if way > 0 else (self.left, self.right)
        ahead = lax.rem(self.chip + CHIPS + way, CHIPS)
        behind = lax.rem(self.chip + CHIPS - way, CHIPS)
        opposite = lax.rem(self.chip + 2, CHIPS)
        if kind < 4:
            k = (opposite, behind, ahead, self.chip)[kind]
            k = slice(None) if self.joint else k
            src, dst, peer = self.part.at[k, 1 - self.core, :, cols], self.from_other.at[k, :, cols], self.other
        else:
            src, dst, peer = (
                (self.chip_sum.at[opposite, :, cols], self.far_in.at[:, cols], opposite * 2 + self.core if direct else nxt),
                (self.chip_sum.at[behind, :, cols], self.near_in.at[:, cols], prv),
                (self.chip_sum.at[ahead, :, cols], self.last_in.at[:, cols], nxt),
            )[kind - 4]
        return remote(src, dst, self.send_sems.at[kind, j], self.recv_sems.at[kind, j], peer)

    def go(self, kind, j, cols, way, direct):
        copy = self.copy(kind, j, cols, way, direct)
        copy.start()
        self.sends.append(copy)

    def begin(self, j, cols, way, direct):
        for kind in range(1 if self.joint else 4):
            self.go(kind, j, cols, way, direct)

    def pair(self, kind, k, j, cols, way, direct):
        if kind == 0 or not self.joint:
            self.copy(kind, j, cols, way, direct).wait_recv()
        return self.part[k, self.core, :, cols].astype(F32) + self.from_other[k, :, cols].astype(F32)

    def far(self, j, cols, way, direct):
        opposite = lax.rem(self.chip + 2, CHIPS)
        self.chip_sum[opposite, :, cols] = self.pair(0, opposite, j, cols, way, direct).astype(BF16)
        self.go(4, j, cols, way, direct)

    def near(self, j, cols, way, direct):
        behind = lax.rem(self.chip + CHIPS - way, CHIPS)
        self.chip_sum[behind, :, cols] = self.pair(1, behind, j, cols, way, direct).astype(BF16)
        self.go(5, j, cols, way, direct)

    def third(self, j, cols, way, direct):
        ahead = lax.rem(self.chip + CHIPS + way, CHIPS)
        mine = self.pair(2, ahead, j, cols, way, direct)
        if not direct:
            self.copy(4, j, cols, way, direct).wait_recv()
            mine = mine + self.far_in[:, cols].astype(F32)
        self.chip_sum[ahead, :, cols] = mine.astype(BF16)
        self.go(6, j, cols, way, direct)

    def last(self, j, cols, way, direct):
        own = self.pair(3, self.chip, j, cols, way, direct)
        self.copy(5, j, cols, way, direct).wait_recv()
        own = own + self.near_in[:, cols].astype(F32)
        if direct:
            self.copy(4, j, cols, way, direct).wait_recv()
            own = own + self.far_in[:, cols].astype(F32)
        self.copy(6, j, cols, way, direct).wait_recv()
        return own + self.last_in[:, cols].astype(F32)

    def finish(self):
        for copy in self.sends:
            copy.wait_send()


def mlp_kernel(attn_ref, x_buf, gain_ref, wo_ref, w1_hbm, w3_hbm, w2_hbm, out_ref,
               part, other_in, chip_sum, far_in, near_in, last_in,
               x1_buf, h_buf, act_buf, w1_buf, w3_buf, w2_buf,
               w_sems, rs1_send, rs1_recv, ag_send, ag_recv, rs2_send, rs2_recv):
    me, core, chip, other, right, left = places()
    knock(other, right, left, lax.rem(chip + 2, CHIPS) * 2 + core)
    width = x_buf.shape[1]
    n_tok = act_buf.shape[0]
    n_chunks = w1_buf.shape[0]
    chunk = w1_buf.shape[2]

    def weight(kind, i):
        src = (w1_hbm, w3_hbm, w2_hbm)[kind]
        dst = (w1_buf, w3_buf, w2_buf)[kind]
        return pltpu.make_async_copy(src.at[0, :, pl.ds(pl.multiple_of(i * chunk, 128), chunk)], dst.at[i], w_sems.at[kind, i])

    queue = [weight(kind, i) for i in range(n_chunks) for kind in range(2)] + [weight(2, i) for i in range(n_chunks)]

    def feed(n):
        for copy in queue[:n]:
            copy.start()
        del queue[:n]

    feed(2)

    def plan(pieces, straight=0):
        size = width // pieces
        return [(j, pl.ds(j * size, size), 1 if j % 2 == 0 else -1, j >= pieces - straight) for j in range(pieces)]

    def put_part(cols, value):
        part[:, :, :, cols] = value.astype(BF16).reshape(CHIPS, 2, n_tok // (2 * CHIPS), value.shape[1])

    plan1 = plan(RS1_PIECES)
    rs1 = Reducer(part, other_in, chip_sum, far_in, near_in, last_in, rs1_send, rs1_recv)
    attn = attn_ref[...]
    for item in plan1:
        put_part(item[1], jnp.dot(attn, wo_ref[0, :, item[1]], preferred_element_type=F32))
    enter(4)
    for kind in range(4):
        for item in plan1:
            rs1.go(kind, *item)
    feed(1)
    for stage, n in ((rs1.far, 0), (rs1.near, 4), (rs1.third, 3)):
        for item in plan1:
            stage(*item)
        feed(n)
    for item in plan1:
        cols = item[1]
        x1_buf[:, cols] = (x_buf[:, cols].astype(F32) + rs1.last(*item)).astype(BF16)
    rs1.finish()
    h_buf[me] = norm_rows(x1_buf[...].astype(F32), gain_ref[...].astype(F32))
    gather_rows(h_buf, ag_send, ag_recv, queue)

    def gate_up(i, carry):
        weight(0, i).wait()
        weight(1, i).wait()
        h_all = h_buf[...].reshape(n_tok, width)
        gate = jnp.dot(h_all, w1_buf[i], preferred_element_type=F32)
        up = jnp.dot(h_all, w3_buf[i], preferred_element_type=F32)
        act_buf[:, pl.ds(pl.multiple_of(i * chunk, 128), chunk)] = (gate * jax.nn.sigmoid(gate) * up).astype(BF16)
        return carry

    lax.fori_loop(0, n_chunks, gate_up, 0)

    rs2 = Reducer(part, other_in, chip_sum, far_in, near_in, last_in, rs2_send, rs2_recv, joint=True)
    plan2 = plan(n_chunks, RS2_STRAIGHT)
    for j in range(n_chunks + RS2_LAG):
        if j < n_chunks:
            weight(2, j).wait()
            put_part(plan2[j][1], jnp.dot(act_buf[...], w2_buf[j], preferred_element_type=F32))
            rs2.begin(*plan2[j])
        if j >= RS2_LAG:
            rs2.far(*plan2[j - RS2_LAG])
            rs2.near(*plan2[j - RS2_LAG])
            if plan2[j - RS2_LAG][3]:
                rs2.third(*plan2[j - RS2_LAG])
    for item in plan2:
        if not item[3]:
            rs2.third(*item)
    for item in plan2:
        cols = item[1]
        out_ref[:, cols] = (x1_buf[:, cols].astype(F32) + rs2.last(*item)).astype(BF16)
    rs2.finish()


def shape(dims, dtype=BF16):
    return jax.ShapeDtypeStruct(dims, dtype)


def to_tiles(cache):
    _, n_tok, n_rows, n_heads, head = cache.shape
    halves = head // LANES
    return cache.reshape(n_tok, n_rows, n_heads, halves, LANES).transpose(0, 1, 3, 2, 4).reshape(n_tok, n_rows * halves * n_heads, LANES)


def from_tiles(tiles, like):
    _, n_tok, n_rows, n_heads, head = like.shape
    halves = head // LANES
    return tiles.reshape(n_tok, n_rows, halves, n_heads, LANES).transpose(0, 1, 3, 2, 4).reshape(like.shape)


def run_qkv(x, gain, pos2, wq, wk, wv, k_tiles, v_tiles, wo):
    n_tok = k_tiles.shape[0]
    rows, width = x.shape
    cols = wq.shape[2]
    blocks = n_tok // rows
    dma = pltpu.SemaphoreType.DMA
    args = (x, gain, pos2, wq, wk, wv, k_tiles, v_tiles, wo)
    return pl.pallas_call(
        qkv_kernel,
        out_shape=[shape((n_tok, cols))] * 3 + [shape(k_tiles.shape)] * 2 + [shape((cols // (2 * LANES) * n_tok, LANES), F32), shape(wo.shape)],
        in_specs=[HBM] * len(args),
        out_specs=[VMEM] * 7,
        scratch_shapes=[
            pltpu.VMEM((2, n_tok, LANES), F32), pltpu.VMEM((rows, width), BF16), pltpu.VMEM(gain.shape, BF16), pltpu.VMEM(pos2.shape, pos2.dtype),
            pltpu.VMEM((blocks, rows, width), BF16), pltpu.VMEM((3, width, cols), BF16),
            dma((7,)), dma((2, 8)), dma((GATHER_SEMS,)), dma((GATHER_SEMS,))],
        compiler_params=pltpu.CompilerParams(collective_id=0, has_side_effects=True, vmem_limit_bytes=16 << 20),
        name='gather_qkv',
    )(*(pltpu.with_memory_space_constraint(a, pltpu.HBM) for a in args))


def run_attn(pos2, pos_rows, q, k, v, k_tiles, v_tiles):
    n_tok = k_tiles.shape[0]
    rows2 = q.shape[1] // (2 * LANES) * n_tok
    dma = pltpu.SemaphoreType.DMA
    wide = pltpu.VMEM((2, rows2, LANES), F32)
    tiles = shape(k_tiles.shape)
    attn, _, _, k_out, v_out = pl.pallas_call(
        attn_kernel,
        out_shape=[shape(q.shape), tiles, tiles, tiles, tiles],
        in_specs=[HBM, VMEM, VMEM, VMEM, VMEM, VMEM, VMEM],
        out_specs=[VMEM, VMEM, VMEM, HBM, HBM],
        scratch_shapes=[
            pltpu.SMEM(pos2.shape, pos2.dtype), pltpu.VMEM((2, n_tok * 8, LANES), F32), wide, wide,
            pltpu.VMEM((TOK_STEP // TOK_UNIT, 4 * TOK_SUB, k_tiles.shape[1]), F32), pltpu.VMEM((TOK_STEP // TOK_UNIT, 8 * TOK_SUB, k_tiles.shape[1]), F32),
            dma, dma((2, n_tok // TOK_STEP))],
        input_output_aliases={5: 1, 6: 2},
        compiler_params=pltpu.CompilerParams(vmem_limit_bytes=8 << 20),
        name='attention',
    )(pltpu.with_memory_space_constraint(pos2, pltpu.HBM), pos_rows, q, k, v, k_tiles, v_tiles)
    return attn, k_out, v_out


def run_mlp(attn, x, gain, wo, w1, w3, w2):
    rows, width = x.shape
    n_tok = attn.shape[0]
    ffn = w1.shape[2]
    chunk = MLP_CHUNK
    n_chunks = ffn // chunk
    dma = pltpu.SemaphoreType.DMA
    block = pltpu.VMEM((rows, width), BF16)
    chips = pltpu.VMEM((CHIPS, rows, width), BF16)
    return pl.pallas_call(
        mlp_kernel,
        out_shape=pltpu.VMEM((rows, width), BF16),
        in_specs=[VMEM, VMEM, VMEM, VMEM, HBM, HBM, HBM],
        out_specs=VMEM,
        scratch_shapes=[
            pltpu.VMEM((CHIPS, 2, rows, width), BF16), chips, chips, block, block, block,
            block, pltpu.VMEM((n_tok // rows, rows, width), BF16), pltpu.VMEM((n_tok, ffn), BF16),
            pltpu.VMEM((n_chunks, width, chunk), BF16), pltpu.VMEM((n_chunks, width, chunk), BF16), pltpu.VMEM((width // chunk, ffn, chunk), BF16),
            dma((3, n_chunks)), dma((7, RS1_PIECES)), dma((7, RS1_PIECES)), dma((GATHER_SEMS,)), dma((GATHER_SEMS,)),
            dma((7, n_chunks)), dma((7, n_chunks))],
        compiler_params=pltpu.CompilerParams(collective_id=1, has_side_effects=True, vmem_limit_bytes=MLP_VMEM),
        name='reduce_mlp',
    )(*(pltpu.with_memory_space_constraint(a, pltpu.VMEM) for a in (attn, x, gain, wo)), w1, w3, w2)


def solution(mesh):
    row_spec = P(('data', 'model'), None)
    cache_spec = P(None, 'data', None, 'model', None)
    col_spec = P(None, None, 'model')
    inner_spec = P(None, 'model', None)
    in_specs = (row_spec, P('data'), P(), P(), col_spec, col_spec, col_spec, inner_spec, col_spec, col_spec, inner_spec, cache_spec, cache_spec)
    out_specs = (row_spec, cache_spec, cache_spec)

    def device_step(hidden, positions, attn_gain, mlp_gain, w_query, w_key, w_value, w_out, w_gate, w_up, w_down, k_cache, v_cache):
        n_tok = positions.shape[0]
        pos2 = positions.reshape(1, n_tok)
        q, k, v, k_tiles, v_tiles, pos_rows, wo = run_qkv(hidden, attn_gain, pos2, w_query, w_key, w_value, to_tiles(k_cache), to_tiles(v_cache), w_out)
        attn, k_out, v_out = run_attn(pos2, pos_rows, q, k, v, k_tiles, v_tiles)
        out = run_mlp(attn, hidden, mlp_gain, wo, w_gate, w_up, w_down)
        return out, from_tiles(k_out, k_cache), from_tiles(v_out, v_cache)

    return jax.shard_map(device_step, mesh=mesh, in_specs=in_specs, out_specs=out_specs, check_vma=False)
```
